128 devices in a mesh: fsdp: 8 (over z_hi, y), tp: 16 (over z_lo, x, core).
Axes of the slice: x: 4, y: 4, z: 4 (z_hi: 2, z_lo: 2; z = z_hi * 2 + z_lo), core: 2. Of those that a mesh axis runs over, the one named last changes fastest.
Arguments:
- tokens: bfloat16 [2048, 8192], P('fsdp', 'tp'), may hold values from -6 to 6
- out_grad: bfloat16 [2048, 8192], P('fsdp', 'tp'), may hold values from -6 to 6
- gate_weight: bfloat16 [8192, 2048], P('fsdp', 'tp'), may hold values from -0.0625 to 0.0625
- up_weight: bfloat16 [8192, 2048], P('fsdp', 'tp'), may hold values from -0.0625 to 0.0625
- down_weight: bfloat16 [2048, 8192], P('tp', 'fsdp'), may hold values from -0.125 to 0.125
Outputs:
- input_grad: bfloat16 [2048, 8192], P('fsdp', 'tp')
- gate_grad: float32 [8192, 2048], P('fsdp', 'tp')
- up_grad: float32 [8192, 2048], P('fsdp', 'tp')
- down_grad: float32 [2048, 8192], P('tp', 'fsdp')
The draws below stay inside these ranges and needn't reach their ends.
All inputs are finite; a program needn't handle non-finite values.
Results may differ from the reference program's by a relative error of at most 0.0023.
Values may be sent and summed in bfloat16 or wider, within the bound.
A program may use at most 128 MiB of HBM per device.

```python
import math
import jax
import jax.numpy as jnp

D = 8192
FF_WIN = 2048
TOKENS = 2048


def spiked(values, stream_key, source, target, blocks, factor):
    def block_of(dim):
        return (jnp.arange(values.shape[dim]) // (values.shape[dim] // blocks)).reshape((-1,) + (1,) * (values.ndim - 1 - dim))

    one_side = jax.random.permutation(stream_key, blocks)[block_of(target)]
    other_side = (block_of(target) + blocks // 2) % blocks
    return jnp.where((block_of(source) == one_side) | (block_of(source) == other_side), factor * values, values)


def level_of(key, dims, shards, low, largest):
    factor_of = 1.0
    for dim, shards_of in shards:
        heights = jax.random.uniform(jax.random.fold_in(jax.random.fold_in(key, 6), dim), (shards_of,), jnp.float32, low / len(shards), largest / len(shards))
        factor_of = factor_of * jnp.repeat(jnp.exp(heights), dims[dim] // shards_of).reshape((-1,) + (1,) * (len(dims) - 1 - dim))
    return factor_of


def gaussian(key, extent, deviation, bound, pieces=(), dtype=jnp.bfloat16):
    array = jax.random.normal(key, extent, jnp.float32) * deviation
    if len(pieces) > 0:
        array = level_of(key, extent, pieces, -0.22, 0.18) * array
    return jnp.clip(array, min=-bound, max=bound).astype(dtype)


def bell_draw_with(rng, shape, width, most, split, heavy, kind=jnp.bfloat16):
    result = width * jax.random.normal(rng, shape, jnp.float32)
    if split:
        result = result * level_of(rng, shape, split, -0.22, 0.18)
    return jnp.clip(spiked(result, jax.random.fold_in(rng, 3), *heavy), -most, most).astype(kind)


def setup_inputs(seed: int = 0) -> dict:
    seeds = jax.random.split(jax.random.key(seed), 6)
    return {
        "tokens": bell_draw_with(seeds[0], (TOKENS, D), 1.0, 6.0, ((0, 8), (1, 16)), (0, 1, 16, 2.0)),
        "out_grad": bell_draw_with(seeds[1], (TOKENS, D), 1.0, 6.0, ((0, 8), (1, 16)), (0, 1, 16, 2.0)),
        "gate_weight": gaussian(seeds[2], (D, FF_WIN), D ** -0.5, 0.0625, ((0, 8), (1, 16))),
        "up_weight": gaussian(seeds[3], (D, FF_WIN), D ** -0.5, 0.0625, ((0, 8), (1, 16))),
        "down_weight": gaussian(seeds[4], (FF_WIN, D), FF_WIN ** -0.5, 0.125, ((0, 16), (1, 8))),
    }


def reference(tokens, out_grad, gate_weight, up_weight, down_weight):
    gate = jnp.dot(tokens, gate_weight, preferred_element_type=jnp.float32)
    up = jnp.dot(tokens, up_weight, preferred_element_type=jnp.float32)
    squashed = jax.nn.sigmoid(gate)
    activated = gate * squashed
    slope = squashed * (1.0 + gate * (1.0 - squashed))
    hidden = (activated * up).astype(jnp.bfloat16)
    hidden_grad = jnp.dot(out_grad, down_weight.T, preferred_element_type=jnp.float32)
    gate_delta = (hidden_grad * up * slope).astype(jnp.bfloat16)
    up_delta = (hidden_grad * activated).astype(jnp.bfloat16)
    input_grad = jnp.dot(gate_delta, gate_weight.T, preferred_element_type=jnp.float32)
    input_grad = input_grad + jnp.dot(up_delta, up_weight.T, preferred_element_type=jnp.float32)
    factor = 1.0 / math.sqrt(TOKENS)
    gate_grad = jnp.dot(tokens.T, gate_delta, preferred_element_type=jnp.float32) * factor
    up_grad = jnp.dot(tokens.T, up_delta, preferred_element_type=jnp.float32) * factor
    down_grad = jnp.dot(hidden.T, out_grad, preferred_element_type=jnp.float32) * factor
    return (input_grad.astype(jnp.bfloat16), gate_grad, up_grad, down_grad)
```

```python
import math

import jax
import jax.numpy as jnp
from jax import lax
from jax.sharding import Mesh
from jax.sharding import PartitionSpec as P

FSDP = ("z_hi", "y")
TP = ("z_lo", "x", "core")
SWAP = ((0, 0), (1, 2), (2, 1), (3, 3))


def dot(a, b, ca, cb):
    return lax.dot_general(a, b, (((ca,), (cb,)), ((), ())), preferred_element_type=jnp.float32)


def shards(tokens, out_grad, gate_weight, up_weight, down_weight):
    rows, width = tokens.shape
    factor = 1.0 / math.sqrt(rows * lax.axis_size(FSDP))
    both = jnp.stack([tokens, out_grad])
    both = lax.ppermute(both, ("z_hi", "z_lo"), SWAP)
    both = lax.all_gather(both, TP)
    n = both.shape[0] // 2
    both = both.reshape(2, n, 2, rows, width).transpose(2, 0, 3, 1, 4).reshape(2, 2 * rows, n * width)
    whole, grads = both[0], both[1]
    weights = jnp.stack([gate_weight, up_weight, down_weight.T])
    weights = lax.all_gather(weights, "y")
    weights = weights.transpose(1, 0, 2, 3).reshape(3, -1, gate_weight.shape[1])
    wg, wu, wd = weights[0], weights[1], weights[2]
    partial = jnp.stack([dot(whole, wg, 1, 0), dot(whole, wu, 1, 0), dot(grads, wd, 1, 0)])
    partial = partial.reshape(3, 2, rows, -1).transpose(1, 0, 2, 3)
    gate, up, hidden_grad = lax.psum_scatter(partial, "z_hi", scatter_dimension=0, tiled=False)
    squashed = jax.nn.sigmoid(gate)
    activated = gate * squashed
    slope = squashed * (1.0 + gate * (1.0 - squashed))
    hidden = (activated * up).astype(jnp.bfloat16)
    gate_delta = (hidden_grad * up * slope).astype(jnp.bfloat16)
    up_delta = (hidden_grad * activated).astype(jnp.bfloat16)
    acts = lax.all_gather(jnp.stack([gate_delta, up_delta, hidden]), "z_hi")
    acts = acts.transpose(1, 0, 2, 3).reshape(3, 2 * rows, -1)
    gd, ud, hid = acts[0], acts[1], acts[2]
    ig = dot(gd, wg, 1, 1) + dot(ud, wu, 1, 1)
    ig = ig.reshape(2, rows, n, width).transpose(0, 2, 1, 3).reshape(2 * n, rows, width)
    ig = lax.psum_scatter(ig, TP, scatter_dimension=0, tiled=False)
    input_grad = lax.ppermute(ig.astype(jnp.bfloat16), ("z_hi", "z_lo"), SWAP)
    joint = jnp.concatenate([dot(whole, gd, 0, 0), dot(whole, ud, 0, 0), dot(grads, hid, 0, 0)], axis=1) * factor
    summed = lax.psum_scatter(joint, "y", scatter_dimension=0, tiled=True)
    k = gd.shape[1]
    return (input_grad, summed[:, :k], summed[:, k : 2 * k], summed[:, 2 * k :].T)


def solution(mesh):
    finer = Mesh(mesh.devices.reshape(2, 4, 2, 4, 2), ("z_hi", "y", "z_lo", "x", "core"))
    return jax.shard_map(
        shards,
        mesh=finer,
        in_specs=(P(FSDP, TP), P(FSDP, TP), P(FSDP, TP), P(FSDP, TP), P(TP, FSDP)),
        out_specs=(P(FSDP, TP), P(FSDP, TP), P(FSDP, TP), P(TP, FSDP)),
        check_vma=False,
    )
```

```python
import functools
import math

import jax
import jax.numpy as jnp
from jax import lax
from jax.experimental import pallas as pl
from jax.experimental.pallas import tpu as pltpu
from jax.sharding import Mesh
from jax.sharding import PartitionSpec as P

FSDP = ("z_hi", "y")
TP = ("z_lo", "x", "core")
MESH = pl.DeviceIdType.MESH
BF = jnp.bfloat16
F32 = jnp.float32
NSEM = 160
ROUNDS = ((0, 0), (0, 1), (1, 1), (1, 0))


def dot(a, b, ca, cb):
    return lax.dot_general(a, b, (((ca,), (cb,)), ((), ())), preferred_element_type=F32)


def kernel(factor, tok, og, wg, wu, wd, ig_o, gg_o, ug_o, dg_o,
           own, xb, wgu, wdn, pgu, ph, pgur, phr, agu, ah, igp, sibr, farr, nearr, zr, igs, igr,
           ws, hs, gb, hb, gfr, hfr, gnr, hnr, lsem, ssem, rsem):
    R, C = tok.shape
    F = wg.shape[1]
    H = R // 2
    z_hi, y, z_lo, x, core = (lax.axis_index(a) for a in ("z_hi", "y", "z_lo", "x", "core"))
    inner = (z_hi - z_lo) * (z_hi - z_lo)
    is_inner, is_outer = inner == 1, inner == 0
    nx, ny = 4, 4
    xr, xl, xf = lax.rem(x + 1, nx), lax.rem(x + nx - 1, nx), lax.rem(x + 2, nx)
    yr, yl, yf = lax.rem(y + 1, ny), lax.rem(y + ny - 1, ny), lax.rem(y + 2, ny)
    oc = 1 - core
    t_of = (z_hi, 1 - z_hi)
    d_xr, d_xl = (z_hi, y, z_lo, xr, core), (z_hi, y, z_lo, xl, core)
    d_yr, d_yl = (z_hi, yr, z_lo, x, core), (z_hi, yl, z_lo, x, core)
    d_sib = (z_hi, y, z_lo, x, oc)
    d_zlo = (z_hi, y, 1 - z_lo, x, core)
    d_zhi = (1 - z_hi, y, z_lo, x, core)
    d_zz = (1 - z_hi, y, 1 - z_lo, x, core)
    d_zs = (z_lo, y, 1 - z_lo, x, core)
    partners = (d_xr, d_xl, d_yr, d_yl, d_sib, d_zlo, d_zhi, d_zz)

    ids = {}

    def sid(name):
        return ids.setdefault(name, len(ids))

    for k in range(8):
        sid(("z", k))
    pending = []

    def send(name, src, dst, dev, rs=None, wait_later=True):
        i = sid(name)
        c = pltpu.make_async_remote_copy(
            src_ref=src, dst_ref=dst, send_sem=ssem.at[i], recv_sem=rsem.at[i if rs is None else rs],
            device_id=dev, device_id_type=MESH)
        c.start()
        if wait_later:
            pending.append(c)
        return c

    def recv(name, dst):
        i = sid(name)
        pltpu.make_async_remote_copy(
            src_ref=dst, dst_ref=dst, send_sem=ssem.at[i], recv_sem=rsem.at[i],
            device_id=d_sib, device_id_type=MESH).wait_recv()

    def trow(t):
        return pl.ds(pl.multiple_of(t * R, R), R)

    def blk(a, xp, c, t):
        return xb.at[a, 2 * xp + c, trow(t), :]

    def chunk(a, xp, t, h):
        return xb.at[a, 2 * xp + core, pl.ds(pl.multiple_of(t * R + h * H, H), H), :]

    loads_w = [
        pltpu.make_async_copy(wg, wgu.at[y, :, pl.ds(0, F)], lsem.at[0]),
        pltpu.make_async_copy(wu, wgu.at[y, :, pl.ds(F, F)], lsem.at[1]),
        pltpu.make_async_copy(wd, wdn.at[y], lsem.at[2]),
    ]
    loads_t = [
        pltpu.make_async_copy(tok, own.at[0], lsem.at[3]),
        pltpu.make_async_copy(og, own.at[1], lsem.at[4]),
    ]
    for c in loads_t + loads_w:
        c.start()

    @pl.when(is_outer)
    def _():
        pltpu.make_async_copy(tok, blk(0, x, core, z_hi), lsem.at[5]).start()
        pltpu.make_async_copy(og, blk(1, x, core, z_hi), lsem.at[6]).start()

    barrier = pltpu.get_barrier_semaphore()
    for d in partners:
        pl.semaphore_signal(barrier, inc=1, device_id=d, device_id_type=MESH)
    pl.semaphore_wait(barrier, len(partners))

    for c in loads_t:
        c.wait()

    for a in range(2):
        for h in range(2):
            k = 2 * a + h
            send(("zs", k), own.at[a, pl.ds(h * H, H), :], chunk(a, x, z_hi, h), d_zs, rs=4 * inner + k)

    @pl.when(is_outer)
    def _():
        pltpu.make_async_copy(tok, blk(0, x, core, z_hi), lsem.at[5]).wait()
        pltpu.make_async_copy(og, blk(1, x, core, z_hi), lsem.at[6]).wait()

    for c in loads_w:
        c.wait()

    def wchunk(which, yp, h):
        if which == 0:
            return wgu.at[yp, pl.ds(h * C, C), :]
        return wdn.at[yp, pl.ds(h * (F // 2), F // 2), :]

    def ysend(w):
        for h in range(2):
            send(("y", w, 0, h), wchunk(w, y, h), wchunk(w, y, h), d_yr)
            send(("y", w, 1, h), wchunk(w, y, h), wchunk(w, y, h), d_yl)

    def yfwd(w):
        recv(("y", w, 0, 0), wchunk(w, yl, 0))
        send(("yf", w, 0), wchunk(w, yl, 0), wchunk(w, yl, 0), d_yr)
        recv(("y", w, 1, 1), wchunk(w, yr, 1))
        send(("yf", w, 1), wchunk(w, yr, 1), wchunk(w, yr, 1), d_yl)

    def yfin(w):
        recv(("y", w, 0, 1), wchunk(w, yl, 1))
        recv(("y", w, 1, 0), wchunk(w, yr, 0))
        recv(("yf", w, 0), wchunk(w, yf, 0))
        recv(("yf", w, 1), wchunk(w, yf, 1))

    def xsend(r):
        a, rel = ROUNDS[r]
        t = t_of[rel]
        for h in range(2):
            k = 2 * a + h
            if rel == 0:
                @pl.when(is_inner)
                def _():
                    recv(("z", k), chunk(a, x, t, h))
            else:
                recv(("z", 4 + k), chunk(a, x, t, h))

                @pl.when(is_inner)
                def _():
                    send(("zr", k), chunk(a, x, t, h), chunk(a, x, t, h), d_zlo,
                         rs=4 + k, wait_later=False)
            send(("x", r, 0, h), chunk(a, x, t, h), chunk(a, x, t, h), d_xr)
            send(("x", r, 1, h), chunk(a, x, t, h), chunk(a, x, t, h), d_xl)
        send(("s", r, 0), blk(a, x, core, t), blk(a, x, core, t), d_sib)

    def xfwd(r):
        a, rel = ROUNDS[r]
        t = t_of[rel]
        recv(("x", r, 0, 0), chunk(a, xl, t, 0))
        send(("xf", r, 0), chunk(a, xl, t, 0), chunk(a, xl, t, 0), d_xr)
        recv(("x", r, 1, 1), chunk(a, xr, t, 1))
        send(("xf", r, 1), chunk(a, xr, t, 1), chunk(a, xr, t, 1), d_xl)

    def xfin(r):
        a, rel = ROUNDS[r]
        t = t_of[rel]
        recv(("x", r, 0, 1), chunk(a, xl, t, 1))
        send(("s", r, 1), blk(a, xl, core, t), blk(a, xl, core, t), d_sib)
        recv(("x", r, 1, 0), chunk(a, xr, t, 0))
        send(("s", r, 2), blk(a, xr, core, t), blk(a, xr, core, t), d_sib)
        recv(("xf", r, 0), chunk(a, xf, t, 0))
        recv(("xf", r, 1), chunk(a, xf, t, 1))
        send(("s", r, 3), blk(a, xf, core, t), blk(a, xf, core, t), d_sib)

    def sfin(r):
        a, rel = ROUNDS[r]
        t = t_of[rel]
        for j, xp in enumerate((x, xl, xr, xf)):
            recv(("s", r, j), blk(a, xp, oc, t))

    def half(e):
        return pl.ds(pl.multiple_of(lax.rem(e, 2) * C, C), C)

    def forward(r):
        a, rel = ROUNDS[r]
        t = t_of[rel]
        out = (pgu, ph)[a].at[rel]
        out[...] = jnp.zeros(out.shape, F32)

        def step(e, carry):
            block = xb[a, e, trow(t), :]
            if a == 0:
                out[...] += dot(block, wgu[e // 2, half(e), :], 1, 0)
            else:
                out[...] += dot(block, wdn[e // 2, :, half(e)], 1, 1)
            return carry

        lax.fori_loop(0, 2 * nx, step, 0)

    ysend(0)
    xsend(0)
    xfwd(0)
    xsend(1)
    yfwd(0)
    ysend(1)
    xfin(0)
    xfwd(1)
    xsend(2)
    xfin(1)
    xfwd(2)
    xsend(3)
    yfwd(1)
    yfin(0)
    sfin(0)
    sfin(1)
    forward(1)
    send("pgu", pgu.at[1], pgur, d_zhi)
    forward(0)
    xfin(2)
    xfwd(3)
    yfin(1)
    sfin(2)
    forward(2)
    send("ph", ph.at[1], phr, d_zhi)
    xfin(3)
    sfin(3)
    forward(3)

    recv("pgu", pgur)
    recv("ph", phr)
    gate = pgu[0, :, :F] + pgur[:, :F]
    up = pgu[0, :, F:] + pgur[:, F:]
    hg = ph[0] + phr[...]
    squashed = jax.nn.sigmoid(gate)
    activated = gate * squashed
    slope = squashed * (1.0 + gate * (1.0 - squashed))
    agu[trow(z_hi), :F] = (hg * up * slope).astype(BF)
    agu[trow(z_hi), F:] = (hg * activated).astype(BF)
    ah[trow(z_hi), :] = (activated * up).astype(BF)
    send("agu", agu.at[trow(z_hi), :], agu.at[trow(z_hi), :], d_zhi)
    send("ah", ah.at[trow(z_hi), :], ah.at[trow(z_hi), :], d_zhi)

    order = (xf, xr, xl, x)

    def igstart(rel):
        def step(e, carry):
            igp[rel, e] = dot(agu[trow(t_of[rel]), :], wgu[e // 2, half(e), :], 1, 1)
            return carry

        lax.fori_loop(0, 2 * nx, step, 0)
        for j, xp in enumerate(order):
            send(("is", rel, j), igp.at[rel, 2 * xp + oc], sibr.at[rel, xp], d_sib)

    def addsib(rel, j):
        xp = order[j]
        recv(("is", rel, j), sibr.at[rel, xp])
        igp[rel, 2 * xp + core] += sibr[rel, xp]

    def hrow(h):
        return pl.ds(h * H, H)

    def igfirst(rel):
        addsib(rel, 0)
        for h, d in enumerate((d_xr, d_xl)):
            send(("if", rel, h), igp.at[rel, 2 * xf + core, hrow(h), :], farr.at[rel, h], d)
        for h, (j, xp, d) in enumerate(((1, xr, d_xr), (2, xl, d_xl))):
            addsib(rel, j)
            send(("in", rel, h, 1 - h), igp.at[rel, 2 * xp + core, hrow(1 - h), :],
                 nearr.at[rel, h, hrow(1 - h), :], d)

    def igsecond(rel):
        for h, (xp, d) in enumerate(((xr, d_xr), (xl, d_xl))):
            recv(("if", rel, h), farr.at[rel, h])
            igp[rel, 2 * xp + core, hrow(h), :] += farr[rel, h]
            send(("in", rel, h, h), igp.at[rel, 2 * xp + core, hrow(h), :], nearr.at[rel, h, hrow(h), :], d)
        addsib(rel, 3)

    def iglast(rel):
        for h in range(2):
            for g in range(2):
                recv(("in", rel, h, g), nearr.at[rel, h, hrow(g), :])
        igp[rel, 2 * x + core] += nearr[rel, 0] + nearr[rel, 1]

    igstart(0)
    igfirst(0)
    recv("agu", agu.at[trow(1 - z_hi), :])
    recv("ah", ah.at[trow(1 - z_hi), :])
    igstart(1)
    igfirst(1)

    def wstep(e, carry):
        g = dot(xb[0, e], agu[...], 0, 0)
        ws[e] = g
        gb[e] = g.astype(BF)
        d = dot(ah[...], xb[1, e], 0, 0)
        hs[e] = d
        hb[e] = d.astype(BF)
        return carry

    lax.fori_loop(0, 2 * ny, wstep, 0)
    sides = ((yr, d_yr), (yl, d_yl))
    for h, (yp, d) in enumerate(sides):
        send(("gf", h), gb.at[2 * yf + h], gfr.at[h], d)
        send(("hf", h), hb.at[2 * yf + h], hfr.at[h], d)
    for h, (yp, d) in enumerate(sides):
        send(("gn", h, 1 - h), gb.at[2 * yp + 1 - h], gnr.at[h, 1 - h], d)
        send(("hn", h, 1 - h), hb.at[2 * yp + 1 - h], hnr.at[h, 1 - h], d)

    igsecond(1)
    igsecond(0)

    for h, (yp, d) in enumerate(sides):
        recv(("gf", h), gfr.at[h])
        gb[2 * yp + h] = (ws[2 * yp + h] + gfr[h].astype(F32)).astype(BF)
        send(("gn", h, h), gb.at[2 * yp + h], gnr.at[h, h], d)
        recv(("hf", h), hfr.at[h])
        hb[2 * yp + h] = (hs[2 * yp + h] + hfr[h].astype(F32)).astype(BF)
        send(("hn", h, h), hb.at[2 * yp + h], hnr.at[h, h], d)

    def zsend(rel):
        for h in range(2):
            send(("zi", rel, h), igp.at[rel, 2 * x + core, hrow(h), :], zr.at[hrow(h), :], d_zlo,
                 rs=sid(("zir", h)), wait_later=False)

    iglast(1)

    @pl.when(is_outer)
    def _():
        zsend(1)

    iglast(0)

    @pl.when(is_inner)
    def _():
        zsend(0)

    @pl.when(is_inner)
    def _():
        for h in range(2):
            recv(("zir", h), zr.at[hrow(h), :])
            igs[hrow(h), :] = (igp[1, 2 * x + core, hrow(h), :] + zr[hrow(h), :]).astype(BF)
            send(("zo", h), igs.at[hrow(h), :], igr.at[hrow(h), :], d_zz, wait_later=False)

    for h in range(2):
        for s in range(2):
            recv(("gn", s, h), gnr.at[s, h])
            recv(("hn", s, h), hnr.at[s, h])
        g = (ws[2 * y + h] + gnr[0, h].astype(F32) + gnr[1, h].astype(F32)) * factor
        gg_o[pl.ds(h * C, C), :] = g[:, :F]
        ug_o[pl.ds(h * C, C), :] = g[:, F:]
        dg_o[:, pl.ds(h * C, C)] = (hs[2 * y + h] + hnr[0, h].astype(F32) + hnr[1, h].astype(F32)) * factor

    @pl.when(is_outer)
    def _():
        for h in range(2):
            recv(("zir", h), zr.at[hrow(h), :])
            ig_o[hrow(h), :] = (igp[0, 2 * x + core, hrow(h), :] + zr[hrow(h), :]).astype(BF)

    def wait_send(name, src):
        i = sid(name)
        pltpu.make_async_remote_copy(
            src_ref=src, dst_ref=src, send_sem=ssem.at[i], recv_sem=rsem.at[i],
            device_id=d_sib, device_id_type=MESH).wait_send()

    @pl.when(is_inner)
    def _():
        for h in range(2):
            recv(("zo", h), igr.at[hrow(h), :])
        ig_o[...] = igr[...]
        for h in range(2):
            wait_send(("zo", h), igs.at[hrow(h), :])
            wait_send(("zi", 0, h), zr.at[hrow(h), :])
        for k in range(4):
            wait_send(("zr", k), own.at[k // 2, hrow(k % 2), :])

    @pl.when(is_outer)
    def _():
        for h in range(2):
            wait_send(("zi", 1, h), zr.at[hrow(h), :])

    for c in pending:
        c.wait_send()
    assert len(ids) <= NSEM


def shards(tokens, out_grad, gate_weight, up_weight, down_weight):
    R, C = tokens.shape
    F = gate_weight.shape[1]
    H = R // 2
    factor = 1.0 / math.sqrt(R * lax.axis_size(FSDP))
    anyspec = pl.BlockSpec(memory_space=pl.ANY)
    vm = pl.BlockSpec(memory_space=pltpu.VMEM)
    V = pltpu.VMEM
    scratch = [
        V((2, R, C), BF), V((2, 8, 2 * R, C), BF), V((4, 2 * C, 2 * F), BF), V((4, F, 2 * C), BF),
        V((2, R, 2 * F), F32), V((2, R, F), F32), V((R, 2 * F), F32), V((R, F), F32),
        V((2 * R, 2 * F), BF), V((2 * R, F), BF),
        V((2, 8, R, C), F32), V((2, 4, R, C), F32), V((2, 2, H, C), F32), V((2, 2, R, C), F32),
        V((R, C), F32), V((R, C), BF), V((R, C), BF),
        V((8, C, 2 * F), F32), V((8, F, C), F32), V((8, C, 2 * F), BF), V((8, F, C), BF),
        V((2, C, 2 * F), BF), V((2, F, C), BF), V((2, 2, C, 2 * F), BF), V((2, 2, F, C), BF),
        pltpu.SemaphoreType.DMA((8,)), pltpu.SemaphoreType.DMA((NSEM,)), pltpu.SemaphoreType.DMA((NSEM,)),
    ]
    return pl.pallas_call(
        functools.partial(kernel, factor),
        out_shape=(
            jax.ShapeDtypeStruct((R, C), BF),
            jax.ShapeDtypeStruct((2 * C, F), F32),
            jax.ShapeDtypeStruct((2 * C, F), F32),
            jax.ShapeDtypeStruct((F, 2 * C), F32),
        ),
        in_specs=[anyspec] * 5,
        out_specs=(vm,) * 4,
        scratch_shapes=scratch,
        compiler_params=pltpu.CompilerParams(
            collective_id=0, has_side_effects=True, vmem_limit_bytes=60 * 1024 * 1024),
        name="ffn_backward",
    )(tokens, out_grad, gate_weight, up_weight, down_weight)


def solution(mesh):
    finer = Mesh(mesh.devices.reshape(2, 4, 2, 4, 2), ("z_hi", "y", "z_lo", "x", "core"))
    return jax.shard_map(
        shards,
        mesh=finer,
        in_specs=(P(FSDP, TP), P(FSDP, TP), P(FSDP, TP), P(FSDP, TP), P(TP, FSDP)),
        out_specs=(P(FSDP, TP), P(FSDP, TP), P(FSDP, TP), P(TP, FSDP)),
        check_vma=False,
    )
```

```python
import functools
import math

import jax
import jax.numpy as jnp
from jax import lax
from jax.experimental import pallas as pl
from jax.experimental.pallas import tpu as pltpu
from jax.sharding import Mesh
from jax.sharding import PartitionSpec as P

FSDP = ("z_hi", "y")
TP = ("z_lo", "x", "core")
MESH = pl.DeviceIdType.MESH
BF = jnp.bfloat16
F32 = jnp.float32
NSEM = 192
HOME = 128
ROUNDS = ((0, 0, HOME, 256 - HOME), (0, 1, HOME, 256 - HOME), (1, 1, 0, 256), (1, 0, 0, 256))


def dot(a, b, ca, cb):
    return lax.dot_general(a, b, (((ca,), (cb,)), ((), ())), preferred_element_type=F32)


def kernel(factor, tok, og, wg, wu, wd, ig_o, gg_o, ug_o, dg_o,
           own, xb, wgu, wdn, pgu, ph, pgur, phr, agu, ah, igp, sibr, farr, nearr, fs, zr, igs, igr,
           ws, hs, gb, hb, gfr, hfr, gnr, hnr, lsem, ssem, rsem):
    R, C = tok.shape
    F = wg.shape[1]
    H = R // 2
    z_hi, y, z_lo, x, core = (lax.axis_index(a) for a in ("z_hi", "y", "z_lo", "x", "core"))
    inner = (z_hi - z_lo) * (z_hi - z_lo)
    is_inner, is_outer = inner == 1, inner == 0
    nx, ny = 4, 4
    xr, xl, xf = lax.rem(x + 1, nx), lax.rem(x + nx - 1, nx), lax.rem(x + 2, nx)
    yr, yl, yf = lax.rem(y + 1, ny), lax.rem(y + ny - 1, ny), lax.rem(y + 2, ny)
    oc = 1 - core
    t_of = (z_hi, 1 - z_hi)
    d_xr, d_xl = (z_hi, y, z_lo, xr, core), (z_hi, y, z_lo, xl, core)
    d_yr, d_yl = (z_hi, yr, z_lo, x, core), (z_hi, yl, z_lo, x, core)
    d_sib = (z_hi, y, z_lo, x, oc)
    d_zlo = (z_hi, y, 1 - z_lo, x, core)
    d_zhi = (1 - z_hi, y, z_lo, x, core)
    d_zz = (1 - z_hi, y, 1 - z_lo, x, core)
    d_zs = (z_lo, y, 1 - z_lo, x, core)
    partners = (d_xr, d_xl, d_yr, d_yl, d_sib, d_zlo, d_zhi, d_zz)

    ids = {}

    def sid(name):
        return ids.setdefault(name, len(ids))

    for k in range(8):
        sid(("z", k))
    for k in range(8):
        sid(("zh", k))
    pending = []

    def send(name, src, dst, dev, rs=None, wait_later=True):
        i = sid(name)
        c = pltpu.make_async_remote_copy(
            src_ref=src, dst_ref=dst, send_sem=ssem.at[i], recv_sem=rsem.at[i if rs is None else rs],
            device_id=dev, device_id_type=MESH)
        c.start()
        if wait_later:
            pending.append(c)
        return c

    def recv(name, dst):
        i = sid(name)
        pltpu.make_async_remote_copy(
            src_ref=dst, dst_ref=dst, send_sem=ssem.at[i], recv_sem=rsem.at[i],
            device_id=d_sib, device_id_type=MESH).wait_recv()

    def trow(t):
        return pl.ds(pl.multiple_of(t * R, R), R)

    def blk(a, xp, c, t):
        return xb.at[a, 2 * xp + c, trow(t), :]

    def rows(start, n):
        return pl.ds(pl.multiple_of(start, 16), n)

    def chunk(a, xp, t, h, r0, n):
        return xb.at[a, 2 * xp + core, rows(t * R + r0 + h * (n // 2), n // 2), :]

    def part(a, xp, c, t, r0, n):
        return xb.at[a, 2 * xp + c, rows(t * R + r0, n), :]

    home_at = (1 - inner) * z_hi * R + inner * 2 * R

    def home(xp, h=None):
        if h is None:
            return xb.at[0, 2 * xp + core, rows(home_at, HOME), :]
        return xb.at[0, 2 * xp + core, rows(home_at + h * (HOME // 2), HOME // 2), :]

    loads_w = [
        pltpu.make_async_copy(wg, wgu.at[y, :, pl.ds(0, F)], lsem.at[0]),
        pltpu.make_async_copy(wu, wgu.at[y, :, pl.ds(F, F)], lsem.at[1]),
        pltpu.make_async_copy(wd, wdn.at[y], lsem.at[2]),
    ]
    loads_t = [
        pltpu.make_async_copy(tok, own.at[0], lsem.at[3]),
        pltpu.make_async_copy(og, own.at[1], lsem.at[4]),
    ]
    for c in loads_t + loads_w:
        c.start()

    outer_loads = (
        (tok.at[pl.ds(HOME, R - HOME), :], part(0, x, core, z_hi, HOME, R - HOME), lsem.at[5]),
        (og, blk(1, x, core, z_hi), lsem.at[6]),
    )
    load_home = pltpu.make_async_copy(tok.at[pl.ds(0, HOME), :], home(x), lsem.at[7])
    load_home.start()

    @pl.when(is_outer)
    def _():
        for c in outer_loads:
            pltpu.make_async_copy(*c).start()

    barrier = pltpu.get_barrier_semaphore()
    for d in partners:
        pl.semaphore_signal(barrier, inc=1, device_id=d, device_id_type=MESH)
    pl.semaphore_wait(barrier, len(partners))

    for c in loads_t:
        c.wait()
    load_home.wait()

    for a, rel, r0, n in (ROUNDS[0], ROUNDS[3]):
        for h in range(2):
            k = 2 * a + h
            send(("zs", k), own.at[a, pl.ds(r0 + h * (n // 2), n // 2), :], chunk(a, x, z_hi, h, r0, n), d_zs,
                 rs=4 * inner + k)

    @pl.when(is_outer)
    def _():
        for c in outer_loads:
            pltpu.make_async_copy(*c).wait()

    for c in loads_w:
        c.wait()

    def wchunk(which, yp, h):
        if which == 0:
            return wgu.at[yp, pl.ds(h * C, C), :]
        return wdn.at[yp, pl.ds(h * (F // 2), F // 2), :]

    def ysend(w):
        for h in range(2):
            send(("y", w, 0, h), wchunk(w, y, h), wchunk(w, y, h), d_yr)
            send(("y", w, 1, h), wchunk(w, y, h), wchunk(w, y, h), d_yl)

    def yfwd(w):
        recv(("y", w, 0, 0), wchunk(w, yl, 0))
        send(("yf", w, 0), wchunk(w, yl, 0), wchunk(w, yl, 0), d_yr)
        recv(("y", w, 1, 1), wchunk(w, yr, 1))
        send(("yf", w, 1), wchunk(w, yr, 1), wchunk(w, yr, 1), d_yl)

    def yfin(w):
        recv(("y", w, 0, 1), wchunk(w, yl, 1))
        recv(("y", w, 1, 0), wchunk(w, yr, 0))
        recv(("yf", w, 0), wchunk(w, yf, 0))
        recv(("yf", w, 1), wchunk(w, yf, 1))

    def hsend():
        for h in range(2):
            send(("h", 0, h), home(x, h), home(x, h), d_xr)
            send(("h", 1, h), home(x, h), home(x, h), d_xl)

    def homez(j, xp):
        send(("hz", j), home(xp), xb.at[0, 2 * xp + core, rows(z_hi * R, HOME), :], d_zs, rs=8 + 4 * inner + j)

    def hfwd():
        recv(("h", 0, 0), home(xl, 0))
        send(("hf", 0), home(xl, 0), home(xl, 0), d_xr)
        recv(("h", 1, 1), home(xr, 1))
        send(("hf", 1), home(xr, 1), home(xr, 1), d_xl)

    def hfin():
        homez(0, x)
        recv(("h", 0, 1), home(xl, 1))
        homez(1, xl)
        recv(("h", 1, 0), home(xr, 0))
        homez(2, xr)
        recv(("hf", 0), home(xf, 0))
        recv(("hf", 1), home(xf, 1))
        homez(3, xf)

    xorder = (x, xl, xr, xf)

    def hz(rel):
        t = t_of[rel]
        for j, xp in enumerate(xorder):
            p = part(0, xp, core, t, 0, HOME)
            if rel == 0:
                @pl.when(is_inner)
                def _():
                    recv(("zh", j), p)
            else:
                recv(("zh", 4 + j), p)

                @pl.when(is_inner)
                def _():
                    send(("hzr", j), p, p, d_zlo, rs=12 + j, wait_later=False)
            send(("hs", rel, j), p, p, d_sib)

    def hsfin(rel):
        for j, xp in enumerate(xorder):
            recv(("hs", rel, j), part(0, xp, oc, t_of[rel], 0, HOME))

    def relay(r):
        a, rel, r0, n = ROUNDS[r]
        t = t_of[rel]
        for h in range(2):
            k = 2 * a + h

            @pl.when(is_inner)
            def _():
                c = chunk(a, x, t, h, r0, n)
                recv(("z", 4 + k), c)
                send(("zr", k), c, c, d_zlo, rs=4 + k, wait_later=False)

    def xsend(r):
        a, rel, r0, n = ROUNDS[r]
        t = t_of[rel]
        for h in range(2):
            k = 2 * a + h
            c = chunk(a, x, t, h, r0, n)
            if rel == 0:
                @pl.when(is_inner)
                def _():
                    recv(("z", k), c)
            else:
                @pl.when(is_outer)
                def _():
                    recv(("z", 4 + k), c)
            send(("x", r, 0, h), c, c, d_xr)
            send(("x", r, 1, h), c, c, d_xl)
        p = part(a, x, core, t, r0, n)
        send(("s", r, 0), p, p, d_sib)

    def xfwd(r):
        a, rel, r0, n = ROUNDS[r]
        t = t_of[rel]
        c = chunk(a, xl, t, 0, r0, n)
        recv(("x", r, 0, 0), c)
        send(("xf", r, 0), c, c, d_xr)
        c = chunk(a, xr, t, 1, r0, n)
        recv(("x", r, 1, 1), c)
        send(("xf", r, 1), c, c, d_xl)

    def xfin(r):
        a, rel, r0, n = ROUNDS[r]
        t = t_of[rel]
        recv(("x", r, 0, 1), chunk(a, xl, t, 1, r0, n))
        p = part(a, xl, core, t, r0, n)
        send(("s", r, 1), p, p, d_sib)
        recv(("x", r, 1, 0), chunk(a, xr, t, 0, r0, n))
        p = part(a, xr, core, t, r0, n)
        send(("s", r, 2), p, p, d_sib)
        recv(("xf", r, 0), chunk(a, xf, t, 0, r0, n))
        recv(("xf", r, 1), chunk(a, xf, t, 1, r0, n))
        p = part(a, xf, core, t, r0, n)
        send(("s", r, 3), p, p, d_sib)

    def sfin(r):
        a, rel, r0, n = ROUNDS[r]
        for j, xp in enumerate(xorder):
            recv(("s", r, j), part(a, xp, oc, t_of[rel], r0, n))

    def half(e):
        return pl.ds(pl.multiple_of(lax.rem(e, 2) * C, C), C)

    def forward(r):
        a, rel, r0, n = ROUNDS[r]
        t = t_of[rel]
        out = (pgu, ph)[a].at[rel]
        out[...] = jnp.zeros(out.shape, F32)

        def step(e, carry):
            block = xb[a, e, trow(t), :]
            if a == 0:
                out[...] += dot(block, wgu[e // 2, half(e), :], 1, 0)
            else:
                out[...] += dot(block, wdn[e // 2, :, half(e)], 1, 1)
            return carry

        lax.fori_loop(0, 2 * nx, step, 0)

    hsend()
    ysend(0)
    xsend(0)
    hfwd()
    relay(1)
    xsend(1)
    hfin()
    relay(2)
    yfwd(0)
    ysend(1)
    xfwd(0)
    xsend(2)
    xfin(0)
    xfwd(1)
    xsend(3)
    xfin(1)
    xfwd(2)
    hz(0)
    hz(1)
    yfwd(1)
    yfin(0)
    sfin(0)
    sfin(1)
    xfin(2)
    xfwd(3)
    hsfin(0)
    hsfin(1)
    forward(1)
    send("pgu", pgu.at[1], pgur, d_zhi)
    forward(0)
    yfin(1)
    sfin(2)
    forward(2)
    send("ph", ph.at[1], phr, d_zhi)
    xfin(3)
    sfin(3)
    forward(3)

    recv("pgu", pgur)
    recv("ph", phr)
    gate = pgu[0, :, :F] + pgur[:, :F]
    up = pgu[0, :, F:] + pgur[:, F:]
    hg = ph[0] + phr[...]
    squashed = jax.nn.sigmoid(gate)
    activated = gate * squashed
    slope = squashed * (1.0 + gate * (1.0 - squashed))
    agu[trow(z_hi), :F] = (hg * up * slope).astype(BF)
    agu[trow(z_hi), F:] = (hg * activated).astype(BF)
    ah[trow(z_hi), :] = (activated * up).astype(BF)
    send("agu", agu.at[trow(z_hi), :], agu.at[trow(z_hi), :], d_zhi)
    send("ah", ah.at[trow(z_hi), :], ah.at[trow(z_hi), :], d_zhi)

    order = (xf, xr, xl, x)

    def igstart(rel):
        def step(e, carry):
            igp[rel, e] = dot(agu[trow(t_of[rel]), :], wgu[e // 2, half(e), :], 1, 1)
            return carry

        lax.fori_loop(0, 2 * nx, step, 0)
        for j, xp in enumerate(order):
            send(("is", rel, j), igp.at[rel, 2 * xp + oc], sibr.at[rel, xp], d_sib)

    def addsib(rel, j):
        xp = order[j]
        recv(("is", rel, j), sibr.at[rel, xp])
        igp[rel, 2 * xp + core] += sibr[rel, xp]

    def hrow(h):
        return pl.ds(h * H, H)

    def igfirst(rel):
        addsib(rel, 0)
        for h, d in enumerate((d_xr, d_xl)):
            fs[rel, h] = igp[rel, 2 * xf + core, hrow(h), :].astype(BF)
            send(("if", rel, h), fs.at[rel, h], farr.at[rel, h], d)
        for h, (j, xp, d) in enumerate(((1, xr, d_xr), (2, xl, d_xl))):
            addsib(rel, j)
            send(("in", rel, h, 1 - h), igp.at[rel, 2 * xp + core, hrow(1 - h), :],
                 nearr.at[rel, h, hrow(1 - h), :], d)

    def igsecond(rel):
        for h, (xp, d) in enumerate(((xr, d_xr), (xl, d_xl))):
            recv(("if", rel, h), farr.at[rel, h])
            igp[rel, 2 * xp + core, hrow(h), :] += farr[rel, h].astype(F32)
            send(("in", rel, h, h), igp.at[rel, 2 * xp + core, hrow(h), :], nearr.at[rel, h, hrow(h), :], d)
        addsib(rel, 3)

    def iglast(rel):
        for h in range(2):
            for g in range(2):
                recv(("in", rel, h, g), nearr.at[rel, h, hrow(g), :])
        igp[rel, 2 * x + core] += nearr[rel, 0] + nearr[rel, 1]

    igstart(0)
    igfirst(0)
    recv("agu", agu.at[trow(1 - z_hi), :])
    recv("ah", ah.at[trow(1 - z_hi), :])
    igstart(1)
    igfirst(1)

    def wstep(e, carry):
        g = dot(xb[0, e, : 2 * R], agu[...], 0, 0)
        ws[e] = g
        gb[e] = g.astype(BF)
        d = dot(ah[...], xb[1, e, : 2 * R], 0, 0)
        hs[e] = d
        hb[e] = d.astype(BF)
        return carry

    lax.fori_loop(0, 2 * ny, wstep, 0)
    sides = ((yr, d_yr), (yl, d_yl))
    for h, (yp, d) in enumerate(sides):
        send(("gf", h), gb.at[2 * yf + h], gfr.at[h], d)
        send(("hf", h), hb.at[2 * yf + h], hfr.at[h], d)
    for h, (yp, d) in enumerate(sides):
        send(("gn", h, 1 - h), gb.at[2 * yp + 1 - h], gnr.at[h, 1 - h], d)
        send(("hn", h, 1 - h), hb.at[2 * yp + 1 - h], hnr.at[h, 1 - h], d)

    igsecond(1)
    igsecond(0)

    for h, (yp, d) in enumerate(sides):
        recv(("gf", h), gfr.at[h])
        gb[2 * yp + h] = (ws[2 * yp + h] + gfr[h].astype(F32)).astype(BF)
        send(("gn", h, h), gb.at[2 * yp + h], gnr.at[h, h], d)
        recv(("hf", h), hfr.at[h])
        hb[2 * yp + h] = (hs[2 * yp + h] + hfr[h].astype(F32)).astype(BF)
        send(("hn", h, h), hb.at[2 * yp + h], hnr.at[h, h], d)

    def zsend(rel):
        for h in range(2):
            send(("zi", rel, h), igp.at[rel, 2 * x + core, hrow(h), :], zr.at[hrow(h), :], d_zlo,
                 rs=sid(("zir", h)), wait_later=False)

    iglast(1)

    @pl.when(is_outer)
    def _():
        zsend(1)

    iglast(0)

    @pl.when(is_inner)
    def _():
        zsend(0)

    @pl.when(is_inner)
    def _():
        for h in range(2):
            recv(("zir", h), zr.at[hrow(h), :])
            igs[hrow(h), :] = (igp[1, 2 * x + core, hrow(h), :] + zr[hrow(h), :]).astype(BF)
            send(("zo", h), igs.at[hrow(h), :], igr.at[hrow(h), :], d_zz, wait_later=False)

    for h in range(2):
        for s in range(2):
            recv(("gn", s, h), gnr.at[s, h])
            recv(("hn", s, h), hnr.at[s, h])
        g = (ws[2 * y + h] + gnr[0, h].astype(F32) + gnr[1, h].astype(F32)) * factor
        gg_o[pl.ds(h * C, C), :] = g[:, :F]
        ug_o[pl.ds(h * C, C), :] = g[:, F:]
        dg_o[:, pl.ds(h * C, C)] = (hs[2 * y + h] + hnr[0, h].astype(F32) + hnr[1, h].astype(F32)) * factor

    @pl.when(is_outer)
    def _():
        for h in range(2):
            recv(("zir", h), zr.at[hrow(h), :])
            ig_o[hrow(h), :] = (igp[0, 2 * x + core, hrow(h), :] + zr[hrow(h), :]).astype(BF)

    def wait_send(name, src):
        i = sid(name)
        pltpu.make_async_remote_copy(
            src_ref=src, dst_ref=src, send_sem=ssem.at[i], recv_sem=rsem.at[i],
            device_id=d_sib, device_id_type=MESH).wait_send()

    @pl.when(is_inner)
    def _():
        for h in range(2):
            recv(("zo", h), igr.at[hrow(h), :])
        ig_o[...] = igr[...]
        for h in range(2):
            wait_send(("zo", h), igs.at[hrow(h), :])
            wait_send(("zi", 0, h), zr.at[hrow(h), :])
        for r in (1, 2):
            a, rel, r0, n = ROUNDS[r]
            for h in range(2):
                wait_send(("zr", 2 * a + h), chunk(a, x, t_of[1], h, r0, n))
        for j, xp in enumerate(xorder):
            wait_send(("hzr", j), part(0, xp, core, t_of[1], 0, HOME))

    @pl.when(is_outer)
    def _():
        for h in range(2):
            wait_send(("zi", 1, h), zr.at[hrow(h), :])

    for c in pending:
        c.wait_send()
    assert len(ids) <= NSEM


def shards(tokens, out_grad, gate_weight, up_weight, down_weight):
    R, C = tokens.shape
    F = gate_weight.shape[1]
    H = R // 2
    factor = 1.0 / math.sqrt(R * lax.axis_size(FSDP))
    anyspec = pl.BlockSpec(memory_space=pl.ANY)
    vm = pl.BlockSpec(memory_space=pltpu.VMEM)
    V = pltpu.VMEM
    scratch = [
        V((2, R, C), BF), V((2, 8, 2 * R + HOME, C), BF), V((4, 2 * C, 2 * F), BF), V((4, F, 2 * C), BF),
        V((2, R, 2 * F), F32), V((2, R, F), F32), V((R, 2 * F), F32), V((R, F), F32),
        V((2 * R, 2 * F), BF), V((2 * R, F), BF),
        V((2, 8, R, C), F32), V((2, 4, R, C), F32), V((2, 2, H, C), BF), V((2, 2, R, C), F32), V((2, 2, H, C), BF),
        V((R, C), F32), V((R, C), BF), V((R, C), BF),
        V((8, C, 2 * F), F32), V((8, F, C), F32), V((8, C, 2 * F), BF), V((8, F, C), BF),
        V((2, C, 2 * F), BF), V((2, F, C), BF), V((2, 2, C, 2 * F), BF), V((2, 2, F, C), BF),
        pltpu.SemaphoreType.DMA((8,)), pltpu.SemaphoreType.DMA((NSEM,)), pltpu.SemaphoreType.DMA((NSEM,)),
    ]
    return pl.pallas_call(
        functools.partial(kernel, factor),
        out_shape=(
            jax.ShapeDtypeStruct((R, C), BF),
            jax.ShapeDtypeStruct((2 * C, F), F32),
            jax.ShapeDtypeStruct((2 * C, F), F32),
            jax.ShapeDtypeStruct((F, 2 * C), F32),
        ),
        in_specs=[anyspec] * 5,
        out_specs=(vm,) * 4,
        scratch_shapes=scratch,
        compiler_params=pltpu.CompilerParams(
            collective_id=0, has_side_effects=True, vmem_limit_bytes=60 * 1024 * 1024),
        name="ffn_backward",
    )(tokens, out_grad, gate_weight, up_weight, down_weight)


def solution(mesh):
    finer = Mesh(mesh.devices.reshape(2, 4, 2, 4, 2), ("z_hi", "y", "z_lo", "x", "core"))
    return jax.shard_map(
        shards,
        mesh=finer,
        in_specs=(P(FSDP, TP), P(FSDP, TP), P(FSDP, TP), P(FSDP, TP), P(TP, FSDP)),
        out_specs=(P(FSDP, TP), P(FSDP, TP), P(FSDP, TP), P(TP, FSDP)),
        check_vma=False,
    )
```

```python
import functools
import math

import jax
import jax.numpy as jnp
from jax import lax
from jax.experimental import pallas as pl
from jax.experimental.pallas import tpu as pltpu
from jax.sharding import Mesh
from jax.sharding import PartitionSpec as P

FSDP = ("z_hi", "y")
TP = ("z_lo", "x", "core")
MESH = pl.DeviceIdType.MESH
BF = jnp.bfloat16
F32 = jnp.float32
NSEM = 224
ZF = 64
HOME = 128
ROUNDS = ((0, 0, HOME, 256 - HOME), (0, 1, HOME, 256 - HOME), (1, 1, 0, 256), (1, 0, 0, 256))


def dot(a, b, ca, cb):
    return lax.dot_general(a, b, (((ca,), (cb,)), ((), ())), preferred_element_type=F32)


def kernel(factor, tok, og, wg, wu, wd, ig_o, gg_o, ug_o, dg_o,
           own, xb, wgu, wdn, pgu, ph, pgur, phr, agu, ah, igp, sibr, farr, nearr, fs, zfr, zr, igs, igr,
           ws, hs, gb, hb, gfr, hfr, gnr, hnr, lsem, ssem, rsem):
    R, C = tok.shape
    F = wg.shape[1]
    H = R // 2
    z_hi, y, z_lo, x, core = (lax.axis_index(a) for a in ("z_hi", "y", "z_lo", "x", "core"))
    inner = (z_hi - z_lo) * (z_hi - z_lo)
    is_inner, is_outer = inner == 1, inner == 0
    nx, ny = 4, 4
    xr, xl, xf = lax.rem(x + 1, nx), lax.rem(x + nx - 1, nx), lax.rem(x + 2, nx)
    yr, yl, yf = lax.rem(y + 1, ny), lax.rem(y + ny - 1, ny), lax.rem(y + 2, ny)
    oc = 1 - core
    t_of = (z_hi, 1 - z_hi)
    d_xr, d_xl = (z_hi, y, z_lo, xr, core), (z_hi, y, z_lo, xl, core)
    d_yr, d_yl = (z_hi, yr, z_lo, x, core), (z_hi, yl, z_lo, x, core)
    d_sib = (z_hi, y, z_lo, x, oc)
    d_zlo = (z_hi, y, 1 - z_lo, x, core)
    d_zhi = (1 - z_hi, y, z_lo, x, core)
    d_zz = (1 - z_hi, y, 1 - z_lo, x, core)
    d_zs = (z_lo, y, 1 - z_lo, x, core)
    partners = (d_xr, d_xl, d_yr, d_yl, d_sib, d_zlo, d_zhi, d_zz)

    ids = {}

    def sid(name):
        return ids.setdefault(name, len(ids))

    for k in range(8):
        sid(("z", k))
    for k in range(8):
        sid(("zh", k))
    pending = []

    def send(name, src, dst, dev, rs=None, wait_later=True):
        i = sid(name)
        c = pltpu.make_async_remote_copy(
            src_ref=src, dst_ref=dst, send_sem=ssem.at[i], recv_sem=rsem.at[i if rs is None else rs],
            device_id=dev, device_id_type=MESH)
        c.start()
        if wait_later:
            pending.append(c)
        return c

    def recv(name, dst):
        i = sid(name)
        pltpu.make_async_remote_copy(
            src_ref=dst, dst_ref=dst, send_sem=ssem.at[i], recv_sem=rsem.at[i],
            device_id=d_sib, device_id_type=MESH).wait_recv()

    def trow(t):
        return pl.ds(pl.multiple_of(t * R, R), R)

    def blk(a, xp, c, t):
        return xb.at[a, 2 * xp + c, trow(t), :]

    def rows(start, n):
        return pl.ds(pl.multiple_of(start, 16), n)

    def chunk(a, xp, t, h, r0, n):
        return xb.at[a, 2 * xp + core, rows(t * R + r0 + h * (n // 2), n // 2), :]

    def part(a, xp, c, t, r0, n):
        return xb.at[a, 2 * xp + c, rows(t * R + r0, n), :]

    home_at = (1 - inner) * z_hi * R + inner * 2 * R

    def home(xp, h=None):
        if h is None:
            return xb.at[0, 2 * xp + core, rows(home_at, HOME), :]
        return xb.at[0, 2 * xp + core, rows(home_at + h * (HOME // 2), HOME // 2), :]

    loads_w = [
        pltpu.make_async_copy(wg, wgu.at[y, :, pl.ds(0, F)], lsem.at[0]),
        pltpu.make_async_copy(wu, wgu.at[y, :, pl.ds(F, F)], lsem.at[1]),
        pltpu.make_async_copy(wd, wdn.at[y], lsem.at[2]),
    ]
    loads_t = [
        pltpu.make_async_copy(tok, own.at[0], lsem.at[3]),
        pltpu.make_async_copy(og, own.at[1], lsem.at[4]),
    ]
    for c in loads_t + loads_w:
        c.start()

    outer_loads = (
        (tok.at[pl.ds(HOME, R - HOME), :], part(0, x, core, z_hi, HOME, R - HOME), lsem.at[5]),
        (og, blk(1, x, core, z_hi), lsem.at[6]),
    )
    load_home = pltpu.make_async_copy(tok.at[pl.ds(0, HOME), :], home(x), lsem.at[7])
    load_home.start()

    @pl.when(is_outer)
    def _():
        for c in outer_loads:
            pltpu.make_async_copy(*c).start()

    barrier = pltpu.get_barrier_semaphore()
    for d in partners:
        pl.semaphore_signal(barrier, inc=1, device_id=d, device_id_type=MESH)
    pl.semaphore_wait(barrier, len(partners))

    for c in loads_t:
        c.wait()
    load_home.wait()

    for a, rel, r0, n in (ROUNDS[0], ROUNDS[3]):
        for h in range(2):
            k = 2 * a + h
            send(("zs", k), own.at[a, pl.ds(r0 + h * (n // 2), n // 2), :], chunk(a, x, z_hi, h, r0, n), d_zs,
                 rs=4 * inner + k)

    @pl.when(is_outer)
    def _():
        for c in outer_loads:
            pltpu.make_async_copy(*c).wait()

    for c in loads_w:
        c.wait()

    def wchunk(which, yp, h):
        if which == 0:
            return wgu.at[yp, pl.ds(h * C, C), :]
        return wdn.at[yp, pl.ds(h * (F // 2), F // 2), :]

    def ysend(w):
        for h in range(2):
            send(("y", w, 0, h), wchunk(w, y, h), wchunk(w, y, h), d_yr)
            send(("y", w, 1, 1 - h), wchunk(w, y, 1 - h), wchunk(w, y, 1 - h), d_yl)

    def yfwd(w):
        recv(("y", w, 0, 0), wchunk(w, yl, 0))
        send(("yf", w, 0), wchunk(w, yl, 0), wchunk(w, yl, 0), d_yr)
        recv(("y", w, 1, 1), wchunk(w, yr, 1))
        send(("yf", w, 1), wchunk(w, yr, 1), wchunk(w, yr, 1), d_yl)

    def yfin(w):
        recv(("y", w, 0, 1), wchunk(w, yl, 1))
        recv(("y", w, 1, 0), wchunk(w, yr, 0))
        recv(("yf", w, 0), wchunk(w, yf, 0))
        recv(("yf", w, 1), wchunk(w, yf, 1))

    def hsend():
        for h in range(2):
            send(("h", 0, h), home(x, h), home(x, h), d_xr)
            send(("h", 1, 1 - h), home(x, 1 - h), home(x, 1 - h), d_xl)

    def homez(j, xp):
        send(("hz", j), home(xp), xb.at[0, 2 * xp + core, rows(z_hi * R, HOME), :], d_zs, rs=8 + 4 * inner + j)

    def hfwd():
        recv(("h", 0, 0), home(xl, 0))
        send(("hf", 0), home(xl, 0), home(xl, 0), d_xr)
        recv(("h", 1, 1), home(xr, 1))
        send(("hf", 1), home(xr, 1), home(xr, 1), d_xl)

    def hfin():
        homez(0, x)
        recv(("h", 0, 1), home(xl, 1))
        homez(1, xl)
        recv(("h", 1, 0), home(xr, 0))
        homez(2, xr)
        recv(("hf", 0), home(xf, 0))
        recv(("hf", 1), home(xf, 1))
        homez(3, xf)

    xorder = (x, xl, xr, xf)

    def hpart(rel, j):
        return part(0, xorder[j], core, t_of[rel], 0, HOME)

    def hsib(rel, j):
        send(("hs", rel, j), hpart(rel, j), hpart(rel, j), d_sib, wait_later=False)

    def hz_inner(j):
        @pl.when(is_inner)
        def _():
            recv(("zh", 4 + j), hpart(1, j))
            send(("hzr", j), hpart(1, j), hpart(1, j), d_zlo, rs=12 + j, wait_later=False)
            hsib(1, j)
            recv(("zh", j), hpart(0, j))
            hsib(0, j)

    def hz_outer(j):
        @pl.when(is_outer)
        def _():
            recv(("zh", 4 + j), hpart(1, j))
            hsib(1, j)

    def hs_outer():
        @pl.when(is_outer)
        def _():
            for j in range(4):
                hsib(0, j)

    def hsfin(rel):
        for j, xp in enumerate(xorder):
            recv(("hs", rel, j), part(0, xp, oc, t_of[rel], 0, HOME))

    def relay(r, hs=(0, 1)):
        a, rel, r0, n = ROUNDS[r]
        t = t_of[rel]
        for h in hs:
            k = 2 * a + h

            @pl.when(is_inner)
            def _():
                c = chunk(a, x, t, h, r0, n)
                recv(("z", 4 + k), c)
                send(("zr", k), c, c, d_zlo, rs=4 + k, wait_later=False)

    def xsend(r):
        a, rel, r0, n = ROUNDS[r]
        t = t_of[rel]
        for h in range(2):
            k = 2 * a + h
            c = chunk(a, x, t, h, r0, n)
            if rel == 0:
                @pl.when(is_inner)
                def _():
                    recv(("z", k), c)
            else:
                @pl.when(is_outer)
                def _():
                    recv(("z", 4 + k), c)
            if h == 0:
                send(("x", r, 0, 0), c, c, d_xr)
            else:
                send(("x", r, 1, 1), c, c, d_xl)
                send(("x", r, 0, 1), c, c, d_xr)
                c = chunk(a, x, t, 0, r0, n)
                send(("x", r, 1, 0), c, c, d_xl)
        p = part(a, x, core, t, r0, n)
        send(("s", r, 0), p, p, d_sib)

    def xfwd(r):
        a, rel, r0, n = ROUNDS[r]
        t = t_of[rel]
        c = chunk(a, xl, t, 0, r0, n)
        recv(("x", r, 0, 0), c)
        send(("xf", r, 0), c, c, d_xr)
        c = chunk(a, xr, t, 1, r0, n)
        recv(("x", r, 1, 1), c)
        send(("xf", r, 1), c, c, d_xl)

    def xfin(r):
        a, rel, r0, n = ROUNDS[r]
        t = t_of[rel]
        recv(("x", r, 0, 1), chunk(a, xl, t, 1, r0, n))
        p = part(a, xl, core, t, r0, n)
        send(("s", r, 1), p, p, d_sib)
        recv(("x", r, 1, 0), chunk(a, xr, t, 0, r0, n))
        p = part(a, xr, core, t, r0, n)
        send(("s", r, 2), p, p, d_sib)
        recv(("xf", r, 0), chunk(a, xf, t, 0, r0, n))
        recv(("xf", r, 1), chunk(a, xf, t, 1, r0, n))
        p = part(a, xf, core, t, r0, n)
        send(("s", r, 3), p, p, d_sib)

    def sfin(r):
        a, rel, r0, n = ROUNDS[r]
        for j, xp in enumerate(xorder):
            recv(("s", r, j), part(a, xp, oc, t_of[rel], r0, n))

    def half(e):
        return pl.ds(pl.multiple_of(lax.rem(e, 2) * C, C), C)

    def forward(r):
        a, rel, r0, n = ROUNDS[r]
        t = t_of[rel]
        out = (pgu, ph)[a].at[rel]
        out[...] = jnp.zeros(out.shape, F32)

        def step(e, carry):
            block = xb[a, e, trow(t), :]
            if a == 0:
                out[...] += dot(block, wgu[e // 2, half(e), :], 1, 0)
            else:
                out[...] += dot(block, wdn[e // 2, :, half(e)], 1, 1)
            return carry

        lax.fori_loop(0, 2 * nx, step, 0)

    hsend()
    ysend(0)
    xsend(0)
    hfwd()
    relay(1)
    xsend(1)
    hfin()
    hs_outer()
    relay(2, (0,))
    yfwd(0)
    ysend(1)
    xfwd(0)
    relay(2, (1,))
    xsend(2)
    hz_inner(0)
    xfwd(1)
    xsend(3)
    xfin(0)
    hz_inner(1)
    xfin(1)
    hz_inner(2)
    xfwd(2)
    hz_inner(3)
    yfwd(1)
    xfwd(3)
    yfin(0)
    sfin(0)
    sfin(1)
    for j in range(4):
        hz_outer(j)
    hsfin(0)
    hsfin(1)
    forward(1)
    send("pgu", pgu.at[1], pgur, d_zhi)
    forward(0)
    yfin(1)
    xfin(2)
    sfin(2)
    forward(2)
    send("ph", ph.at[1], phr, d_zhi)
    xfin(3)
    sfin(3)
    forward(3)

    recv("pgu", pgur)
    recv("ph", phr)
    gate = pgu[0, :, :F] + pgur[:, :F]
    up = pgu[0, :, F:] + pgur[:, F:]
    hg = ph[0] + phr[...]
    squashed = jax.nn.sigmoid(gate)
    activated = gate * squashed
    slope = squashed * (1.0 + gate * (1.0 - squashed))
    agu[trow(z_hi), :F] = (hg * up * slope).astype(BF)
    agu[trow(z_hi), F:] = (hg * activated).astype(BF)
    ah[trow(z_hi), :] = (activated * up).astype(BF)
    send("agu", agu.at[trow(z_hi), :], agu.at[trow(z_hi), :], d_zhi)
    send("ah", ah.at[trow(z_hi), :], ah.at[trow(z_hi), :], d_zhi)

    order = (xf, xr, xl, x)
    RA = ((ZF, R - ZF), (0, ZF))

    def hrows(p, h):
        r0, n = RA[p]
        return pl.ds(r0 + h * (n // 2), n // 2)

    def arows(p):
        return pl.ds(*RA[p])

    def igblock(rel, xp, c):
        w = wgu[xp, pl.ds(pl.multiple_of(c * C, C), C), :]
        igp[rel, 2 * xp + c] = dot(agu[trow(t_of[rel]), :], w, 1, 1)

    def igstart(rel):
        for j, xp in enumerate(order):
            igblock(rel, xp, oc)
            send(("is", rel, j), igp.at[rel, 2 * xp + oc], sibr.at[rel, xp], d_sib)
        for xp in order:
            igblock(rel, xp, core)

    def addsib(rel, j):
        xp = order[j]
        recv(("is", rel, j), sibr.at[rel, xp])
        igp[rel, 2 * xp + core] += sibr[rel, xp]

    def zfirst(rel, j):
        xp = order[j]
        send(("zf", j), igp.at[rel, 2 * xp + core, arows(1), :], zfr.at[xp], d_zlo, wait_later=False)

    def igfar(p, rel, k):
        for h, d in enumerate((d_xr, d_xl)):
            fs[k, h, pl.ds(0, RA[p][1] // 2), :] = igp[rel, 2 * xf + core, hrows(p, h), :].astype(BF)
            n = pl.ds(0, RA[p][1] // 2)
            send(("if", k, h), fs.at[k, h, n, :], farr.at[k, h, n, :], d)

    def ignear(p, rel, k):
        for h, (xp, d) in enumerate(((xr, d_xr), (xl, d_xl))):
            send(("in", k, h, 1 - h), igp.at[rel, 2 * xp + core, hrows(p, 1 - h), :],
                 nearr.at[rel, h, hrows(p, 1 - h), :], d)

    def igsecond(p, rel, k):
        for h, (xp, d) in enumerate(((xr, d_xr), (xl, d_xl))):
            n = pl.ds(0, RA[p][1] // 2)
            recv(("if", k, h), farr.at[k, h, n, :])
            igp[rel, 2 * xp + core, hrows(p, h), :] += farr[k, h, n, :].astype(F32)
            send(("in", k, h, h), igp.at[rel, 2 * xp + core, hrows(p, h), :], nearr.at[rel, h, hrows(p, h), :], d)

    def iglast(p, rel, k):
        for h in range(2):
            for g in range(2):
                recv(("in", k, h, g), nearr.at[rel, h, hrows(p, g), :])
        igp[rel, 2 * x + core, arows(p), :] += nearr[rel, 0, arows(p), :] + nearr[rel, 1, arows(p), :]

    def igfirst(rel, when):
        addsib(rel, 0)
        igfar(0, rel, rel)
        addsib(rel, 1)
        addsib(rel, 2)
        ignear(0, rel, rel)
        addsib(rel, 3)

        @pl.when(when)
        def _():
            for j in range(4):
                zfirst(rel, j)

    igstart(0)
    igfirst(0, is_inner)
    recv("agu", agu.at[trow(1 - z_hi), :])
    recv("ah", ah.at[trow(1 - z_hi), :])
    igstart(1)
    igfirst(1, is_outer)

    def wstep(e, carry):
        g = dot(xb[0, e, : 2 * R], agu[...], 0, 0)
        ws[e] = g
        gb[e] = g.astype(BF)
        d = dot(ah[...], xb[1, e, : 2 * R], 0, 0)
        hs[e] = d
        hb[e] = d.astype(BF)
        return carry

    lax.fori_loop(0, 2 * ny, wstep, 0)
    sides = ((yr, d_yr), (yl, d_yl))
    for h, (yp, d) in enumerate(sides):
        send(("gf", h), gb.at[2 * yf + h], gfr.at[h], d)
        send(("hf", h), hb.at[2 * yf + h], hfr.at[h], d)
    for h, (yp, d) in enumerate(sides):
        send(("gn", h, 1 - h), gb.at[2 * yp + 1 - h], gnr.at[h, 1 - h], d)
        send(("hn", h, 1 - h), hb.at[2 * yp + 1 - h], hnr.at[h, 1 - h], d)

    igsecond(0, 1, 1)
    igsecond(0, 0, 0)
    keep = inner
    for j in (0, 1, 2, 3):
        xp = order[j]
        recv(("zf", j), zfr.at[xp])
        igp[keep, 2 * xp + core, arows(1), :] += zfr[xp]
        if j == 0:
            igfar(1, keep, 2)
    ignear(1, keep, 2)

    for h, (yp, d) in enumerate(sides):
        recv(("gf", h), gfr.at[h])
        gb[2 * yp + h] = (ws[2 * yp + h] + gfr[h].astype(F32)).astype(BF)
        send(("gn", h, h), gb.at[2 * yp + h], gnr.at[h, h], d)
        recv(("hf", h), hfr.at[h])
        hb[2 * yp + h] = (hs[2 * yp + h] + hfr[h].astype(F32)).astype(BF)
        send(("hn", h, h), hb.at[2 * yp + h], hnr.at[h, h], d)

    def zsend(rel):
        for h in range(2):
            send(("zi", rel, h), igp.at[rel, 2 * x + core, hrows(0, h), :], zr.at[hrows(0, h), :], d_zlo,
                 rs=sid(("zir", h)), wait_later=False)

    iglast(0, 1, 1)

    @pl.when(is_outer)
    def _():
        zsend(1)

    igsecond(1, keep, 2)
    iglast(0, 0, 0)

    @pl.when(is_inner)
    def _():
        zsend(0)

    iglast(1, keep, 2)

    @pl.when(is_inner)
    def _():
        igs[2, pl.ds(0, ZF), :] = igp[1, 2 * x + core, arows(1), :].astype(BF)
        send(("zo", 2), igs.at[2, pl.ds(0, ZF), :], igr.at[2, pl.ds(0, ZF), :], d_zz, wait_later=False)
        n = pl.ds(0, (R - ZF) // 2)
        for h in range(2):
            recv(("zir", h), zr.at[hrows(0, h), :])
            igs[h, n, :] = (igp[1, 2 * x + core, hrows(0, h), :] + zr[hrows(0, h), :]).astype(BF)
            send(("zo", h), igs.at[h, n, :], igr.at[h, n, :], d_zz, wait_later=False)

    @pl.when(is_outer)
    def _():
        ig_o[arows(1), :] = igp[0, 2 * x + core, arows(1), :].astype(BF)

    for h in range(2):
        for s in range(2):
            recv(("gn", s, h), gnr.at[s, h])
            recv(("hn", s, h), hnr.at[s, h])
        g = (ws[2 * y + h] + gnr[0, h].astype(F32) + gnr[1, h].astype(F32)) * factor
        gg_o[pl.ds(h * C, C), :] = g[:, :F]
        ug_o[pl.ds(h * C, C), :] = g[:, F:]
        dg_o[:, pl.ds(h * C, C)] = (hs[2 * y + h] + hnr[0, h].astype(F32) + hnr[1, h].astype(F32)) * factor

    @pl.when(is_outer)
    def _():
        for h in range(2):
            recv(("zir", h), zr.at[hrows(0, h), :])
            ig_o[hrows(0, h), :] = (igp[0, 2 * x + core, hrows(0, h), :] + zr[hrows(0, h), :]).astype(BF)

    def wait_send(name, src):
        i = sid(name)
        pltpu.make_async_remote_copy(
            src_ref=src, dst_ref=src, send_sem=ssem.at[i], recv_sem=rsem.at[i],
            device_id=d_sib, device_id_type=MESH).wait_send()

    @pl.when(is_inner)
    def _():
        zs, n = pl.ds(0, ZF), pl.ds(0, (R - ZF) // 2)
        recv(("zo", 2), igr.at[2, zs, :])
        ig_o[arows(1), :] = igr[2, zs, :]
        for h in range(2):
            recv(("zo", h), igr.at[h, n, :])
            ig_o[hrows(0, h), :] = igr[h, n, :]
        wait_send(("zo", 2), igs.at[2, zs, :])
        for h in range(2):
            wait_send(("zo", h), igs.at[h, n, :])
            wait_send(("zi", 0, h), zr.at[hrows(0, h), :])
        for r in (1, 2):
            a, rel, r0, n = ROUNDS[r]
            for h in range(2):
                wait_send(("zr", 2 * a + h), chunk(a, x, t_of[1], h, r0, n))
        for j in range(4):
            wait_send(("hzr", j), hpart(1, j))

    @pl.when(is_outer)
    def _():
        for h in range(2):
            wait_send(("zi", 1, h), zr.at[hrows(0, h), :])

    for j in range(4):
        wait_send(("zf", j), zfr.at[j])
        for rel in range(2):
            wait_send(("hs", rel, j), hpart(rel, j))
    for c in pending:
        c.wait_send()
    assert len(ids) <= NSEM


def shards(tokens, out_grad, gate_weight, up_weight, down_weight):
    R, C = tokens.shape
    F = gate_weight.shape[1]
    H = R // 2
    factor = 1.0 / math.sqrt(R * lax.axis_size(FSDP))
    anyspec = pl.BlockSpec(memory_space=pl.ANY)
    vm = pl.BlockSpec(memory_space=pltpu.VMEM)
    V = pltpu.VMEM
    scratch = [
        V((2, R, C), BF), V((2, 8, 2 * R + HOME, C), BF), V((4, 2 * C, 2 * F), BF), V((4, F, 2 * C), BF),
        V((2, R, 2 * F), F32), V((2, R, F), F32), V((R, 2 * F), F32), V((R, F), F32),
        V((2 * R, 2 * F), BF), V((2 * R, F), BF),
        V((2, 8, R, C), F32), V((2, 4, R, C), F32), V((3, 2, H, C), BF), V((2, 2, R, C), F32), V((3, 2, H, C), BF), V((4, ZF, C), F32),
        V((R, C), F32), V((3, H, C), BF), V((3, H, C), BF),
        V((8, C, 2 * F), F32), V((8, F, C), F32), V((8, C, 2 * F), BF), V((8, F, C), BF),
        V((2, C, 2 * F), BF), V((2, F, C), BF), V((2, 2, C, 2 * F), BF), V((2, 2, F, C), BF),
        pltpu.SemaphoreType.DMA((8,)), pltpu.SemaphoreType.DMA((NSEM,)), pltpu.SemaphoreType.DMA((NSEM,)),
    ]
    return pl.pallas_call(
        functools.partial(kernel, factor),
        out_shape=(
            jax.ShapeDtypeStruct((R, C), BF),
            jax.ShapeDtypeStruct((2 * C, F), F32),
            jax.ShapeDtypeStruct((2 * C, F), F32),
            jax.ShapeDtypeStruct((F, 2 * C), F32),
        ),
        in_specs=[anyspec] * 5,
        out_specs=(vm,) * 4,
        scratch_shapes=scratch,
        compiler_params=pltpu.CompilerParams(
            collective_id=0, has_side_effects=True, vmem_limit_bytes=60 * 1024 * 1024),
        name="ffn_backward",
    )(tokens, out_grad, gate_weight, up_weight, down_weight)


def solution(mesh):
    finer = Mesh(mesh.devices.reshape(2, 4, 2, 4, 2), ("z_hi", "y", "z_lo", "x", "core"))
    return jax.shard_map(
        shards,
        mesh=finer,
        in_specs=(P(FSDP, TP), P(FSDP, TP), P(FSDP, TP), P(FSDP, TP), P(TP, FSDP)),
        out_specs=(P(FSDP, TP), P(FSDP, TP), P(FSDP, TP), P(TP, FSDP)),
        check_vma=False,
    )
```

```python
import functools
import math

import jax
import jax.numpy as jnp
from jax import lax
from jax.experimental import pallas as pl
from jax.experimental.pallas import tpu as pltpu
from jax.sharding import Mesh
from jax.sharding import PartitionSpec as P

FSDP = ("z_hi", "y")
TP = ("z_lo", "x", "core")
MESH = pl.DeviceIdType.MESH
BF = jnp.bfloat16
F32 = jnp.float32
NSEM = 224
ZF = 64
HOME = 160
ROUNDS = ((0, 0, 0, 256), (0, 1, 0, 256), (1, 0, HOME, 256 - HOME), (1, 1, HOME, 256 - HOME))


def dot(a, b, ca, cb):
    return lax.dot_general(a, b, (((ca,), (cb,)), ((), ())), preferred_element_type=F32)


def kernel(factor, tok, og, wg, wu, wd, ig_o, gg_o, ug_o, dg_o,
           own, xb, wgu, wdn, pgu, ph, pgur, phr, agu, ah, igp, sibr, farr, nearr, fs, zfr, zr, igs, igr,
           ws, hs, gb, hb, gfr, hfr, gnr, hnr, lsem, ssem, rsem):
    R, C = tok.shape
    F = wg.shape[1]
    H = R // 2
    z_hi, y, z_lo, x, core = (lax.axis_index(a) for a in ("z_hi", "y", "z_lo", "x", "core"))
    inner = (z_hi - z_lo) * (z_hi - z_lo)
    is_inner, is_outer = inner == 1, inner == 0
    nx, ny = 4, 4
    xr, xl, xf = lax.rem(x + 1, nx), lax.rem(x + nx - 1, nx), lax.rem(x + 2, nx)
    yr, yl, yf = lax.rem(y + 1, ny), lax.rem(y + ny - 1, ny), lax.rem(y + 2, ny)
    oc = 1 - core
    t_of = (z_hi, 1 - z_hi)
    d_xr, d_xl = (z_hi, y, z_lo, xr, core), (z_hi, y, z_lo, xl, core)
    d_yr, d_yl = (z_hi, yr, z_lo, x, core), (z_hi, yl, z_lo, x, core)
    d_sib = (z_hi, y, z_lo, x, oc)
    d_zlo = (z_hi, y, 1 - z_lo, x, core)
    d_zhi = (1 - z_hi, y, z_lo, x, core)
    d_zz = (1 - z_hi, y, 1 - z_lo, x, core)
    d_zs = (z_lo, y, 1 - z_lo, x, core)
    partners = (d_xr, d_xl, d_yr, d_yl, d_sib, d_zlo, d_zhi, d_zz)

    ids = {}

    def sid(name):
        return ids.setdefault(name, len(ids))

    for k in range(8):
        sid(("z", k))
    for k in range(8):
        sid(("zh", k))
    pending = []

    def send(name, src, dst, dev, rs=None, wait_later=True):
        i = sid(name)
        c = pltpu.make_async_remote_copy(
            src_ref=src, dst_ref=dst, send_sem=ssem.at[i], recv_sem=rsem.at[i if rs is None else rs],
            device_id=dev, device_id_type=MESH)
        c.start()
        if wait_later:
            pending.append(c)
        return c

    def recv(name, dst):
        i = sid(name)
        pltpu.make_async_remote_copy(
            src_ref=dst, dst_ref=dst, send_sem=ssem.at[i], recv_sem=rsem.at[i],
            device_id=d_sib, device_id_type=MESH).wait_recv()

    def trow(t):
        return pl.ds(pl.multiple_of(t * R, R), R)

    def blk(a, xp, c, t):
        return xb.at[a, 2 * xp + c, trow(t), :]

    def rows(start, n):
        return pl.ds(pl.multiple_of(start, 16), n)

    def chunk(a, xp, t, h, r0, n):
        return xb.at[a, 2 * xp + core, rows(t * R + r0 + h * (n // 2), n // 2), :]

    def part(a, xp, c, t, r0, n):
        return xb.at[a, 2 * xp + c, rows(t * R + r0, n), :]

    home_at = (1 - inner) * z_hi * R + inner * 2 * R

    def home(xp, h=None):
        if h is None:
            return xb.at[1, 2 * xp + core, rows(home_at, HOME), :]
        return xb.at[1, 2 * xp + core, rows(home_at + h * (HOME // 2), HOME // 2), :]

    loads_w = [
        pltpu.make_async_copy(wg, wgu.at[y, :, pl.ds(0, F)], lsem.at[0]),
        pltpu.make_async_copy(wu, wgu.at[y, :, pl.ds(F, F)], lsem.at[1]),
        pltpu.make_async_copy(wd, wdn.at[y], lsem.at[2]),
    ]
    loads_t = [
        pltpu.make_async_copy(tok, own.at[0], lsem.at[3]),
        pltpu.make_async_copy(og, own.at[1], lsem.at[4]),
    ]
    for c in loads_t + loads_w:
        c.start()

    outer_loads = (
        (tok, blk(0, x, core, z_hi), lsem.at[5]),
        (og.at[pl.ds(HOME, R - HOME), :], part(1, x, core, z_hi, HOME, R - HOME), lsem.at[6]),
    )
    load_home = pltpu.make_async_copy(og.at[pl.ds(0, HOME), :], home(x), lsem.at[7])
    load_home.start()

    @pl.when(is_outer)
    def _():
        for c in outer_loads:
            pltpu.make_async_copy(*c).start()

    barrier = pltpu.get_barrier_semaphore()
    for d in partners:
        pl.semaphore_signal(barrier, inc=1, device_id=d, device_id_type=MESH)
    pl.semaphore_wait(barrier, len(partners))

    for c in loads_t:
        c.wait()
    load_home.wait()

    for a, rel, r0, n in (ROUNDS[0], ROUNDS[2]):
        for h in range(2):
            k = 2 * a + h
            send(("zs", k), own.at[a, pl.ds(r0 + h * (n // 2), n // 2), :], chunk(a, x, z_hi, h, r0, n), d_zs,
                 rs=4 * inner + k)

    @pl.when(is_outer)
    def _():
        for c in outer_loads:
            pltpu.make_async_copy(*c).wait()

    for c in loads_w:
        c.wait()

    def wchunk(which, yp, h):
        if which == 0:
            return wgu.at[yp, pl.ds(h * C, C), :]
        return wdn.at[yp, pl.ds(h * (F // 2), F // 2), :]

    def ysend(w):
        for h in range(2):
            send(("y", w, 0, h), wchunk(w, y, h), wchunk(w, y, h), d_yr)
            send(("y", w, 1, 1 - h), wchunk(w, y, 1 - h), wchunk(w, y, 1 - h), d_yl)

    def yfwd(w):
        recv(("y", w, 0, 0), wchunk(w, yl, 0))
        send(("yf", w, 0), wchunk(w, yl, 0), wchunk(w, yl, 0), d_yr)
        recv(("y", w, 1, 1), wchunk(w, yr, 1))
        send(("yf", w, 1), wchunk(w, yr, 1), wchunk(w, yr, 1), d_yl)

    def yfin(w):
        recv(("y", w, 0, 1), wchunk(w, yl, 1))
        recv(("y", w, 1, 0), wchunk(w, yr, 0))
        recv(("yf", w, 0), wchunk(w, yf, 0))
        recv(("yf", w, 1), wchunk(w, yf, 1))

    def hsend():
        for h in range(2):
            send(("h", 0, h), home(x, h), home(x, h), d_xr)
            send(("h", 1, 1 - h), home(x, 1 - h), home(x, 1 - h), d_xl)

    def homez(j, xp):
        send(("hz", j), home(xp), xb.at[1, 2 * xp + core, rows(z_hi * R, HOME), :], d_zs, rs=8 + 4 * inner + j)

    def hfwd():
        recv(("h", 0, 0), home(xl, 0))
        send(("hf", 0), home(xl, 0), home(xl, 0), d_xr)
        recv(("h", 1, 1), home(xr, 1))
        send(("hf", 1), home(xr, 1), home(xr, 1), d_xl)

    def hfin_a():
        homez(0, x)
        recv(("h", 0, 1), home(xl, 1))
        homez(1, xl)
        recv(("h", 1, 0), home(xr, 0))
        homez(2, xr)

    def hfin_b():
        recv(("hf", 0), home(xf, 0))
        recv(("hf", 1), home(xf, 1))
        homez(3, xf)

    xorder = (x, xl, xr, xf)

    def hpart(rel, j):
        return part(1, xorder[j], core, t_of[rel], 0, HOME)

    def hsib(rel, j):
        send(("hs", rel, j), hpart(rel, j), hpart(rel, j), d_sib, wait_later=False)

    def hz_inner(j):
        @pl.when(is_inner)
        def _():
            recv(("zh", 4 + j), hpart(1, j))
            send(("hzr", j), hpart(1, j), hpart(1, j), d_zlo, rs=12 + j, wait_later=False)
            hsib(1, j)
            recv(("zh", j), hpart(0, j))
            hsib(0, j)

    def hz_outer(j):
        @pl.when(is_outer)
        def _():
            recv(("zh", 4 + j), hpart(1, j))
            hsib(1, j)

    def hs_outer():
        @pl.when(is_outer)
        def _():
            for j in range(4):
                hsib(0, j)

    def hsfin(rel):
        for j, xp in enumerate(xorder):
            recv(("hs", rel, j), part(1, xp, oc, t_of[rel], 0, HOME))

    def relay(r, hs=(0, 1)):
        a, rel, r0, n = ROUNDS[r]
        t = t_of[rel]
        for h in hs:
            k = 2 * a + h

            @pl.when(is_inner)
            def _():
                c = chunk(a, x, t, h, r0, n)
                recv(("z", 4 + k), c)
                send(("zr", k), c, c, d_zlo, rs=4 + k, wait_later=False)

    def xsend_h(r, h):
        a, rel, r0, n = ROUNDS[r]
        t = t_of[rel]
        k = 2 * a + h
        c = chunk(a, x, t, h, r0, n)
        if rel == 0:
            @pl.when(is_inner)
            def _():
                recv(("z", k), c)
        else:
            @pl.when(is_outer)
            def _():
                recv(("z", 4 + k), c)
        if h == 0:
            send(("x", r, 0, 0), c, c, d_xr)
        else:
            send(("x", r, 1, 1), c, c, d_xl)
            send(("x", r, 0, 1), c, c, d_xr)
            c = chunk(a, x, t, 0, r0, n)
            send(("x", r, 1, 0), c, c, d_xl)
            p = part(a, x, core, t, r0, n)
            send(("s", r, 0), p, p, d_sib)

    def xsend(r):
        xsend_h(r, 0)
        xsend_h(r, 1)

    def xfwd(r):
        a, rel, r0, n = ROUNDS[r]
        t = t_of[rel]
        c = chunk(a, xl, t, 0, r0, n)
        recv(("x", r, 0, 0), c)
        send(("xf", r, 0), c, c, d_xr)
        c = chunk(a, xr, t, 1, r0, n)
        recv(("x", r, 1, 1), c)
        send(("xf", r, 1), c, c, d_xl)

    def xfin(r):
        a, rel, r0, n = ROUNDS[r]
        t = t_of[rel]
        recv(("x", r, 0, 1), chunk(a, xl, t, 1, r0, n))
        p = part(a, xl, core, t, r0, n)
        send(("s", r, 1), p, p, d_sib)
        recv(("x", r, 1, 0), chunk(a, xr, t, 0, r0, n))
        p = part(a, xr, core, t, r0, n)
        send(("s", r, 2), p, p, d_sib)
        recv(("xf", r, 0), chunk(a, xf, t, 0, r0, n))
        recv(("xf", r, 1), chunk(a, xf, t, 1, r0, n))
        p = part(a, xf, core, t, r0, n)
        send(("s", r, 3), p, p, d_sib)

    def sfin(r):
        a, rel, r0, n = ROUNDS[r]
        for j, xp in enumerate(xorder):
            recv(("s", r, j), part(a, xp, oc, t_of[rel], r0, n))

    def forward(a, rel, r0, n):
        t = t_of[rel]
        terms = []
        for e in range(2 * nx):
            block = xb[a, e, rows(t * R + r0, n), :]
            cols = pl.ds((e % 2) * C, C)
            if a == 0:
                terms.append(dot(block, wgu[e // 2, cols, :], 1, 0))
            else:
                terms.append(dot(block, wdn[e // 2, :, cols], 1, 1))
        (pgu, ph)[a][rel, pl.ds(r0, n)] = functools.reduce(jnp.add, terms)

    REST = (HOME, R - HOME)

    hsend()
    ysend(0)
    xsend_h(0, 0)
    relay(1, (0,))
    hfwd()
    xsend_h(0, 1)
    relay(1, (1,))
    hfin_a()
    yfwd(0)
    ysend(1)
    relay(3)
    xfwd(0)
    xsend(2)
    xsend(1)
    xsend(3)
    hfin_b()
    hs_outer()
    hz_inner(0)
    hz_inner(1)
    xfin(0)
    xfwd(2)
    hz_inner(2)
    yfin(0)
    sfin(0)
    hz_inner(3)
    forward(0, 0, 0, R)
    send("pgu", pgu.at[0], pgur, d_zhi)
    yfwd(1)
    xfwd(1)
    xfwd(3)
    xfin(2)
    sfin(2)
    hsfin(0)
    yfin(1)
    forward(1, 0, 0, R)
    send("ph", ph.at[0], phr, d_zhi)
    xfin(1)
    for j in range(4):
        hz_outer(j)
    xfin(3)
    sfin(1)
    forward(0, 1, 0, R)
    hsfin(1)
    forward(1, 1, 0, HOME)
    sfin(3)
    forward(1, 1, *REST)

    recv("pgu", pgur)
    recv("ph", phr)
    gate = pgu[1, :, :F] + pgur[:, :F]
    up = pgu[1, :, F:] + pgur[:, F:]
    hg = ph[1] + phr[...]
    squashed = jax.nn.sigmoid(gate)
    activated = gate * squashed
    slope = squashed * (1.0 + gate * (1.0 - squashed))
    agu[trow(1 - z_hi), :F] = (hg * up * slope).astype(BF)
    agu[trow(1 - z_hi), F:] = (hg * activated).astype(BF)
    ah[trow(1 - z_hi), :] = (activated * up).astype(BF)
    send("agu", agu.at[trow(1 - z_hi), :], agu.at[trow(1 - z_hi), :], d_zhi)
    send("ah", ah.at[trow(1 - z_hi), :], ah.at[trow(1 - z_hi), :], d_zhi)

    order = (xf, xr, xl, x)
    RA = ((ZF, R - ZF), (0, ZF))

    def hrows(p, h):
        r0, n = RA[p]
        return pl.ds(r0 + h * (n // 2), n // 2)

    def arows(p):
        return pl.ds(*RA[p])

    def igblock(rel, xp, c):
        w = wgu[xp, pl.ds(pl.multiple_of(c * C, C), C), :]
        igp[rel, 2 * xp + c] = dot(agu[trow(t_of[rel]), :], w, 1, 1)

    def igstart(rel):
        for j, xp in enumerate(order):
            igblock(rel, xp, oc)
            send(("is", rel, j), igp.at[rel, 2 * xp + oc], sibr.at[rel, xp], d_sib)
        for xp in order:
            igblock(rel, xp, core)

    def addsib(rel, j):
        xp = order[j]
        recv(("is", rel, j), sibr.at[rel, xp])
        igp[rel, 2 * xp + core] += sibr[rel, xp]

    def zfirst(rel, j):
        xp = order[j]
        send(("zf", j), igp.at[rel, 2 * xp + core, arows(1), :], zfr.at[xp], d_zlo, wait_later=False)

    def igfar(p, rel, k):
        for h, d in enumerate((d_xr, d_xl)):
            fs[k, h, pl.ds(0, RA[p][1] // 2), :] = igp[rel, 2 * xf + core, hrows(p, h), :].astype(BF)
            n = pl.ds(0, RA[p][1] // 2)
            send(("if", k, h), fs.at[k, h, n, :], farr.at[k, h, n, :], d)

    def ignear(p, rel, k):
        for h, (xp, d) in enumerate(((xr, d_xr), (xl, d_xl))):
            send(("in", k, h, 1 - h), igp.at[rel, 2 * xp + core, hrows(p, 1 - h), :],
                 nearr.at[rel, h, hrows(p, 1 - h), :], d)

    def igsecond(p, rel, k):
        for h, (xp, d) in enumerate(((xr, d_xr), (xl, d_xl))):
            n = pl.ds(0, RA[p][1] // 2)
            recv(("if", k, h), farr.at[k, h, n, :])
            igp[rel, 2 * xp + core, hrows(p, h), :] += farr[k, h, n, :].astype(F32)
            send(("in", k, h, h), igp.at[rel, 2 * xp + core, hrows(p, h), :], nearr.at[rel, h, hrows(p, h), :], d)

    def iglast(p, rel, k):
        for h in range(2):
            for g in range(2):
                recv(("in", k, h, g), nearr.at[rel, h, hrows(p, g), :])
        igp[rel, 2 * x + core, arows(p), :] += nearr[rel, 0, arows(p), :] + nearr[rel, 1, arows(p), :]

    def igfirst(rel, when):
        addsib(rel, 0)
        igfar(0, rel, rel)
        addsib(rel, 1)
        addsib(rel, 2)
        ignear(0, rel, rel)
        addsib(rel, 3)

        @pl.when(when)
        def _():
            for j in range(4):
                zfirst(rel, j)

    def wunit(e):
        g = dot(xb[0, e, : 2 * R], agu[...], 0, 0)
        ws[e] = g
        gb[e] = g.astype(BF)
        d = dot(ah[...], xb[1, e, : 2 * R], 0, 0)
        hs[e] = d
        hb[e] = d.astype(BF)

    sides = ((yr, d_yr), (yl, d_yl))
    def zsend(rel):
        for h in range(2):
            send(("zi", rel, h), igp.at[rel, 2 * x + core, hrows(0, h), :], zr.at[hrows(0, h), :], d_zlo,
                 rs=sid(("zir", h)), wait_later=False)

    def wfirst(e, s, h):
        wunit(e)
        send(("gn", s, h), gb.at[e], gnr.at[s, h], sides[s][1])
        send(("hn", s, h), hb.at[e], hnr.at[s, h], sides[s][1])

    def zfadd(j):
        xp = order[j]
        recv(("zf", j), zfr.at[xp])
        igp[keep, 2 * xp + core, arows(1), :] += zfr[xp]

    def wsecond(h):
        yp, d = sides[h]
        recv(("gf", h), gfr.at[h])
        gb[2 * yp + h] = (ws[2 * yp + h] + gfr[h].astype(F32)).astype(BF)
        send(("gn", h, h), gb.at[2 * yp + h], gnr.at[h, h], d)
        recv(("hf2", h), hfr.at[h])
        hb[2 * yp + h] = (hs[2 * yp + h] + hfr[h].astype(F32)).astype(BF)
        send(("hn", h, h), hb.at[2 * yp + h], hnr.at[h, h], d)

    keep = inner
    igstart(1)
    igfirst(1, is_outer)
    recv("agu", agu.at[trow(z_hi), :])
    recv("ah", ah.at[trow(z_hi), :])
    for h, (yp, d) in enumerate(sides):
        wunit(2 * yf + h)
        send(("gf", h), gb.at[2 * yf + h], gfr.at[h], d)
        send(("hf2", h), hb.at[2 * yf + h], hfr.at[h], d)
    igsecond(0, 1, 1)
    igstart(0)
    igfirst(0, is_inner)
    for h, (yp, d) in enumerate(sides):
        wfirst(2 * yp + 1 - h, h, 1 - h)
    for h, (yp, d) in enumerate(sides):
        wunit(2 * yp + h)
    iglast(0, 1, 1)

    @pl.when(is_outer)
    def _():
        zsend(1)

    zfadd(0)
    igfar(1, keep, 2)
    wsecond(0)
    wsecond(1)
    igsecond(0, 0, 0)
    zfadd(1)
    zfadd(2)
    ignear(1, keep, 2)
    for h in range(2):
        wunit(2 * y + h)
    igsecond(1, keep, 2)
    iglast(0, 0, 0)

    @pl.when(is_inner)
    def _():
        zsend(0)
        n = pl.ds(0, (R - ZF) // 2)
        for h in range(2):
            recv(("zir", h), zr.at[hrows(0, h), :])
            igs[h, n, :] = (igp[1, 2 * x + core, hrows(0, h), :] + zr[hrows(0, h), :]).astype(BF)
            send(("zo", h), igs.at[h, n, :], igr.at[h, n, :], d_zz, wait_later=False)

    zfadd(3)
    iglast(1, keep, 2)

    @pl.when(is_inner)
    def _():
        igs[2, pl.ds(0, ZF), :] = igp[1, 2 * x + core, arows(1), :].astype(BF)
        send(("zo", 2), igs.at[2, pl.ds(0, ZF), :], igr.at[2, pl.ds(0, ZF), :], d_zz, wait_later=False)

    @pl.when(is_outer)
    def _():
        ig_o[arows(1), :] = igp[0, 2 * x + core, arows(1), :].astype(BF)

    for h in range(2):
        for s in range(2):
            recv(("gn", s, h), gnr.at[s, h])
            recv(("hn", s, h), hnr.at[s, h])
        g = (ws[2 * y + h] + gnr[0, h].astype(F32) + gnr[1, h].astype(F32)) * factor
        gg_o[pl.ds(h * C, C), :] = g[:, :F]
        ug_o[pl.ds(h * C, C), :] = g[:, F:]
        dg_o[:, pl.ds(h * C, C)] = (hs[2 * y + h] + hnr[0, h].astype(F32) + hnr[1, h].astype(F32)) * factor

    @pl.when(is_outer)
    def _():
        for h in range(2):
            recv(("zir", h), zr.at[hrows(0, h), :])
            ig_o[hrows(0, h), :] = (igp[0, 2 * x + core, hrows(0, h), :] + zr[hrows(0, h), :]).astype(BF)

    def wait_send(name, src):
        i = sid(name)
        pltpu.make_async_remote_copy(
            src_ref=src, dst_ref=src, send_sem=ssem.at[i], recv_sem=rsem.at[i],
            device_id=d_sib, device_id_type=MESH).wait_send()

    @pl.when(is_inner)
    def _():
        zs, n = pl.ds(0, ZF), pl.ds(0, (R - ZF) // 2)
        recv(("zo", 2), igr.at[2, zs, :])
        ig_o[arows(1), :] = igr[2, zs, :]
        for h in range(2):
            recv(("zo", h), igr.at[h, n, :])
            ig_o[hrows(0, h), :] = igr[h, n, :]
        wait_send(("zo", 2), igs.at[2, zs, :])
        for h in range(2):
            wait_send(("zo", h), igs.at[h, n, :])
            wait_send(("zi", 0, h), zr.at[hrows(0, h), :])
        for r in (1, 3):
            a, rel, r0, n = ROUNDS[r]
            for h in range(2):
                wait_send(("zr", 2 * a + h), chunk(a, x, t_of[1], h, r0, n))
        for j in range(4):
            wait_send(("hzr", j), hpart(1, j))

    @pl.when(is_outer)
    def _():
        for h in range(2):
            wait_send(("zi", 1, h), zr.at[hrows(0, h), :])

    for j in range(4):
        wait_send(("zf", j), zfr.at[j])
        for rel in range(2):
            wait_send(("hs", rel, j), hpart(rel, j))
    for c in pending:
        c.wait_send()
    assert len(ids) <= NSEM


def shards(tokens, out_grad, gate_weight, up_weight, down_weight):
    R, C = tokens.shape
    F = gate_weight.shape[1]
    H = R // 2
    factor = 1.0 / math.sqrt(R * lax.axis_size(FSDP))
    anyspec = pl.BlockSpec(memory_space=pl.ANY)
    vm = pl.BlockSpec(memory_space=pltpu.VMEM)
    V = pltpu.VMEM
    scratch = [
        V((2, R, C), BF), V((2, 8, 2 * R + HOME, C), BF), V((4, 2 * C, 2 * F), BF), V((4, F, 2 * C), BF),
        V((2, R, 2 * F), F32), V((2, R, F), F32), V((R, 2 * F), F32), V((R, F), F32),
        V((2 * R, 2 * F), BF), V((2 * R, F), BF),
        V((2, 8, R, C), F32), V((2, 4, R, C), F32), V((3, 2, H, C), BF), V((2, 2, R, C), F32), V((3, 2, H, C), BF), V((4, ZF, C), F32),
        V((R, C), F32), V((3, H, C), BF), V((3, H, C), BF),
        V((8, C, 2 * F), F32), V((8, F, C), F32), V((8, C, 2 * F), BF), V((8, F, C), BF),
        V((2, C, 2 * F), BF), V((2, F, C), BF), V((2, 2, C, 2 * F), BF), V((2, 2, F, C), BF),
        pltpu.SemaphoreType.DMA((8,)), pltpu.SemaphoreType.DMA((NSEM,)), pltpu.SemaphoreType.DMA((NSEM,)),
    ]
    return pl.pallas_call(
        functools.partial(kernel, factor),
        out_shape=(
            jax.ShapeDtypeStruct((R, C), BF),
            jax.ShapeDtypeStruct((2 * C, F), F32),
            jax.ShapeDtypeStruct((2 * C, F), F32),
            jax.ShapeDtypeStruct((F, 2 * C), F32),
        ),
        in_specs=[anyspec] * 5,
        out_specs=(vm,) * 4,
        scratch_shapes=scratch,
        compiler_params=pltpu.CompilerParams(
            collective_id=0, has_side_effects=True, vmem_limit_bytes=60 * 1024 * 1024),
        name="ffn_backward",
    )(tokens, out_grad, gate_weight, up_weight, down_weight)


def solution(mesh):
    finer = Mesh(mesh.devices.reshape(2, 4, 2, 4, 2), ("z_hi", "y", "z_lo", "x", "core"))
    return jax.shard_map(
        shards,
        mesh=finer,
        in_specs=(P(FSDP, TP), P(FSDP, TP), P(FSDP, TP), P(FSDP, TP), P(TP, FSDP)),
        out_specs=(P(FSDP, TP), P(FSDP, TP), P(FSDP, TP), P(TP, FSDP)),
        check_vma=False,
    )
```

```python
import functools
import math

import jax
import jax.numpy as jnp
from jax import lax
from jax.experimental import pallas as pl
from jax.experimental.pallas import tpu as pltpu
from jax.sharding import Mesh
from jax.sharding import PartitionSpec as P

FSDP = ("z_hi", "y")
TP = ("z_lo", "x", "core")
MESH = pl.DeviceIdType.MESH
BF = jnp.bfloat16
F32 = jnp.float32
NSEM = 224
ZF = 64
HOME = 160
ROUNDS = ((0, 0, 0, 256), (0, 1, 0, 256), (1, 0, HOME, 256 - HOME), (1, 1, HOME, 256 - HOME))


def dot(a, b, ca, cb):
    return lax.dot_general(a, b, (((ca,), (cb,)), ((), ())), preferred_element_type=F32)


def kernel(factor, tok, og, wg, wu, wd, ig_o, gg_o, ug_o, dg_o,
           own, xb, wgu, wdn, pgu, ph, pgur, phr, agu, ah, igp, sibr, farr, nearr, fs, zfr, zr, igs, igr,
           ws, hs, gb, hb, gfr, hfr, gnr, hnr, lsem, ssem, rsem):
    R, C = tok.shape
    F = wg.shape[1]
    H = R // 2
    z_hi, y, z_lo, x, core = (lax.axis_index(a) for a in ("z_hi", "y", "z_lo", "x", "core"))
    inner = (z_hi - z_lo) * (z_hi - z_lo)
    is_inner, is_outer = inner == 1, inner == 0
    nx, ny = 4, 4
    xr, xl, xf = lax.rem(x + 1, nx), lax.rem(x + nx - 1, nx), lax.rem(x + 2, nx)
    yr, yl, yf = lax.rem(y + 1, ny), lax.rem(y + ny - 1, ny), lax.rem(y + 2, ny)
    oc = 1 - core
    t_of = (z_hi, 1 - z_hi)
    d_xr, d_xl = (z_hi, y, z_lo, xr, core), (z_hi, y, z_lo, xl, core)
    d_yr, d_yl = (z_hi, yr, z_lo, x, core), (z_hi, yl, z_lo, x, core)
    d_sib = (z_hi, y, z_lo, x, oc)
    d_zlo = (z_hi, y, 1 - z_lo, x, core)
    d_zhi = (1 - z_hi, y, z_lo, x, core)
    d_zz = (1 - z_hi, y, 1 - z_lo, x, core)
    d_zs = (z_lo, y, 1 - z_lo, x, core)
    partners = (d_xr, d_xl, d_yr, d_yl, d_sib, d_zlo, d_zhi, d_zz)

    ids = {}

    def sid(name):
        return ids.setdefault(name, len(ids))

    for k in range(8):
        sid(("z", k))
    for k in range(8):
        sid(("zh", k))
    pending = []

    def send(name, src, dst, dev, rs=None, wait_later=True):
        i = sid(name)
        c = pltpu.make_async_remote_copy(
            src_ref=src, dst_ref=dst, send_sem=ssem.at[i], recv_sem=rsem.at[i if rs is None else rs],
            device_id=dev, device_id_type=MESH)
        c.start()
        if wait_later:
            pending.append(c)
        return c

    def recv(name, dst):
        i = sid(name)
        pltpu.make_async_remote_copy(
            src_ref=dst, dst_ref=dst, send_sem=ssem.at[i], recv_sem=rsem.at[i],
            device_id=d_sib, device_id_type=MESH).wait_recv()

    def trow(t):
        return pl.ds(pl.multiple_of(t * R, R), R)

    def blk(a, xp, c, t):
        return xb.at[a, 2 * xp + c, trow(t), :]

    def rows(start, n):
        return pl.ds(pl.multiple_of(start, 16), n)

    def chunk(a, xp, t, h, r0, n):
        return xb.at[a, 2 * xp + core, rows(t * R + r0 + h * (n // 2), n // 2), :]

    def part(a, xp, c, t, r0, n):
        return xb.at[a, 2 * xp + c, rows(t * R + r0, n), :]

    home_at = (1 - inner) * z_hi * R + inner * 2 * R

    def home(xp, h=None):
        if h is None:
            return xb.at[1, 2 * xp + core, rows(home_at, HOME), :]
        return xb.at[1, 2 * xp + core, rows(home_at + h * (HOME // 2), HOME // 2), :]

    loads_w = [
        pltpu.make_async_copy(wg, wgu.at[y, :, pl.ds(0, F)], lsem.at[0]),
        pltpu.make_async_copy(wu, wgu.at[y, :, pl.ds(F, F)], lsem.at[1]),
        pltpu.make_async_copy(wd, wdn.at[y], lsem.at[2]),
    ]
    loads_t = [
        pltpu.make_async_copy(tok, own.at[0], lsem.at[3]),
        pltpu.make_async_copy(og, own.at[1], lsem.at[4]),
    ]
    for c in loads_t + loads_w:
        c.start()

    outer_loads = (
        (tok, blk(0, x, core, z_hi), lsem.at[5]),
        (og.at[pl.ds(HOME, R - HOME), :], part(1, x, core, z_hi, HOME, R - HOME), lsem.at[6]),
    )
    load_home = pltpu.make_async_copy(og.at[pl.ds(0, HOME), :], home(x), lsem.at[7])
    load_home.start()

    @pl.when(is_outer)
    def _():
        for c in outer_loads:
            pltpu.make_async_copy(*c).start()

    barrier = pltpu.get_barrier_semaphore()
    for d in partners:
        pl.semaphore_signal(barrier, inc=1, device_id=d, device_id_type=MESH)
    pl.semaphore_wait(barrier, len(partners))

    for c in loads_t:
        c.wait()
    load_home.wait()

    for a, rel, r0, n in (ROUNDS[0], ROUNDS[2]):
        for h in range(2):
            k = 2 * a + h
            send(("zs", k), own.at[a, pl.ds(r0 + h * (n // 2), n // 2), :], chunk(a, x, z_hi, h, r0, n), d_zs,
                 rs=4 * inner + k)

    @pl.when(is_outer)
    def _():
        for c in outer_loads:
            pltpu.make_async_copy(*c).wait()

    for c in loads_w:
        c.wait()

    def wchunk(which, yp, h):
        if which == 0:
            return wgu.at[yp, pl.ds(h * C, C), :]
        return wdn.at[yp, pl.ds(h * (F // 2), F // 2), :]

    def ysend(w):
        for h in range(2):
            send(("y", w, 0, h), wchunk(w, y, h), wchunk(w, y, h), d_yr)
            send(("y", w, 1, 1 - h), wchunk(w, y, 1 - h), wchunk(w, y, 1 - h), d_yl)

    def yfwd(w):
        recv(("y", w, 0, 0), wchunk(w, yl, 0))
        send(("yf", w, 0), wchunk(w, yl, 0), wchunk(w, yl, 0), d_yr)
        recv(("y", w, 1, 1), wchunk(w, yr, 1))
        send(("yf", w, 1), wchunk(w, yr, 1), wchunk(w, yr, 1), d_yl)

    def yfin(w):
        recv(("y", w, 0, 1), wchunk(w, yl, 1))
        recv(("y", w, 1, 0), wchunk(w, yr, 0))
        recv(("yf", w, 0), wchunk(w, yf, 0))
        recv(("yf", w, 1), wchunk(w, yf, 1))

    def hsend():
        for h in range(2):
            send(("h", 0, h), home(x, h), home(x, h), d_xr)
            send(("h", 1, 1 - h), home(x, 1 - h), home(x, 1 - h), d_xl)

    def homez(j, xp):
        send(("hz", j), home(xp), xb.at[1, 2 * xp + core, rows(z_hi * R, HOME), :], d_zs, rs=8 + 4 * inner + j)

    def hfwd():
        recv(("h", 0, 0), home(xl, 0))
        send(("hf", 0), home(xl, 0), home(xl, 0), d_xr)
        recv(("h", 1, 1), home(xr, 1))
        send(("hf", 1), home(xr, 1), home(xr, 1), d_xl)

    def hfin_a():
        homez(0, x)
        recv(("h", 0, 1), home(xl, 1))
        homez(1, xl)
        recv(("h", 1, 0), home(xr, 0))
        homez(2, xr)

    def hfin_b():
        recv(("hf", 0), home(xf, 0))
        recv(("hf", 1), home(xf, 1))
        homez(3, xf)

    xorder = (x, xl, xr, xf)

    def hpart(rel, j):
        return part(1, xorder[j], core, t_of[rel], 0, HOME)

    def hsib(rel, j):
        send(("hs", rel, j), hpart(rel, j), hpart(rel, j), d_sib, wait_later=False)

    def hz_inner(j):
        @pl.when(is_inner)
        def _():
            recv(("zh", 4 + j), hpart(1, j))
            send(("hzr", j), hpart(1, j), hpart(1, j), d_zlo, rs=12 + j, wait_later=False)
            hsib(1, j)
            recv(("zh", j), hpart(0, j))
            hsib(0, j)

    def hz_outer(j):
        @pl.when(is_outer)
        def _():
            recv(("zh", 4 + j), hpart(1, j))
            hsib(1, j)

    def hs_outer():
        @pl.when(is_outer)
        def _():
            for j in range(4):
                hsib(0, j)

    def hsfin(rel):
        for j, xp in enumerate(xorder):
            recv(("hs", rel, j), part(1, xp, oc, t_of[rel], 0, HOME))

    def relay(r, hs=(0, 1)):
        a, rel, r0, n = ROUNDS[r]
        t = t_of[rel]
        for h in hs:
            k = 2 * a + h

            @pl.when(is_inner)
            def _():
                c = chunk(a, x, t, h, r0, n)
                recv(("z", 4 + k), c)
                send(("zr", k), c, c, d_zlo, rs=4 + k, wait_later=False)

    def xsend_h(r, h):
        a, rel, r0, n = ROUNDS[r]
        t = t_of[rel]
        k = 2 * a + h
        c = chunk(a, x, t, h, r0, n)
        if rel == 0:
            @pl.when(is_inner)
            def _():
                recv(("z", k), c)
        else:
            @pl.when(is_outer)
            def _():
                recv(("z", 4 + k), c)
        if h == 0:
            send(("x", r, 0, 0), c, c, d_xr)
        else:
            send(("x", r, 1, 1), c, c, d_xl)
            send(("x", r, 0, 1), c, c, d_xr)
            c = chunk(a, x, t, 0, r0, n)
            send(("x", r, 1, 0), c, c, d_xl)
            p = part(a, x, core, t, r0, n)
            send(("s", r, 0), p, p, d_sib)

    def xsend(r):
        xsend_h(r, 0)
        xsend_h(r, 1)

    def xfwd(r):
        a, rel, r0, n = ROUNDS[r]
        t = t_of[rel]
        c = chunk(a, xl, t, 0, r0, n)
        recv(("x", r, 0, 0), c)
        send(("xf", r, 0), c, c, d_xr)
        c = chunk(a, xr, t, 1, r0, n)
        recv(("x", r, 1, 1), c)
        send(("xf", r, 1), c, c, d_xl)

    def xfin(r):
        a, rel, r0, n = ROUNDS[r]
        t = t_of[rel]
        recv(("x", r, 0, 1), chunk(a, xl, t, 1, r0, n))
        p = part(a, xl, core, t, r0, n)
        send(("s", r, 1), p, p, d_sib)
        recv(("x", r, 1, 0), chunk(a, xr, t, 0, r0, n))
        p = part(a, xr, core, t, r0, n)
        send(("s", r, 2), p, p, d_sib)
        recv(("xf", r, 0), chunk(a, xf, t, 0, r0, n))
        recv(("xf", r, 1), chunk(a, xf, t, 1, r0, n))
        p = part(a, xf, core, t, r0, n)
        send(("s", r, 3), p, p, d_sib)

    def sfin(r):
        a, rel, r0, n = ROUNDS[r]
        for j, xp in enumerate(xorder):
            recv(("s", r, j), part(a, xp, oc, t_of[rel], r0, n))

    def forward(a, rel, r0, n):
        t = t_of[rel]
        terms = []
        for e in range(2 * nx):
            block = xb[a, e, rows(t * R + r0, n), :]
            cols = pl.ds((e % 2) * C, C)
            if a == 0:
                terms.append(dot(block, wgu[e // 2, cols, :], 1, 0))
            else:
                terms.append(dot(block, wdn[e // 2, :, cols], 1, 1))
        (pgu, ph)[a][rel, pl.ds(r0, n)] = functools.reduce(jnp.add, terms)

    REST = (HOME, R - HOME)

    hsend()
    ysend(0)
    xsend_h(0, 0)
    relay(1, (0,))
    hfwd()
    xsend_h(0, 1)
    relay(1, (1,))
    hfin_a()
    yfwd(0)
    ysend(1)
    relay(3)
    xfwd(0)
    xsend(2)
    xsend(1)
    xsend(3)
    hfin_b()
    hs_outer()
    hz_inner(0)
    hz_inner(1)
    xfin(0)
    xfwd(2)
    hz_inner(2)
    yfin(0)
    sfin(0)
    hz_inner(3)
    forward(0, 0, 0, R)
    send("pgu", pgu.at[0], pgur, d_zhi)
    yfwd(1)
    xfwd(1)
    xfwd(3)
    xfin(2)
    sfin(2)
    hsfin(0)
    yfin(1)
    forward(1, 0, 0, R)
    send("ph", ph.at[0], phr, d_zhi)
    xfin(1)
    for j in range(4):
        hz_outer(j)
    xfin(3)
    sfin(1)
    forward(0, 1, 0, R)
    hsfin(1)
    forward(1, 1, 0, HOME)
    sfin(3)
    forward(1, 1, *REST)

    recv("pgu", pgur)
    recv("ph", phr)
    gate = pgu[1, :, :F] + pgur[:, :F]
    up = pgu[1, :, F:] + pgur[:, F:]
    hg = ph[1] + phr[...]
    squashed = jax.nn.sigmoid(gate)
    activated = gate * squashed
    slope = squashed * (1.0 + gate * (1.0 - squashed))
    agu[trow(1 - z_hi), :F] = (hg * up * slope).astype(BF)
    agu[trow(1 - z_hi), F:] = (hg * activated).astype(BF)
    ah[trow(1 - z_hi), :] = (activated * up).astype(BF)
    send("agu", agu.at[trow(1 - z_hi), :], agu.at[trow(1 - z_hi), :], d_zhi)
    send("ah", ah.at[trow(1 - z_hi), :], ah.at[trow(1 - z_hi), :], d_zhi)

    order = (xf, xr, xl, x)
    RA = ((ZF, R - ZF), (0, ZF))

    def hrows(p, h):
        r0, n = RA[p]
        return pl.ds(r0 + h * (n // 2), n // 2)

    def arows(p):
        return pl.ds(*RA[p])

    def igblock(rel, xp, c):
        w = wgu[xp, pl.ds(pl.multiple_of(c * C, C), C), :]
        igp[rel, 2 * xp + c] = dot(agu[trow(t_of[rel]), :], w, 1, 1)

    def igstart(rel):
        for j, xp in enumerate(order):
            igblock(rel, xp, oc)
            send(("is", rel, j), igp.at[rel, 2 * xp + oc], sibr.at[rel, xp], d_sib)
        for xp in order:
            igblock(rel, xp, core)

    def addsib(rel, j):
        xp = order[j]
        recv(("is", rel, j), sibr.at[rel, xp])
        igp[rel, 2 * xp + core] += sibr[rel, xp]

    def zfirst(rel, j):
        xp = order[j]
        send(("zf", j), igp.at[rel, 2 * xp + core, arows(1), :], zfr.at[xp], d_zlo, wait_later=False)

    def igfar(p, rel, k):
        for h, d in enumerate((d_xr, d_xl)):
            fs[k, h, pl.ds(0, RA[p][1] // 2), :] = igp[rel, 2 * xf + core, hrows(p, h), :].astype(BF)
            n = pl.ds(0, RA[p][1] // 2)
            send(("if", k, h), fs.at[k, h, n, :], farr.at[k, h, n, :], d)

    def ignear(p, rel, k):
        for h, (xp, d) in enumerate(((xr, d_xr), (xl, d_xl))):
            send(("in", k, h, 1 - h), igp.at[rel, 2 * xp + core, hrows(p, 1 - h), :],
                 nearr.at[rel, h, hrows(p, 1 - h), :], d)

    def igsecond(p, rel, k):
        for h, (xp, d) in enumerate(((xr, d_xr), (xl, d_xl))):
            n = pl.ds(0, RA[p][1] // 2)
            recv(("if", k, h), farr.at[k, h, n, :])
            igp[rel, 2 * xp + core, hrows(p, h), :] += farr[k, h, n, :].astype(F32)
            send(("in", k, h, h), igp.at[rel, 2 * xp + core, hrows(p, h), :], nearr.at[rel, h, hrows(p, h), :], d)

    def iglast(p, rel, k):
        for h in range(2):
            for g in range(2):
                recv(("in", k, h, g), nearr.at[rel, h, hrows(p, g), :])
        igp[rel, 2 * x + core, arows(p), :] += nearr[rel, 0, arows(p), :] + nearr[rel, 1, arows(p), :]

    def igfirst(rel, when):
        addsib(rel, 0)
        igfar(0, rel, rel)
        addsib(rel, 1)
        addsib(rel, 2)
        ignear(0, rel, rel)
        addsib(rel, 3)

        @pl.when(when)
        def _():
            for j in range(4):
                zfirst(rel, j)

    def wunit(e):
        g = dot(xb[0, e, : 2 * R], agu[...], 0, 0)
        ws[e] = g
        gb[e] = g.astype(BF)
        d = dot(ah[...], xb[1, e, : 2 * R], 0, 0)
        hs[e] = d
        hb[e] = d.astype(BF)

    sides = ((yr, d_yr), (yl, d_yl))
    def zsend(rel):
        for h in range(2):
            send(("zi", rel, h), igp.at[rel, 2 * x + core, hrows(0, h), :], zr.at[hrows(0, h), :], d_zlo,
                 rs=sid(("zir", h)), wait_later=False)

    def wfirst(e, s, h):
        wunit(e)
        send(("gn", s, h), gb.at[e], gnr.at[s, h], sides[s][1])
        send(("hn", s, h), hb.at[e], hnr.at[s, h], sides[s][1])

    def zfadd(j):
        xp = order[j]
        recv(("zf", j), zfr.at[xp])
        igp[keep, 2 * xp + core, arows(1), :] += zfr[xp]

    def wsecond(h):
        yp, d = sides[h]
        recv(("gf", h), gfr.at[h])
        gb[2 * yp + h] = (ws[2 * yp + h] + gfr[h].astype(F32)).astype(BF)
        send(("gn", h, h), gb.at[2 * yp + h], gnr.at[h, h], d)
        recv(("hf2", h), hfr.at[h])
        hb[2 * yp + h] = (hs[2 * yp + h] + hfr[h].astype(F32)).astype(BF)
        send(("hn", h, h), hb.at[2 * yp + h], hnr.at[h, h], d)

    keep = inner
    igstart(1)
    igfirst(1, is_outer)
    recv("agu", agu.at[trow(z_hi), :])
    recv("ah", ah.at[trow(z_hi), :])
    for h, (yp, d) in enumerate(sides):
        wunit(2 * yf + h)
        send(("gf", h), gb.at[2 * yf + h], gfr.at[h], d)
        send(("hf2", h), hb.at[2 * yf + h], hfr.at[h], d)
    igsecond(0, 1, 1)
    igstart(0)
    igfirst(0, is_inner)
    for h, (yp, d) in enumerate(sides):
        wfirst(2 * yp + 1 - h, h, 1 - h)
    for h, (yp, d) in enumerate(sides):
        wunit(2 * yp + h)
    iglast(0, 1, 1)

    @pl.when(is_outer)
    def _():
        zsend(1)

    zfadd(0)
    igfar(1, keep, 2)
    wsecond(0)
    wsecond(1)
    igsecond(0, 0, 0)
    zfadd(1)
    zfadd(2)
    ignear(1, keep, 2)
    for h in range(2):
        wunit(2 * y + h)
    igsecond(1, keep, 2)
    iglast(0, 0, 0)

    @pl.when(is_inner)
    def _():
        zsend(0)
        n = pl.ds(0, (R - ZF) // 2)
        for h in range(2):
            recv(("zir", h), zr.at[hrows(0, h), :])
            igs[h, n, :] = (igp[1, 2 * x + core, hrows(0, h), :] + zr[hrows(0, h), :]).astype(BF)
            send(("zo", h), igs.at[h, n, :], igr.at[h, n, :], d_zz, wait_later=False)

    zfadd(3)
    iglast(1, keep, 2)

    @pl.when(is_inner)
    def _():
        igs[2, pl.ds(0, ZF), :] = igp[1, 2 * x + core, arows(1), :].astype(BF)
        send(("zo", 2), igs.at[2, pl.ds(0, ZF), :], igr.at[2, pl.ds(0, ZF), :], d_zz, wait_later=False)

    @pl.when(is_outer)
    def _():
        ig_o[arows(1), :] = igp[0, 2 * x + core, arows(1), :].astype(BF)

    for h in range(2):
        for s in range(2):
            recv(("gn", s, h), gnr.at[s, h])
            recv(("hn", s, h), hnr.at[s, h])
        g = (ws[2 * y + h] + gnr[0, h].astype(F32) + gnr[1, h].astype(F32)) * factor
        gg_o[pl.ds(h * C, C), :] = g[:, :F]
        ug_o[pl.ds(h * C, C), :] = g[:, F:]
        dg_o[:, pl.ds(h * C, C)] = (hs[2 * y + h] + hnr[0, h].astype(F32) + hnr[1, h].astype(F32)) * factor

    @pl.when(is_outer)
    def _():
        for h in range(2):
            recv(("zir", h), zr.at[hrows(0, h), :])
            ig_o[hrows(0, h), :] = (igp[0, 2 * x + core, hrows(0, h), :] + zr[hrows(0, h), :]).astype(BF)

    def wait_send(name, src):
        i = sid(name)
        pltpu.make_async_remote_copy(
            src_ref=src, dst_ref=src, send_sem=ssem.at[i], recv_sem=rsem.at[i],
            device_id=d_sib, device_id_type=MESH).wait_send()

    @pl.when(is_inner)
    def _():
        zs, n = pl.ds(0, ZF), pl.ds(0, (R - ZF) // 2)
        recv(("zo", 2), igr.at[2, zs, :])
        ig_o[arows(1), :] = igr[2, zs, :]
        for h in range(2):
            recv(("zo", h), igr.at[h, n, :])
            ig_o[hrows(0, h), :] = igr[h, n, :]
        wait_send(("zo", 2), igs.at[2, zs, :])
        for h in range(2):
            wait_send(("zo", h), igs.at[h, n, :])
            wait_send(("zi", 0, h), zr.at[hrows(0, h), :])
        for r in (1, 3):
            a, rel, r0, n = ROUNDS[r]
            for h in range(2):
                wait_send(("zr", 2 * a + h), chunk(a, x, t_of[1], h, r0, n))
        for j in range(4):
            wait_send(("hzr", j), hpart(1, j))

    @pl.when(is_outer)
    def _():
        for h in range(2):
            wait_send(("zi", 1, h), zr.at[hrows(0, h), :])

    for j in range(4):
        wait_send(("zf", j), zfr.at[j])
        for rel in range(2):
            wait_send(("hs", rel, j), hpart(rel, j))
    for c in pending:
        c.wait_send()
    assert len(ids) <= NSEM


def deliver(*refs):
    n = (len(refs) - 1) // 2
    copies = [pltpu.make_async_copy(refs[k], refs[n + k], refs[-1].at[k]) for k in range(n)]
    for c in copies:
        c.start()
    for c in copies:
        c.wait()


def shards(tokens, out_grad, gate_weight, up_weight, down_weight):
    R, C = tokens.shape
    F = gate_weight.shape[1]
    H = R // 2
    factor = 1.0 / math.sqrt(R * lax.axis_size(FSDP))
    anyspec = pl.BlockSpec(memory_space=pl.ANY)
    vm = pl.BlockSpec(memory_space=pltpu.VMEM)
    V = pltpu.VMEM
    scratch = [
        V((2, R, C), BF), V((2, 8, 2 * R + HOME, C), BF), V((4, 2 * C, 2 * F), BF), V((4, F, 2 * C), BF),
        V((2, R, 2 * F), F32), V((2, R, F), F32), V((R, 2 * F), F32), V((R, F), F32),
        V((2 * R, 2 * F), BF), V((2 * R, F), BF),
        V((2, 8, R, C), F32), V((2, 4, R, C), F32), V((3, 2, H, C), BF), V((2, 2, R, C), F32), V((3, 2, H, C), BF), V((4, ZF, C), F32),
        V((R, C), F32), V((3, H, C), BF), V((3, H, C), BF),
        V((8, C, 2 * F), F32), V((8, F, C), F32), V((8, C, 2 * F), BF), V((8, F, C), BF),
        V((2, C, 2 * F), BF), V((2, F, C), BF), V((2, 2, C, 2 * F), BF), V((2, 2, F, C), BF),
        pltpu.SemaphoreType.DMA((8,)), pltpu.SemaphoreType.DMA((NSEM,)), pltpu.SemaphoreType.DMA((NSEM,)),
    ]
    held = pl.pallas_call(
        functools.partial(kernel, factor),
        out_shape=(
            V((R, C), BF),
            V((2 * C, F), F32),
            V((2 * C, F), F32),
            V((F, 2 * C), F32),
        ),
        in_specs=[anyspec] * 5,
        out_specs=(vm,) * 4,
        scratch_shapes=scratch,
        compiler_params=pltpu.CompilerParams(
            collective_id=0, has_side_effects=True, vmem_limit_bytes=60 * 1024 * 1024),
        name="ffn_backward",
    )(tokens, out_grad, gate_weight, up_weight, down_weight)
    return pl.pallas_call(
        deliver,
        out_shape=tuple(jax.ShapeDtypeStruct(a.shape, a.dtype) for a in held),
        in_specs=[vm] * len(held),
        out_specs=(anyspec,) * len(held),
        scratch_shapes=[pltpu.SemaphoreType.DMA((len(held),))],
        name="deliver",
    )(*[pltpu.with_memory_space_constraint(a, pltpu.VMEM) for a in held])


def solution(mesh):
    finer = Mesh(mesh.devices.reshape(2, 4, 2, 4, 2), ("z_hi", "y", "z_lo", "x", "core"))
    return jax.shard_map(
        shards,
        mesh=finer,
        in_specs=(P(FSDP, TP), P(FSDP, TP), P(FSDP, TP), P(FSDP, TP), P(TP, FSDP)),
        out_specs=(P(FSDP, TP), P(FSDP, TP), P(FSDP, TP), P(TP, FSDP)),
        check_vma=False,
    )
```

```python
import functools
import math

import jax
import jax.numpy as jnp
from jax import lax
from jax.experimental import pallas as pl
from jax.experimental.pallas import tpu as pltpu
from jax.sharding import Mesh
from jax.sharding import PartitionSpec as P

FSDP = ("z_hi", "y")
TP = ("z_lo", "x", "core")
MESH = pl.DeviceIdType.MESH
BF = jnp.bfloat16
F32 = jnp.float32
NSEND, NRECV = 48, 96
GROUP = 6
ZF = 64
HOME = 160
ROUNDS = ((0, 0, 0, 256), (0, 1, 0, 256), (1, 0, HOME, 256 - HOME), (1, 1, HOME, 256 - HOME))


def dot(a, b, ca, cb):
    return lax.dot_general(a, b, (((ca,), (cb,)), ((), ())), preferred_element_type=F32)


def kernel(factor, tok, og, wg, wu, wd, ig_o, gg_o, ug_o, dg_o,
           own, xb, wgu, wdn, pgu, ph, pgur, phr, agu, ah, igp, sibr, farr, nearr, fs, zfr, zr, igs, igr,
           ws, hs, gb, hb, gfr, hfr, gnr, hnr, lsem, ssem, rsem):
    R, C = tok.shape
    F = wg.shape[1]
    H = R // 2
    z_hi, y, z_lo, x, core = (lax.axis_index(a) for a in ("z_hi", "y", "z_lo", "x", "core"))
    inner = (z_hi - z_lo) * (z_hi - z_lo)
    is_inner, is_outer = inner == 1, inner == 0
    nx, ny = 4, 4
    xr, xl, xf = lax.rem(x + 1, nx), lax.rem(x + nx - 1, nx), lax.rem(x + 2, nx)
    yr, yl, yf = lax.rem(y + 1, ny), lax.rem(y + ny - 1, ny), lax.rem(y + 2, ny)
    oc = 1 - core
    t_of = (z_hi, 1 - z_hi)
    d_xr, d_xl = (z_hi, y, z_lo, xr, core), (z_hi, y, z_lo, xl, core)
    d_yr, d_yl = (z_hi, yr, z_lo, x, core), (z_hi, yl, z_lo, x, core)
    d_sib = (z_hi, y, z_lo, x, oc)
    d_zlo = (z_hi, y, 1 - z_lo, x, core)
    d_zhi = (1 - z_hi, y, z_lo, x, core)
    d_zz = (1 - z_hi, y, 1 - z_lo, x, core)
    d_zs = (z_lo, y, 1 - z_lo, x, core)
    partners = (d_xr, d_xl, d_yr, d_yl, d_sib, d_zlo, d_zhi, d_zz)

    sends, recvs = {}, {}

    def slot(table, name):
        return table.setdefault(name, len(table))

    for k in range(8):
        slot(recvs, ("z", k))
    for k in range(8):
        slot(recvs, ("zh", k))
    groups = []

    def size(ref):
        return math.prod(ref.shape) * jnp.dtype(ref.dtype).itemsize

    def unit_of(nbytes):
        k = nbytes // 16384
        if nbytes % 16384 == 0:
            for n in (8, 7, 6, 5, 4, 3, 2, 1):
                if k % n == 0 and k // n <= 2 * R // 16:
                    return n, 16 * (k // n)
        return None

    def wait_bytes(sem, nbytes):
        n, m = unit_of(nbytes)
        r = xb.at[0, pl.ds(0, n), pl.ds(0, m), :]
        pltpu.make_async_copy(r, r, sem).wait()

    def remote(src, dst, dev, i, j):
        return pltpu.make_async_remote_copy(
            src_ref=src, dst_ref=dst, send_sem=ssem.at[i], recv_sem=rsem.at[j],
            device_id=dev, device_id_type=MESH)

    def send(name, src, dst, dev, rs=None, wait_later=True):
        if wait_later:
            total = sum(groups[-1]) if groups else 0
            if not groups or ((len(groups[-1]) >= GROUP or total >= 1 << 21) and unit_of(total) is not None):
                groups.append([])
            groups[-1].append(size(src))
            i = slot(sends, ("group", len(groups) - 1))
        else:
            i = slot(sends, name)
        remote(src, dst, dev, i, slot(recvs, name) if rs is None else rs).start()

    def recv(name, *dsts):
        if len(dsts) == 1:
            remote(dsts[0], dsts[0], d_sib, 0, slot(recvs, name)).wait_recv()
        else:
            wait_bytes(rsem.at[slot(recvs, name)], sum(size(d) for d in dsts))

    def wait_send(name, src):
        remote(src, src, d_sib, slot(sends, name), 0).wait_send()

    def trow(t):
        return pl.ds(pl.multiple_of(t * R, R), R)

    def blk(a, xp, c, t):
        return xb.at[a, 2 * xp + c, trow(t), :]

    def rows(start, n):
        return pl.ds(pl.multiple_of(start, 16), n)

    def chunk(a, xp, t, h, r0, n):
        return xb.at[a, 2 * xp + core, rows(t * R + r0 + h * (n // 2), n // 2), :]

    def part(a, xp, c, t, r0, n):
        return xb.at[a, 2 * xp + c, rows(t * R + r0, n), :]

    home_at = (1 - inner) * z_hi * R + inner * 2 * R

    def home(xp, h=None):
        if h is None:
            return xb.at[1, 2 * xp + core, rows(home_at, HOME), :]
        return xb.at[1, 2 * xp + core, rows(home_at + h * (HOME // 2), HOME // 2), :]

    loads_w = [
        pltpu.make_async_copy(wg, wgu.at[y, :, pl.ds(0, F)], lsem.at[0]),
        pltpu.make_async_copy(wu, wgu.at[y, :, pl.ds(F, F)], lsem.at[1]),
        pltpu.make_async_copy(wd, wdn.at[y], lsem.at[2]),
    ]
    loads_t = [
        pltpu.make_async_copy(tok, own.at[0], lsem.at[3]),
        pltpu.make_async_copy(og, own.at[1], lsem.at[4]),
    ]
    for c in loads_t + loads_w:
        c.start()

    outer_loads = (
        (tok, blk(0, x, core, z_hi), lsem.at[5]),
        (og.at[pl.ds(HOME, R - HOME), :], part(1, x, core, z_hi, HOME, R - HOME), lsem.at[6]),
    )
    load_home = pltpu.make_async_copy(og.at[pl.ds(0, HOME), :], home(x), lsem.at[7])
    load_home.start()

    @pl.when(is_outer)
    def _():
        for c in outer_loads:
            pltpu.make_async_copy(*c).start()

    barrier = pltpu.get_barrier_semaphore()
    for d in partners:
        pl.semaphore_signal(barrier, inc=1, device_id=d, device_id_type=MESH)
    pl.semaphore_wait(barrier, len(partners))

    for c in loads_t:
        c.wait()
    load_home.wait()

    for a, rel, r0, n in (ROUNDS[0], ROUNDS[2]):
        for h in range(2):
            k = 2 * a + h
            send(("zs", k), own.at[a, pl.ds(r0 + h * (n // 2), n // 2), :], chunk(a, x, z_hi, h, r0, n), d_zs,
                 rs=4 * inner + k)

    @pl.when(is_outer)
    def _():
        for c in outer_loads:
            pltpu.make_async_copy(*c).wait()

    for c in loads_w:
        c.wait()

    def wchunk(which, yp, h):
        if which == 0:
            return wgu.at[yp, pl.ds(h * C, C), :]
        return wdn.at[yp, pl.ds(h * (F // 2), F // 2), :]

    def ysend(w):
        for h in range(2):
            send(("yf", w) if h else ("y", w, 0), wchunk(w, y, h), wchunk(w, y, h), d_yr)
            send(("yf", w) if h else ("y", w, 1), wchunk(w, y, 1 - h), wchunk(w, y, 1 - h), d_yl)

    def yfwd(w):
        recv(("y", w, 0), wchunk(w, yl, 0))
        send(("yf", w), wchunk(w, yl, 0), wchunk(w, yl, 0), d_yr)
        recv(("y", w, 1), wchunk(w, yr, 1))
        send(("yf", w), wchunk(w, yr, 1), wchunk(w, yr, 1), d_yl)

    def yfin(w):
        recv(("yf", w), wchunk(w, yl, 1), wchunk(w, yr, 0), wchunk(w, yf, 0), wchunk(w, yf, 1))

    def hsend():
        for h in range(2):
            send(("h", 0, h), home(x, h), home(x, h), d_xr)
            send(("h", 1, 1 - h), home(x, 1 - h), home(x, 1 - h), d_xl)

    def homez(j, xp):
        send(("hz", j), home(xp), xb.at[1, 2 * xp + core, rows(z_hi * R, HOME), :], d_zs, rs=8 + 4 * inner + j)

    def hfwd():
        recv(("h", 0, 0), home(xl, 0))
        send("hf", home(xl, 0), home(xl, 0), d_xr)
        recv(("h", 1, 1), home(xr, 1))
        send("hf", home(xr, 1), home(xr, 1), d_xl)

    def hfin_a():
        homez(0, x)
        recv(("h", 0, 1), home(xl, 1))
        homez(1, xl)
        recv(("h", 1, 0), home(xr, 0))
        homez(2, xr)

    def hfin_b():
        recv("hf", home(xf, 0), home(xf, 1))
        homez(3, xf)

    xorder = (x, xl, xr, xf)

    def hpart(rel, j):
        return part(1, xorder[j], core, t_of[rel], 0, HOME)

    def hsib(rel, j):
        send(("hs", rel, j), hpart(rel, j), hpart(rel, j), d_sib, rs=slot(recvs, ("hs", rel)), wait_later=False)

    def hz_inner(j):
        @pl.when(is_inner)
        def _():
            recv(("zh", 4 + j), hpart(1, j))
            send(("hzr", j), hpart(1, j), hpart(1, j), d_zlo, rs=12 + j, wait_later=False)
            hsib(1, j)
            recv(("zh", j), hpart(0, j))
            hsib(0, j)

    def hz_outer(j):
        @pl.when(is_outer)
        def _():
            recv(("zh", 4 + j), hpart(1, j))
            hsib(1, j)

    def hs_outer():
        @pl.when(is_outer)
        def _():
            for j in range(4):
                hsib(0, j)

    def hsfin(rel):
        recv(("hs", rel), *[part(1, xp, oc, t_of[rel], 0, HOME) for xp in xorder])

    def relay(r, hs=(0, 1)):
        a, rel, r0, n = ROUNDS[r]
        t = t_of[rel]
        for h in hs:
            k = 2 * a + h

            @pl.when(is_inner)
            def _():
                c = chunk(a, x, t, h, r0, n)
                recv(("z", 4 + k), c)
                send(("zr", k), c, c, d_zlo, rs=4 + k, wait_later=False)

    def xsend_h(r, h):
        a, rel, r0, n = ROUNDS[r]
        t = t_of[rel]
        k = 2 * a + h
        c = chunk(a, x, t, h, r0, n)
        if rel == 0:
            @pl.when(is_inner)
            def _():
                recv(("z", k), c)
        else:
            @pl.when(is_outer)
            def _():
                recv(("z", 4 + k), c)
        if h == 0:
            send(("x", r, 0, 0), c, c, d_xr)
        else:
            send(("x", r, 1, 1), c, c, d_xl)
            send(("x", r, 0, 1), c, c, d_xr)
            c = chunk(a, x, t, 0, r0, n)
            send(("x", r, 1, 0), c, c, d_xl)
            p = part(a, x, core, t, r0, n)
            send(("s", r), p, p, d_sib)

    def xsend(r):
        xsend_h(r, 0)
        xsend_h(r, 1)

    def xfwd(r):
        a, rel, r0, n = ROUNDS[r]
        t = t_of[rel]
        c = chunk(a, xl, t, 0, r0, n)
        recv(("x", r, 0, 0), c)
        send(("xf", r), c, c, d_xr)
        c = chunk(a, xr, t, 1, r0, n)
        recv(("x", r, 1, 1), c)
        send(("xf", r), c, c, d_xl)

    def xfin(r):
        a, rel, r0, n = ROUNDS[r]
        t = t_of[rel]
        recv(("x", r, 0, 1), chunk(a, xl, t, 1, r0, n))
        p = part(a, xl, core, t, r0, n)
        send(("s", r), p, p, d_sib)
        recv(("x", r, 1, 0), chunk(a, xr, t, 0, r0, n))
        p = part(a, xr, core, t, r0, n)
        send(("s", r), p, p, d_sib)
        recv(("xf", r), chunk(a, xf, t, 0, r0, n), chunk(a, xf, t, 1, r0, n))
        p = part(a, xf, core, t, r0, n)
        send(("s", r), p, p, d_sib)

    def sfin(r):
        a, rel, r0, n = ROUNDS[r]
        recv(("s", r), *[part(a, xp, oc, t_of[rel], r0, n) for xp in xorder])

    def forward(a, rel, r0, n):
        t = t_of[rel]
        terms = []
        for e in range(2 * nx):
            block = xb[a, e, rows(t * R + r0, n), :]
            cols = pl.ds((e % 2) * C, C)
            if a == 0:
                terms.append(dot(block, wgu[e // 2, cols, :], 1, 0))
            else:
                terms.append(dot(block, wdn[e // 2, :, cols], 1, 1))
        (pgu, ph)[a][rel, pl.ds(r0, n)] = functools.reduce(jnp.add, terms)

    REST = (HOME, R - HOME)

    hsend()
    ysend(0)
    xsend_h(0, 0)
    relay(1, (0,))
    hfwd()
    xsend_h(0, 1)
    relay(1, (1,))
    hfin_a()
    yfwd(0)
    ysend(1)
    relay(3)
    xfwd(0)
    xsend(2)
    xsend(1)
    xsend(3)
    hfin_b()
    hs_outer()
    hz_inner(0)
    hz_inner(1)
    xfin(0)
    xfwd(2)
    hz_inner(2)
    yfin(0)
    sfin(0)
    hz_inner(3)
    forward(0, 0, 0, R)
    send("ex", pgu.at[0], pgur, d_zhi)
    yfwd(1)
    xfwd(1)
    xfwd(3)
    xfin(2)
    sfin(2)
    hsfin(0)
    yfin(1)
    forward(1, 0, 0, R)
    send("ex", ph.at[0], phr, d_zhi)
    xfin(1)
    for j in range(4):
        hz_outer(j)
    xfin(3)
    sfin(1)
    forward(0, 1, 0, R)
    hsfin(1)
    forward(1, 1, 0, HOME)
    sfin(3)
    forward(1, 1, *REST)

    recv("ex", pgur, phr)
    gate = pgu[1, :, :F] + pgur[:, :F]
    up = pgu[1, :, F:] + pgur[:, F:]
    hg = ph[1] + phr[...]
    squashed = jax.nn.sigmoid(gate)
    activated = gate * squashed
    slope = squashed * (1.0 + gate * (1.0 - squashed))
    agu[trow(1 - z_hi), :F] = (hg * up * slope).astype(BF)
    agu[trow(1 - z_hi), F:] = (hg * activated).astype(BF)
    ah[trow(1 - z_hi), :] = (activated * up).astype(BF)
    send("act", agu.at[trow(1 - z_hi), :], agu.at[trow(1 - z_hi), :], d_zhi)
    send("act", ah.at[trow(1 - z_hi), :], ah.at[trow(1 - z_hi), :], d_zhi)

    order = (xf, xr, xl, x)
    RA = ((ZF, R - ZF), (0, ZF))

    def hrows(p, h):
        r0, n = RA[p]
        return pl.ds(r0 + h * (n // 2), n // 2)

    def arows(p):
        return pl.ds(*RA[p])

    def igblock(rel, xp, c):
        w = wgu[xp, pl.ds(pl.multiple_of(c * C, C), C), :]
        igp[rel, 2 * xp + c] = dot(agu[trow(t_of[rel]), :], w, 1, 1)

    def igstart(rel):
        for j, xp in enumerate(order):
            igblock(rel, xp, oc)
            send(("is", rel, j), igp.at[rel, 2 * xp + oc], sibr.at[rel, xp], d_sib)
        for xp in order:
            igblock(rel, xp, core)

    def addsib(rel, j):
        xp = order[j]
        recv(("is", rel, j), sibr.at[rel, xp])
        igp[rel, 2 * xp + core] += sibr[rel, xp]

    def zfirst(rel, j):
        xp = order[j]
        send(("zf", j), igp.at[rel, 2 * xp + core, arows(1), :], zfr.at[xp], d_zlo, wait_later=False)

    def igfar(p, rel, k):
        for h, d in enumerate((d_xr, d_xl)):
            fs[k, h, pl.ds(0, RA[p][1] // 2), :] = igp[rel, 2 * xf + core, hrows(p, h), :].astype(BF)
            n = pl.ds(0, RA[p][1] // 2)
            send(("if", k, h), fs.at[k, h, n, :], farr.at[k, h, n, :], d)

    def ignear(p, rel, k):
        for h, (xp, d) in enumerate(((xr, d_xr), (xl, d_xl))):
            send(("in", k), igp.at[rel, 2 * xp + core, hrows(p, 1 - h), :],
                 nearr.at[rel, h, hrows(p, 1 - h), :], d)

    def igsecond(p, rel, k):
        for h, (xp, d) in enumerate(((xr, d_xr), (xl, d_xl))):
            n = pl.ds(0, RA[p][1] // 2)
            recv(("if", k, h), farr.at[k, h, n, :])
            igp[rel, 2 * xp + core, hrows(p, h), :] += farr[k, h, n, :].astype(F32)
            send(("in", k), igp.at[rel, 2 * xp + core, hrows(p, h), :], nearr.at[rel, h, hrows(p, h), :], d)

    def iglast(p, rel, k):
        recv(("in", k), *[nearr.at[rel, h, hrows(p, g), :] for h in range(2) for g in range(2)])
        igp[rel, 2 * x + core, arows(p), :] += nearr[rel, 0, arows(p), :] + nearr[rel, 1, arows(p), :]

    def igfirst(rel, when):
        addsib(rel, 0)
        igfar(0, rel, rel)
        addsib(rel, 1)
        addsib(rel, 2)
        ignear(0, rel, rel)
        addsib(rel, 3)

        @pl.when(when)
        def _():
            for j in range(4):
                zfirst(rel, j)

    def wunit(e):
        g = dot(xb[0, e, : 2 * R], agu[...], 0, 0)
        ws[e] = g
        gb[e] = g.astype(BF)
        d = dot(ah[...], xb[1, e, : 2 * R], 0, 0)
        hs[e] = d
        hb[e] = d.astype(BF)

    sides = ((yr, d_yr), (yl, d_yl))
    def zsend(rel):
        for h in range(2):
            send(("zi", rel, h), igp.at[rel, 2 * x + core, hrows(0, h), :], zr.at[hrows(0, h), :], d_zlo,
                 rs=slot(recvs, ("zir", h)), wait_later=False)

    def wfirst(e, s, h):
        wunit(e)
        send("gn", gb.at[e], gnr.at[s, h], sides[s][1])
        send("gn", hb.at[e], hnr.at[s, h], sides[s][1])

    def zfadd(j):
        xp = order[j]
        recv(("zf", j), zfr.at[xp])
        igp[keep, 2 * xp + core, arows(1), :] += zfr[xp]

    def wsecond(h):
        yp, d = sides[h]
        recv(("gf", h), gfr.at[h], hfr.at[h])
        gb[2 * yp + h] = (ws[2 * yp + h] + gfr[h].astype(F32)).astype(BF)
        send("gn", gb.at[2 * yp + h], gnr.at[h, h], d)
        hb[2 * yp + h] = (hs[2 * yp + h] + hfr[h].astype(F32)).astype(BF)
        send("gn", hb.at[2 * yp + h], hnr.at[h, h], d)

    keep = inner
    igstart(1)
    igfirst(1, is_outer)
    recv("act", agu.at[trow(z_hi), :], ah.at[trow(z_hi), :])
    for h, (yp, d) in enumerate(sides):
        wunit(2 * yf + h)
        send(("gf", h), gb.at[2 * yf + h], gfr.at[h], d)
        send(("gf", h), hb.at[2 * yf + h], hfr.at[h], d)
    igsecond(0, 1, 1)
    igstart(0)
    igfirst(0, is_inner)
    for h, (yp, d) in enumerate(sides):
        wfirst(2 * yp + 1 - h, h, 1 - h)
    for h, (yp, d) in enumerate(sides):
        wunit(2 * yp + h)
    iglast(0, 1, 1)

    @pl.when(is_outer)
    def _():
        zsend(1)

    zfadd(0)
    igfar(1, keep, 2)
    wsecond(0)
    wsecond(1)
    igsecond(0, 0, 0)
    zfadd(1)
    zfadd(2)
    ignear(1, keep, 2)
    for h in range(2):
        wunit(2 * y + h)
    igsecond(1, keep, 2)
    iglast(0, 0, 0)

    @pl.when(is_inner)
    def _():
        zsend(0)
        n = pl.ds(0, (R - ZF) // 2)
        for h in range(2):
            recv(("zir", h), zr.at[hrows(0, h), :])
            igs[h, n, :] = (igp[1, 2 * x + core, hrows(0, h), :] + zr[hrows(0, h), :]).astype(BF)
            send(("zo", h), igs.at[h, n, :], igr.at[h, n, :], d_zz, wait_later=False)

    zfadd(3)
    iglast(1, keep, 2)

    @pl.when(is_inner)
    def _():
        igs[2, pl.ds(0, ZF), :] = igp[1, 2 * x + core, arows(1), :].astype(BF)
        send(("zo", 2), igs.at[2, pl.ds(0, ZF), :], igr.at[2, pl.ds(0, ZF), :], d_zz, wait_later=False)

    @pl.when(is_outer)
    def _():
        ig_o[arows(1), :] = igp[0, 2 * x + core, arows(1), :].astype(BF)

    recv("gn", *[b.at[s, h] for b in (gnr, hnr) for s in range(2) for h in range(2)])
    for h in range(2):
        g = (ws[2 * y + h] + gnr[0, h].astype(F32) + gnr[1, h].astype(F32)) * factor
        gg_o[pl.ds(h * C, C), :] = g[:, :F]
        ug_o[pl.ds(h * C, C), :] = g[:, F:]
        dg_o[:, pl.ds(h * C, C)] = (hs[2 * y + h] + hnr[0, h].astype(F32) + hnr[1, h].astype(F32)) * factor

    @pl.when(is_outer)
    def _():
        for h in range(2):
            recv(("zir", h), zr.at[hrows(0, h), :])
            ig_o[hrows(0, h), :] = (igp[0, 2 * x + core, hrows(0, h), :] + zr[hrows(0, h), :]).astype(BF)

    @pl.when(is_inner)
    def _():
        zs, n = pl.ds(0, ZF), pl.ds(0, (R - ZF) // 2)
        recv(("zo", 2), igr.at[2, zs, :])
        ig_o[arows(1), :] = igr[2, zs, :]
        for h in range(2):
            recv(("zo", h), igr.at[h, n, :])
            ig_o[hrows(0, h), :] = igr[h, n, :]
        wait_send(("zo", 2), igs.at[2, zs, :])
        for h in range(2):
            wait_send(("zo", h), igs.at[h, n, :])
            wait_send(("zi", 0, h), zr.at[hrows(0, h), :])
        for r in (1, 3):
            a, rel, r0, n = ROUNDS[r]
            for h in range(2):
                wait_send(("zr", 2 * a + h), chunk(a, x, t_of[1], h, r0, n))
        for j in range(4):
            wait_send(("hzr", j), hpart(1, j))

    @pl.when(is_outer)
    def _():
        for h in range(2):
            wait_send(("zi", 1, h), zr.at[hrows(0, h), :])

    for j in range(4):
        wait_send(("zf", j), zfr.at[j])
        for rel in range(2):
            wait_send(("hs", rel, j), hpart(rel, j))
    for k, sizes in enumerate(groups):
        wait_bytes(ssem.at[slot(sends, ("group", k))], sum(sizes))
    assert len(sends) <= NSEND and len(recvs) <= NRECV, (len(sends), len(recvs))


def deliver(*refs):
    n = (len(refs) - 1) // 2
    copies = [pltpu.make_async_copy(refs[k], refs[n + k], refs[-1].at[k]) for k in range(n)]
    for c in copies:
        c.start()
    for c in copies:
        c.wait()


def shards(tokens, out_grad, gate_weight, up_weight, down_weight):
    R, C = tokens.shape
    F = gate_weight.shape[1]
    H = R // 2
    factor = 1.0 / math.sqrt(R * lax.axis_size(FSDP))
    anyspec = pl.BlockSpec(memory_space=pl.ANY)
    vm = pl.BlockSpec(memory_space=pltpu.VMEM)
    V = pltpu.VMEM
    scratch = [
        V((2, R, C), BF), V((2, 8, 2 * R + HOME, C), BF), V((4, 2 * C, 2 * F), BF), V((4, F, 2 * C), BF),
        V((2, R, 2 * F), F32), V((2, R, F), F32), V((R, 2 * F), F32), V((R, F), F32),
        V((2 * R, 2 * F), BF), V((2 * R, F), BF),
        V((2, 8, R, C), F32), V((2, 4, R, C), F32), V((3, 2, H, C), BF), V((2, 2, R, C), F32), V((3, 2, H, C), BF), V((4, ZF, C), F32),
        V((R, C), F32), V((3, H, C), BF), V((3, H, C), BF),
        V((8, C, 2 * F), F32), V((8, F, C), F32), V((8, C, 2 * F), BF), V((8, F, C), BF),
        V((2, C, 2 * F), BF), V((2, F, C), BF), V((2, 2, C, 2 * F), BF), V((2, 2, F, C), BF),
        pltpu.SemaphoreType.DMA((8,)), pltpu.SemaphoreType.DMA((NSEND,)), pltpu.SemaphoreType.DMA((NRECV,)),
    ]
    held = pl.pallas_call(
        functools.partial(kernel, factor),
        out_shape=(
            V((R, C), BF),
            V((2 * C, F), F32),
            V((2 * C, F), F32),
            V((F, 2 * C), F32),
        ),
        in_specs=[anyspec] * 5,
        out_specs=(vm,) * 4,
        scratch_shapes=scratch,
        compiler_params=pltpu.CompilerParams(
            collective_id=0, has_side_effects=True, vmem_limit_bytes=60 * 1024 * 1024),
        name="ffn_backward",
    )(tokens, out_grad, gate_weight, up_weight, down_weight)
    return pl.pallas_call(
        deliver,
        out_shape=tuple(jax.ShapeDtypeStruct(a.shape, a.dtype) for a in held),
        in_specs=[vm] * len(held),
        out_specs=(anyspec,) * len(held),
        scratch_shapes=[pltpu.SemaphoreType.DMA((len(held),))],
        name="deliver",
    )(*[pltpu.with_memory_space_constraint(a, pltpu.VMEM) for a in held])


def solution(mesh):
    finer = Mesh(mesh.devices.reshape(2, 4, 2, 4, 2), ("z_hi", "y", "z_lo", "x", "core"))
    return jax.shard_map(
        shards,
        mesh=finer,
        in_specs=(P(FSDP, TP), P(FSDP, TP), P(FSDP, TP), P(FSDP, TP), P(TP, FSDP)),
        out_specs=(P(FSDP, TP), P(FSDP, TP), P(FSDP, TP), P(TP, FSDP)),
        check_vma=False,
    )
```

```python
import functools
import math

import jax
import jax.numpy as jnp
from jax import lax
from jax.experimental import pallas as pl
from jax.experimental.pallas import tpu as pltpu
from jax.sharding import Mesh
from jax.sharding import PartitionSpec as P

FSDP = ("z_hi", "y")
TP = ("z_lo", "x", "core")
MESH = pl.DeviceIdType.MESH
BF = jnp.bfloat16
F32 = jnp.float32
NSEND, NRECV = 48, 96
GROUP = 6
ROUNDED = (0, 1, 2)
ZF = 64
HOME = 160
ROUNDS = ((0, 0, 0, 256), (0, 1, 0, 256), (1, 0, HOME, 256 - HOME), (1, 1, HOME, 256 - HOME))


def dot(a, b, ca, cb):
    return lax.dot_general(a, b, (((ca,), (cb,)), ((), ())), preferred_element_type=F32)


def kernel(factor, tok, og, wg, wu, wd, ig_o, gg_o, ug_o, dg_o,
           own, xb, wgu, wdn, pgu, ph, pgur, phr, agu, ah, igp, sibr, farr, nearr, fs, ns, nowr, zfr, zr, igs, igr,
           ws, hs, gb, hb, gfr, hfr, gnr, hnr, lsem, ssem, rsem):
    R, C = tok.shape
    F = wg.shape[1]
    H = R // 2
    z_hi, y, z_lo, x, core = (lax.axis_index(a) for a in ("z_hi", "y", "z_lo", "x", "core"))
    inner = (z_hi - z_lo) * (z_hi - z_lo)
    is_inner, is_outer = inner == 1, inner == 0
    nx, ny = 4, 4
    xr, xl, xf = lax.rem(x + 1, nx), lax.rem(x + nx - 1, nx), lax.rem(x + 2, nx)
    yr, yl, yf = lax.rem(y + 1, ny), lax.rem(y + ny - 1, ny), lax.rem(y + 2, ny)
    oc = 1 - core
    t_of = (z_hi, 1 - z_hi)
    d_xr, d_xl = (z_hi, y, z_lo, xr, core), (z_hi, y, z_lo, xl, core)
    d_yr, d_yl = (z_hi, yr, z_lo, x, core), (z_hi, yl, z_lo, x, core)
    d_sib = (z_hi, y, z_lo, x, oc)
    d_zlo = (z_hi, y, 1 - z_lo, x, core)
    d_zhi = (1 - z_hi, y, z_lo, x, core)
    d_zz = (1 - z_hi, y, 1 - z_lo, x, core)
    d_zs = (z_lo, y, 1 - z_lo, x, core)
    partners = (d_xr, d_xl, d_yr, d_yl, d_sib, d_zlo, d_zhi, d_zz)

    sends, recvs = {}, {}

    def slot(table, name):
        return table.setdefault(name, len(table))

    for k in range(8):
        slot(recvs, ("z", k))
    for k in range(8):
        slot(recvs, ("zh", k))
    groups = []

    def size(ref):
        return math.prod(ref.shape) * jnp.dtype(ref.dtype).itemsize

    def unit_of(nbytes):
        k = nbytes // 16384
        if nbytes % 16384 == 0:
            for n in (8, 7, 6, 5, 4, 3, 2, 1):
                if k % n == 0 and k // n <= 2 * R // 16:
                    return n, 16 * (k // n)
        return None

    def wait_bytes(sem, nbytes):
        n, m = unit_of(nbytes)
        r = xb.at[0, pl.ds(0, n), pl.ds(0, m), :]
        pltpu.make_async_copy(r, r, sem).wait()

    def remote(src, dst, dev, i, j):
        return pltpu.make_async_remote_copy(
            src_ref=src, dst_ref=dst, send_sem=ssem.at[i], recv_sem=rsem.at[j],
            device_id=dev, device_id_type=MESH)

    def send(name, src, dst, dev, rs=None, wait_later=True):
        if wait_later:
            total = sum(groups[-1]) if groups else 0
            if not groups or ((len(groups[-1]) >= GROUP or total >= 1 << 21) and unit_of(total) is not None):
                groups.append([])
            groups[-1].append(size(src))
            i = slot(sends, ("group", len(groups) - 1))
        else:
            i = slot(sends, name)
        remote(src, dst, dev, i, slot(recvs, name) if rs is None else rs).start()

    def recv(name, *dsts):
        if len(dsts) == 1:
            remote(dsts[0], dsts[0], d_sib, 0, slot(recvs, name)).wait_recv()
        else:
            wait_bytes(rsem.at[slot(recvs, name)], sum(size(d) for d in dsts))

    def wait_send(name, src):
        remote(src, src, d_sib, slot(sends, name), 0).wait_send()

    def trow(t):
        return pl.ds(pl.multiple_of(t * R, R), R)

    def blk(a, xp, c, t):
        return xb.at[a, 2 * xp + c, trow(t), :]

    def rows(start, n):
        return pl.ds(pl.multiple_of(start, 16), n)

    def chunk(a, xp, t, h, r0, n):
        return xb.at[a, 2 * xp + core, rows(t * R + r0 + h * (n // 2), n // 2), :]

    def part(a, xp, c, t, r0, n):
        return xb.at[a, 2 * xp + c, rows(t * R + r0, n), :]

    home_at = (1 - inner) * z_hi * R + inner * 2 * R

    def home(xp, h=None):
        if h is None:
            return xb.at[1, 2 * xp + core, rows(home_at, HOME), :]
        return xb.at[1, 2 * xp + core, rows(home_at + h * (HOME // 2), HOME // 2), :]

    loads_w = [
        pltpu.make_async_copy(wg, wgu.at[y, :, pl.ds(0, F)], lsem.at[0]),
        pltpu.make_async_copy(wu, wgu.at[y, :, pl.ds(F, F)], lsem.at[1]),
        pltpu.make_async_copy(wd, wdn.at[y], lsem.at[2]),
    ]
    loads_t = [
        pltpu.make_async_copy(tok, own.at[0], lsem.at[3]),
        pltpu.make_async_copy(og, own.at[1], lsem.at[4]),
    ]
    for c in loads_t + loads_w:
        c.start()

    outer_loads = (
        (tok, blk(0, x, core, z_hi), lsem.at[5]),
        (og.at[pl.ds(HOME, R - HOME), :], part(1, x, core, z_hi, HOME, R - HOME), lsem.at[6]),
    )
    load_home = pltpu.make_async_copy(og.at[pl.ds(0, HOME), :], home(x), lsem.at[7])
    load_home.start()

    @pl.when(is_outer)
    def _():
        for c in outer_loads:
            pltpu.make_async_copy(*c).start()

    barrier = pltpu.get_barrier_semaphore()
    for d in partners:
        pl.semaphore_signal(barrier, inc=1, device_id=d, device_id_type=MESH)
    pl.semaphore_wait(barrier, len(partners))

    for c in loads_t:
        c.wait()
    load_home.wait()

    for a, rel, r0, n in (ROUNDS[0], ROUNDS[2]):
        for h in range(2):
            k = 2 * a + h
            send(("zs", k), own.at[a, pl.ds(r0 + h * (n // 2), n // 2), :], chunk(a, x, z_hi, h, r0, n), d_zs,
                 rs=4 * inner + k)

    @pl.when(is_outer)
    def _():
        for c in outer_loads:
            pltpu.make_async_copy(*c).wait()

    for c in loads_w:
        c.wait()

    def wchunk(which, yp, h):
        if which == 0:
            return wgu.at[yp, pl.ds(h * C, C), :]
        return wdn.at[yp, pl.ds(h * (F // 2), F // 2), :]

    def ysend(w):
        for h in range(2):
            send(("yf", w) if h else ("y", w, 0), wchunk(w, y, h), wchunk(w, y, h), d_yr)
            send(("yf", w) if h else ("y", w, 1), wchunk(w, y, 1 - h), wchunk(w, y, 1 - h), d_yl)

    def yfwd(w):
        recv(("y", w, 0), wchunk(w, yl, 0))
        send(("yf", w), wchunk(w, yl, 0), wchunk(w, yl, 0), d_yr)
        recv(("y", w, 1), wchunk(w, yr, 1))
        send(("yf", w), wchunk(w, yr, 1), wchunk(w, yr, 1), d_yl)

    def yfin(w):
        recv(("yf", w), wchunk(w, yl, 1), wchunk(w, yr, 0), wchunk(w, yf, 0), wchunk(w, yf, 1))

    def hsend():
        for h in range(2):
            send(("h", 0, h), home(x, h), home(x, h), d_xr)
            send(("h", 1, 1 - h), home(x, 1 - h), home(x, 1 - h), d_xl)

    def homez(j, xp):
        send(("hz", j), home(xp), xb.at[1, 2 * xp + core, rows(z_hi * R, HOME), :], d_zs, rs=8 + 4 * inner + j)

    def hfwd():
        recv(("h", 0, 0), home(xl, 0))
        send("hf", home(xl, 0), home(xl, 0), d_xr)
        recv(("h", 1, 1), home(xr, 1))
        send("hf", home(xr, 1), home(xr, 1), d_xl)

    def hfin_a():
        homez(0, x)
        recv(("h", 0, 1), home(xl, 1))
        homez(1, xl)
        recv(("h", 1, 0), home(xr, 0))
        homez(2, xr)

    def hfin_b():
        recv("hf", home(xf, 0), home(xf, 1))
        homez(3, xf)

    xorder = (x, xl, xr, xf)

    def hpart(rel, j):
        return part(1, xorder[j], core, t_of[rel], 0, HOME)

    def hsib(rel, j):
        send(("hs", rel, j), hpart(rel, j), hpart(rel, j), d_sib, rs=slot(recvs, ("hs", rel)), wait_later=False)

    def hz_inner(j):
        @pl.when(is_inner)
        def _():
            recv(("zh", 4 + j), hpart(1, j))
            send(("hzr", j), hpart(1, j), hpart(1, j), d_zlo, rs=12 + j, wait_later=False)
            hsib(1, j)
            recv(("zh", j), hpart(0, j))
            hsib(0, j)

    def hz_outer(j):
        @pl.when(is_outer)
        def _():
            recv(("zh", 4 + j), hpart(1, j))
            hsib(1, j)

    def hs_outer():
        @pl.when(is_outer)
        def _():
            for j in range(4):
                hsib(0, j)

    def hsfin(rel):
        recv(("hs", rel), *[part(1, xp, oc, t_of[rel], 0, HOME) for xp in xorder])

    def relay(r, hs=(0, 1)):
        a, rel, r0, n = ROUNDS[r]
        t = t_of[rel]
        for h in hs:
            k = 2 * a + h

            @pl.when(is_inner)
            def _():
                c = chunk(a, x, t, h, r0, n)
                recv(("z", 4 + k), c)
                send(("zr", k), c, c, d_zlo, rs=4 + k, wait_later=False)

    def xsend_h(r, h):
        a, rel, r0, n = ROUNDS[r]
        t = t_of[rel]
        k = 2 * a + h
        c = chunk(a, x, t, h, r0, n)
        if rel == 0:
            @pl.when(is_inner)
            def _():
                recv(("z", k), c)
        else:
            @pl.when(is_outer)
            def _():
                recv(("z", 4 + k), c)
        if h == 0:
            send(("x", r, 0, 0), c, c, d_xr)
        else:
            send(("x", r, 1, 1), c, c, d_xl)
            send(("x", r, 0, 1), c, c, d_xr)
            c = chunk(a, x, t, 0, r0, n)
            send(("x", r, 1, 0), c, c, d_xl)
            p = part(a, x, core, t, r0, n)
            send(("s", r), p, p, d_sib)

    def xsend(r):
        xsend_h(r, 0)
        xsend_h(r, 1)

    def xfwd(r):
        a, rel, r0, n = ROUNDS[r]
        t = t_of[rel]
        c = chunk(a, xl, t, 0, r0, n)
        recv(("x", r, 0, 0), c)
        send(("xf", r), c, c, d_xr)
        c = chunk(a, xr, t, 1, r0, n)
        recv(("x", r, 1, 1), c)
        send(("xf", r), c, c, d_xl)

    def xfin(r):
        a, rel, r0, n = ROUNDS[r]
        t = t_of[rel]
        recv(("x", r, 0, 1), chunk(a, xl, t, 1, r0, n))
        p = part(a, xl, core, t, r0, n)
        send(("s", r), p, p, d_sib)
        recv(("x", r, 1, 0), chunk(a, xr, t, 0, r0, n))
        p = part(a, xr, core, t, r0, n)
        send(("s", r), p, p, d_sib)
        recv(("xf", r), chunk(a, xf, t, 0, r0, n), chunk(a, xf, t, 1, r0, n))
        p = part(a, xf, core, t, r0, n)
        send(("s", r), p, p, d_sib)

    def sfin(r):
        a, rel, r0, n = ROUNDS[r]
        recv(("s", r), *[part(a, xp, oc, t_of[rel], r0, n) for xp in xorder])

    def forward(a, rel, r0, n):
        t = t_of[rel]
        terms = []
        for e in range(2 * nx):
            block = xb[a, e, rows(t * R + r0, n), :]
            cols = pl.ds((e % 2) * C, C)
            if a == 0:
                terms.append(dot(block, wgu[e // 2, cols, :], 1, 0))
            else:
                terms.append(dot(block, wdn[e // 2, :, cols], 1, 1))
        (pgu, ph)[a][rel, pl.ds(r0, n)] = functools.reduce(jnp.add, terms)

    REST = (HOME, R - HOME)

    def gate_up():
        return pgu[1, :, :F] + pgur[:, :F], pgu[1, :, F:] + pgur[:, F:]

    hsend()
    ysend(0)
    xsend_h(0, 0)
    relay(1, (0,))
    hfwd()
    xsend_h(0, 1)
    relay(1, (1,))
    hfin_a()
    yfwd(0)
    ysend(1)
    relay(3)
    xfwd(0)
    xsend(2)
    xsend(1)
    xsend(3)
    hfin_b()
    hs_outer()
    hz_inner(0)
    hz_inner(1)
    xfin(0)
    xfwd(2)
    hz_inner(2)
    yfin(0)
    sfin(0)
    hz_inner(3)
    forward(0, 0, 0, R)
    send("exg", pgu.at[0], pgur, d_zhi)
    yfwd(1)
    xfwd(1)
    xfwd(3)
    xfin(2)
    sfin(2)
    hsfin(0)
    yfin(1)
    forward(1, 0, 0, R)
    send("exh", ph.at[0], phr, d_zhi)
    xfin(1)
    for j in range(4):
        hz_outer(j)
    xfin(3)
    sfin(1)
    forward(0, 1, 0, R)
    recv("exg", pgur)
    mine, away = trow(1 - z_hi), trow(z_hi)
    gate, up = gate_up()
    ah[mine, :] = (gate * jax.nn.sigmoid(gate) * up).astype(BF)
    send("acth", ah.at[mine, :], ah.at[mine, :], d_zhi)
    hsfin(1)
    forward(1, 1, 0, HOME)
    sfin(3)
    forward(1, 1, *REST)

    recv("exh", phr)
    gate, up = gate_up()
    hg = ph[1] + phr[...]
    squashed = jax.nn.sigmoid(gate)
    activated = gate * squashed
    slope = squashed * (1.0 + gate * (1.0 - squashed))
    agu[mine, :F] = (hg * up * slope).astype(BF)
    agu[mine, F:] = (hg * activated).astype(BF)
    send("actg", agu.at[mine, :], agu.at[mine, :], d_zhi)

    order = (xf, xr, xl, x)
    RA = ((ZF, R - ZF), (0, ZF))

    def hrows(p, h):
        r0, n = RA[p]
        return pl.ds(r0 + h * (n // 2), n // 2)

    def arows(p):
        return pl.ds(*RA[p])

    def igblock(rel, xp, c):
        w = wgu[xp, pl.ds(pl.multiple_of(c * C, C), C), :]
        igp[rel, 2 * xp + c] = dot(agu[trow(t_of[rel]), :], w, 1, 1)

    def igstart(rel):
        for j, xp in enumerate(order):
            igblock(rel, xp, oc)
            send(("is", rel, j), igp.at[rel, 2 * xp + oc], sibr.at[rel, xp], d_sib)
        for xp in order:
            igblock(rel, xp, core)

    def addsib(rel, j):
        xp = order[j]
        recv(("is", rel, j), sibr.at[rel, xp])
        igp[rel, 2 * xp + core] += sibr[rel, xp]

    def zfirst(rel, j):
        xp = order[j]
        send(("zf", j), igp.at[rel, 2 * xp + core, arows(1), :], zfr.at[xp], d_zlo, wait_later=False)

    def igfar(p, rel, k):
        for h, d in enumerate((d_xr, d_xl)):
            fs[k, h, pl.ds(0, RA[p][1] // 2), :] = igp[rel, 2 * xf + core, hrows(p, h), :].astype(BF)
            n = pl.ds(0, RA[p][1] // 2)
            send(("if", k, h), fs.at[k, h, n, :], farr.at[k, h, n, :], d)

    def ignear(p, rel, k):
        n = pl.ds(0, RA[p][1] // 2)
        for h, (xp, d) in enumerate(((xr, d_xr), (xl, d_xl))):
            rows_h = hrows(p, 1 - h)
            if k in ROUNDED:
                ns[k, h, n, :] = igp[rel, 2 * xp + core, rows_h, :].astype(BF)
                send(("in", k), ns.at[k, h, n, :], nowr.at[k, h, n, :], d)
            else:
                send(("in", k), igp.at[rel, 2 * xp + core, rows_h, :], nearr.at[rel, h, rows_h, :], d)

    def igsecond(p, rel, k):
        for h, (xp, d) in enumerate(((xr, d_xr), (xl, d_xl))):
            n = pl.ds(0, RA[p][1] // 2)
            recv(("if", k, h), farr.at[k, h, n, :])
            igp[rel, 2 * xp + core, hrows(p, h), :] += farr[k, h, n, :].astype(F32)
            send(("in", k), igp.at[rel, 2 * xp + core, hrows(p, h), :], nearr.at[rel, h, hrows(p, h), :], d)

    def iglast(p, rel, k):
        n = pl.ds(0, RA[p][1] // 2)
        first = [nowr.at[k, h, n, :] if k in ROUNDED else nearr.at[rel, h, hrows(p, 1 - h), :] for h in range(2)]
        second = [nearr.at[rel, h, hrows(p, h), :] for h in range(2)]
        recv(("in", k), *first, *second)
        for h in range(2):
            igp[rel, 2 * x + core, hrows(p, h), :] += second[h][...] + first[1 - h][...].astype(F32)

    def igfirst(rel, when):
        addsib(rel, 0)
        igfar(0, rel, rel)
        addsib(rel, 1)
        addsib(rel, 2)
        ignear(0, rel, rel)
        addsib(rel, 3)

        @pl.when(when)
        def _():
            for j in range(4):
                zfirst(rel, j)

    def gunit(e):
        g = dot(xb[0, e, : 2 * R], agu[...], 0, 0)
        ws[e] = g
        gb[e] = g.astype(BF)

    def hunit(e):
        d = dot(ah[...], xb[1, e, : 2 * R], 0, 0)
        hs[e] = d
        hb[e] = d.astype(BF)

    sides = ((yr, d_yr), (yl, d_yl))
    def zsend(rel):
        for h in range(2):
            send(("zi", rel, h), igp.at[rel, 2 * x + core, hrows(0, h), :], zr.at[hrows(0, h), :], d_zlo,
                 rs=slot(recvs, ("zir", h)), wait_later=False)

    def zfadd(j):
        xp = order[j]
        recv(("zf", j), zfr.at[xp])
        igp[keep, 2 * xp + core, arows(1), :] += zfr[xp]

    def hsecond(h):
        yp, d = sides[h]
        recv(("hf", h), hfr.at[h])
        hb[2 * yp + h] = (hs[2 * yp + h] + hfr[h].astype(F32)).astype(BF)
        send("gn", hb.at[2 * yp + h], hnr.at[h, h], d)

    def gsecond(h):
        yp, d = sides[h]
        recv(("gf", h), gfr.at[h])
        gb[2 * yp + h] = (ws[2 * yp + h] + gfr[h].astype(F32)).astype(BF)
        send("gn", gb.at[2 * yp + h], gnr.at[h, h], d)

    keep = inner
    igstart(1)
    recv("acth", ah.at[away, :])
    for h, (yp, d) in enumerate(sides):
        hunit(2 * yf + h)
        send(("hf", h), hb.at[2 * yf + h], hfr.at[h], d)
    igfirst(1, is_outer)
    for h, (yp, d) in enumerate(sides):
        hunit(2 * yp + 1 - h)
        send("gn", hb.at[2 * yp + 1 - h], hnr.at[h, 1 - h], d)
    recv("actg", agu.at[away, :])
    for h, (yp, d) in enumerate(sides):
        gunit(2 * yf + h)
        send(("gf", h), gb.at[2 * yf + h], gfr.at[h], d)
    igsecond(0, 1, 1)
    igstart(0)
    for h, (yp, d) in enumerate(sides):
        hunit(2 * yp + h)
    igfirst(0, is_inner)
    for h, (yp, d) in enumerate(sides):
        gunit(2 * yp + 1 - h)
        send("gn", gb.at[2 * yp + 1 - h], gnr.at[h, 1 - h], d)
    for h in range(2):
        hsecond(h)
    for h, (yp, d) in enumerate(sides):
        gunit(2 * yp + h)
    iglast(0, 1, 1)

    @pl.when(is_outer)
    def _():
        zsend(1)

    zfadd(0)
    igfar(1, keep, 2)
    gsecond(0)
    gsecond(1)
    igsecond(0, 0, 0)
    zfadd(1)
    zfadd(2)
    ignear(1, keep, 2)
    for h in range(2):
        gunit(2 * y + h)
        hunit(2 * y + h)
    igsecond(1, keep, 2)
    iglast(0, 0, 0)

    @pl.when(is_inner)
    def _():
        zsend(0)
        n = pl.ds(0, (R - ZF) // 2)
        for h in range(2):
            recv(("zir", h), zr.at[hrows(0, h), :])
            igs[h, n, :] = (igp[1, 2 * x + core, hrows(0, h), :] + zr[hrows(0, h), :]).astype(BF)
            send(("zo", h), igs.at[h, n, :], igr.at[h, n, :], d_zz, wait_later=False)

    zfadd(3)
    iglast(1, keep, 2)

    @pl.when(is_inner)
    def _():
        igs[2, pl.ds(0, ZF), :] = igp[1, 2 * x + core, arows(1), :].astype(BF)
        send(("zo", 2), igs.at[2, pl.ds(0, ZF), :], igr.at[2, pl.ds(0, ZF), :], d_zz, wait_later=False)

    @pl.when(is_outer)
    def _():
        ig_o[arows(1), :] = igp[0, 2 * x + core, arows(1), :].astype(BF)

    recv("gn", *[b.at[s, h] for b in (gnr, hnr) for s in range(2) for h in range(2)])
    for h in range(2):
        g = (ws[2 * y + h] + gnr[0, h].astype(F32) + gnr[1, h].astype(F32)) * factor
        gg_o[pl.ds(h * C, C), :] = g[:, :F]
        ug_o[pl.ds(h * C, C), :] = g[:, F:]
        dg_o[:, pl.ds(h * C, C)] = (hs[2 * y + h] + hnr[0, h].astype(F32) + hnr[1, h].astype(F32)) * factor

    @pl.when(is_outer)
    def _():
        for h in range(2):
            recv(("zir", h), zr.at[hrows(0, h), :])
            ig_o[hrows(0, h), :] = (igp[0, 2 * x + core, hrows(0, h), :] + zr[hrows(0, h), :]).astype(BF)

    @pl.when(is_inner)
    def _():
        zs, n = pl.ds(0, ZF), pl.ds(0, (R - ZF) // 2)
        recv(("zo", 2), igr.at[2, zs, :])
        ig_o[arows(1), :] = igr[2, zs, :]
        for h in range(2):
            recv(("zo", h), igr.at[h, n, :])
            ig_o[hrows(0, h), :] = igr[h, n, :]
        wait_send(("zo", 2), igs.at[2, zs, :])
        for h in range(2):
            wait_send(("zo", h), igs.at[h, n, :])
            wait_send(("zi", 0, h), zr.at[hrows(0, h), :])
        for r in (1, 3):
            a, rel, r0, n = ROUNDS[r]
            for h in range(2):
                wait_send(("zr", 2 * a + h), chunk(a, x, t_of[1], h, r0, n))
        for j in range(4):
            wait_send(("hzr", j), hpart(1, j))

    @pl.when(is_outer)
    def _():
        for h in range(2):
            wait_send(("zi", 1, h), zr.at[hrows(0, h), :])

    for j in range(4):
        wait_send(("zf", j), zfr.at[j])
        for rel in range(2):
            wait_send(("hs", rel, j), hpart(rel, j))
    for k, sizes in enumerate(groups):
        wait_bytes(ssem.at[slot(sends, ("group", k))], sum(sizes))
    assert len(sends) <= NSEND and len(recvs) <= NRECV, (len(sends), len(recvs))


def deliver(*refs):
    n = (len(refs) - 1) // 2
    copies = [pltpu.make_async_copy(refs[k], refs[n + k], refs[-1].at[k]) for k in range(n)]
    for c in copies:
        c.start()
    for c in copies:
        c.wait()


def shards(tokens, out_grad, gate_weight, up_weight, down_weight):
    R, C = tokens.shape
    F = gate_weight.shape[1]
    H = R // 2
    factor = 1.0 / math.sqrt(R * lax.axis_size(FSDP))
    anyspec = pl.BlockSpec(memory_space=pl.ANY)
    vm = pl.BlockSpec(memory_space=pltpu.VMEM)
    V = pltpu.VMEM
    scratch = [
        V((2, R, C), BF), V((2, 8, 2 * R + HOME, C), BF), V((4, 2 * C, 2 * F), BF), V((4, F, 2 * C), BF),
        V((2, R, 2 * F), F32), V((2, R, F), F32), V((R, 2 * F), F32), V((R, F), F32),
        V((2 * R, 2 * F), BF), V((2 * R, F), BF),
        V((2, 8, R, C), F32), V((2, 4, R, C), F32), V((3, 2, H, C), BF), V((2, 2, R, C), F32), V((3, 2, H, C), BF), V((3, 2, H, C), BF), V((3, 2, H, C), BF), V((4, ZF, C), F32),
        V((R, C), F32), V((3, H, C), BF), V((3, H, C), BF),
        V((8, C, 2 * F), F32), V((8, F, C), F32), V((8, C, 2 * F), BF), V((8, F, C), BF),
        V((2, C, 2 * F), BF), V((2, F, C), BF), V((2, 2, C, 2 * F), BF), V((2, 2, F, C), BF),
        pltpu.SemaphoreType.DMA((8,)), pltpu.SemaphoreType.DMA((NSEND,)), pltpu.SemaphoreType.DMA((NRECV,)),
    ]
    held = pl.pallas_call(
        functools.partial(kernel, factor),
        out_shape=(
            V((R, C), BF),
            V((2 * C, F), F32),
            V((2 * C, F), F32),
            V((F, 2 * C), F32),
        ),
        in_specs=[anyspec] * 5,
        out_specs=(vm,) * 4,
        scratch_shapes=scratch,
        compiler_params=pltpu.CompilerParams(
            collective_id=0, has_side_effects=True, vmem_limit_bytes=60 * 1024 * 1024),
        name="ffn_backward",
    )(tokens, out_grad, gate_weight, up_weight, down_weight)
    return pl.pallas_call(
        deliver,
        out_shape=tuple(jax.ShapeDtypeStruct(a.shape, a.dtype) for a in held),
        in_specs=[vm] * len(held),
        out_specs=(anyspec,) * len(held),
        scratch_shapes=[pltpu.SemaphoreType.DMA((len(held),))],
        name="deliver",
    )(*[pltpu.with_memory_space_constraint(a, pltpu.VMEM) for a in held])


def solution(mesh):
    finer = Mesh(mesh.devices.reshape(2, 4, 2, 4, 2), ("z_hi", "y", "z_lo", "x", "core"))
    return jax.shard_map(
        shards,
        mesh=finer,
        in_specs=(P(FSDP, TP), P(FSDP, TP), P(FSDP, TP), P(FSDP, TP), P(TP, FSDP)),
        out_specs=(P(FSDP, TP), P(FSDP, TP), P(FSDP, TP), P(TP, FSDP)),
        check_vma=False,
    )
```

```python
import functools
import math

import jax
import jax.numpy as jnp
from jax import lax
from jax.experimental import pallas as pl
from jax.experimental.pallas import tpu as pltpu
from jax.sharding import Mesh
from jax.sharding import PartitionSpec as P

FSDP = ("z_hi", "y")
TP = ("z_lo", "x", "core")
MESH = pl.DeviceIdType.MESH
BF = jnp.bfloat16
F32 = jnp.float32
NSEND, NRECV = 23, 88
GROUP = 6
ROUNDED = (0, 1, 2)
ZF = 64
HOME = 160
ROUNDS = ((0, 0, 0, 256), (0, 1, 0, 256), (1, 0, HOME, 256 - HOME), (1, 1, HOME, 256 - HOME))


def dot(a, b, ca, cb):
    return lax.dot_general(a, b, (((ca,), (cb,)), ((), ())), preferred_element_type=F32)


def kernel(factor, tok, og, wg, wu, wd, ig_o, gg_o, ug_o, dg_o,
           own, xb, wgu, wdn, pgu, ph, pgur, phr, agu, ah, igp, sibr, farr, nearr, fs, ns, nowr, zfr, zr, igs, igr,
           ws, hs, gb, hb, gfr, hfr, gnr, hnr, lsem, ssem, rsem):
    R, C = tok.shape
    F = wg.shape[1]
    H = R // 2
    z_hi, y, z_lo, x, core = (lax.axis_index(a) for a in ("z_hi", "y", "z_lo", "x", "core"))
    inner = (z_hi - z_lo) * (z_hi - z_lo)
    is_inner, is_outer = inner == 1, inner == 0
    nx, ny = 4, 4
    xr, xl, xf = lax.rem(x + 1, nx), lax.rem(x + nx - 1, nx), lax.rem(x + 2, nx)
    yr, yl, yf = lax.rem(y + 1, ny), lax.rem(y + ny - 1, ny), lax.rem(y + 2, ny)
    oc = 1 - core
    t_of = (z_hi, 1 - z_hi)
    d_xr, d_xl = (z_hi, y, z_lo, xr, core), (z_hi, y, z_lo, xl, core)
    d_yr, d_yl = (z_hi, yr, z_lo, x, core), (z_hi, yl, z_lo, x, core)
    d_sib = (z_hi, y, z_lo, x, oc)
    d_zlo = (z_hi, y, 1 - z_lo, x, core)
    d_zhi = (1 - z_hi, y, z_lo, x, core)
    d_zz = (1 - z_hi, y, 1 - z_lo, x, core)
    d_zs = (z_lo, y, 1 - z_lo, x, core)
    partners = (d_xr, d_xl, d_yr, d_yl, d_sib, d_zlo, d_zhi, d_zz)

    sends, recvs = {}, {}

    def slot(table, name):
        return table.setdefault(name, len(table))

    for k in range(8):
        slot(recvs, ("z", k))
    for k in range(8):
        slot(recvs, ("zh", k))
    groups = []

    def size(ref):
        return math.prod(ref.shape) * jnp.dtype(ref.dtype).itemsize

    def unit_of(nbytes):
        k = nbytes // 16384
        if nbytes % 16384 == 0:
            for n in (8, 7, 6, 5, 4, 3, 2, 1):
                if k % n == 0 and k // n <= 2 * R // 16:
                    return n, 16 * (k // n)
        return None

    def wait_bytes(sem, nbytes):
        n, m = unit_of(nbytes)
        r = xb.at[0, pl.ds(0, n), pl.ds(0, m), :]
        pltpu.make_async_copy(r, r, sem).wait()

    def remote(src, dst, dev, i, j):
        return pltpu.make_async_remote_copy(
            src_ref=src, dst_ref=dst, send_sem=ssem.at[i], recv_sem=rsem.at[j],
            device_id=dev, device_id_type=MESH)

    def send(name, src, dst, dev, rs=None, wait_later=True):
        if wait_later:
            total = sum(groups[-1]) if groups else 0
            if not groups or ((len(groups[-1]) >= GROUP or total >= 1 << 21) and unit_of(total) is not None):
                groups.append([])
            groups[-1].append(size(src))
            i = slot(sends, ("group", len(groups) - 1))
        else:
            i = slot(sends, name)
        remote(src, dst, dev, i, slot(recvs, name) if rs is None else rs).start()

    def recv(name, *dsts):
        if len(dsts) == 1:
            remote(dsts[0], dsts[0], d_sib, 0, slot(recvs, name)).wait_recv()
        else:
            wait_bytes(rsem.at[slot(recvs, name)], sum(size(d) for d in dsts))

    def trow(t):
        return pl.ds(pl.multiple_of(t * R, R), R)

    def blk(a, xp, c, t):
        return xb.at[a, 2 * xp + c, trow(t), :]

    def rows(start, n):
        return pl.ds(pl.multiple_of(start, 16), n)

    def chunk(a, xp, t, h, r0, n):
        return xb.at[a, 2 * xp + core, rows(t * R + r0 + h * (n // 2), n // 2), :]

    def part(a, xp, c, t, r0, n):
        return xb.at[a, 2 * xp + c, rows(t * R + r0, n), :]

    home_at = (1 - inner) * z_hi * R + inner * 2 * R

    def home(xp, h=None):
        if h is None:
            return xb.at[1, 2 * xp + core, rows(home_at, HOME), :]
        return xb.at[1, 2 * xp + core, rows(home_at + h * (HOME // 2), HOME // 2), :]

    loads_w = [
        pltpu.make_async_copy(wg, wgu.at[y, :, pl.ds(0, F)], lsem.at[0]),
        pltpu.make_async_copy(wu, wgu.at[y, :, pl.ds(F, F)], lsem.at[1]),
        pltpu.make_async_copy(wd, wdn.at[y], lsem.at[2]),
    ]
    loads_t = [
        pltpu.make_async_copy(tok, own.at[0], lsem.at[3]),
        pltpu.make_async_copy(og, own.at[1], lsem.at[4]),
    ]
    for c in loads_t + loads_w:
        c.start()

    outer_loads = (
        (tok, blk(0, x, core, z_hi), lsem.at[5]),
        (og.at[pl.ds(HOME, R - HOME), :], part(1, x, core, z_hi, HOME, R - HOME), lsem.at[6]),
    )
    load_home = pltpu.make_async_copy(og.at[pl.ds(0, HOME), :], home(x), lsem.at[7])
    load_home.start()

    @pl.when(is_outer)
    def _():
        for c in outer_loads:
            pltpu.make_async_copy(*c).start()

    barrier = pltpu.get_barrier_semaphore()
    for d in partners:
        pl.semaphore_signal(barrier, inc=1, device_id=d, device_id_type=MESH)
    pl.semaphore_wait(barrier, len(partners))

    for c in loads_t:
        c.wait()
    load_home.wait()

    for a, rel, r0, n in (ROUNDS[0], ROUNDS[2]):
        for h in range(2):
            k = 2 * a + h
            send(("zs", k), own.at[a, pl.ds(r0 + h * (n // 2), n // 2), :], chunk(a, x, z_hi, h, r0, n), d_zs,
                 rs=4 * inner + k)

    @pl.when(is_outer)
    def _():
        for c in outer_loads:
            pltpu.make_async_copy(*c).wait()

    for c in loads_w:
        c.wait()

    def wchunk(which, yp, h):
        if which == 0:
            return wgu.at[yp, pl.ds(h * C, C), :]
        return wdn.at[yp, pl.ds(h * (F // 2), F // 2), :]

    def ysend(w):
        for h in range(2):
            send(("yf", w) if h else ("y", w, 0), wchunk(w, y, h), wchunk(w, y, h), d_yr)
            send(("yf", w) if h else ("y", w, 1), wchunk(w, y, 1 - h), wchunk(w, y, 1 - h), d_yl)

    def yfwd(w):
        recv(("y", w, 0), wchunk(w, yl, 0))
        send(("yf", w), wchunk(w, yl, 0), wchunk(w, yl, 0), d_yr)
        recv(("y", w, 1), wchunk(w, yr, 1))
        send(("yf", w), wchunk(w, yr, 1), wchunk(w, yr, 1), d_yl)

    def yfin(w):
        recv(("yf", w), wchunk(w, yl, 1), wchunk(w, yr, 0), wchunk(w, yf, 0), wchunk(w, yf, 1))

    def hsend():
        for h in range(2):
            send(("h", 0, h), home(x, h), home(x, h), d_xr)
            send(("h", 1, 1 - h), home(x, 1 - h), home(x, 1 - h), d_xl)

    def homez(j, xp):
        send(("hz", j), home(xp), xb.at[1, 2 * xp + core, rows(z_hi * R, HOME), :], d_zs, rs=8 + 4 * inner + j)

    def hfwd():
        recv(("h", 0, 0), home(xl, 0))
        send("hf", home(xl, 0), home(xl, 0), d_xr)
        recv(("h", 1, 1), home(xr, 1))
        send("hf", home(xr, 1), home(xr, 1), d_xl)

    def hfin_a():
        homez(0, x)
        recv(("h", 0, 1), home(xl, 1))
        homez(1, xl)
        recv(("h", 1, 0), home(xr, 0))
        homez(2, xr)

    def hfin_b():
        recv("hf", home(xf, 0), home(xf, 1))
        homez(3, xf)

    xorder = (x, xl, xr, xf)

    def hpart(rel, j):
        return part(1, xorder[j], core, t_of[rel], 0, HOME)

    def hsib(rel, j):
        send("hs", hpart(rel, j), hpart(rel, j), d_sib, rs=slot(recvs, ("hs", rel)), wait_later=False)

    def hz_inner(j):
        @pl.when(is_inner)
        def _():
            recv(("zh", 4 + j), hpart(1, j))
            send("zrel", hpart(1, j), hpart(1, j), d_zlo, rs=12 + j, wait_later=False)
            hsib(1, j)
            recv(("zh", j), hpart(0, j))
            hsib(0, j)

    def hz_outer(j):
        @pl.when(is_outer)
        def _():
            recv(("zh", 4 + j), hpart(1, j))
            hsib(1, j)

    def hs_outer():
        @pl.when(is_outer)
        def _():
            for j in range(4):
                hsib(0, j)

    def hsfin(rel):
        recv(("hs", rel), *[part(1, xp, oc, t_of[rel], 0, HOME) for xp in xorder])

    def relay(r, hs=(0, 1)):
        a, rel, r0, n = ROUNDS[r]
        t = t_of[rel]
        for h in hs:
            k = 2 * a + h

            @pl.when(is_inner)
            def _():
                c = chunk(a, x, t, h, r0, n)
                recv(("z", 4 + k), c)
                send("zrel", c, c, d_zlo, rs=4 + k, wait_later=False)

    def xsend_h(r, h):
        a, rel, r0, n = ROUNDS[r]
        t = t_of[rel]
        k = 2 * a + h
        c = chunk(a, x, t, h, r0, n)
        if rel == 0:
            @pl.when(is_inner)
            def _():
                recv(("z", k), c)
        else:
            @pl.when(is_outer)
            def _():
                recv(("z", 4 + k), c)
        if h == 0:
            send(("x", r, 0, 0), c, c, d_xr)
        else:
            send(("x", r, 1, 1), c, c, d_xl)
            send(("x", r, 0, 1), c, c, d_xr)
            c = chunk(a, x, t, 0, r0, n)
            send(("x", r, 1, 0), c, c, d_xl)
            p = part(a, x, core, t, r0, n)
            send(("s", r), p, p, d_sib)

    def xsend(r):
        xsend_h(r, 0)
        xsend_h(r, 1)

    def xfwd(r):
        a, rel, r0, n = ROUNDS[r]
        t = t_of[rel]
        c = chunk(a, xl, t, 0, r0, n)
        recv(("x", r, 0, 0), c)
        send(("xf", r), c, c, d_xr)
        c = chunk(a, xr, t, 1, r0, n)
        recv(("x", r, 1, 1), c)
        send(("xf", r), c, c, d_xl)

    def xfin(r):
        a, rel, r0, n = ROUNDS[r]
        t = t_of[rel]
        recv(("x", r, 0, 1), chunk(a, xl, t, 1, r0, n))
        p = part(a, xl, core, t, r0, n)
        send(("s", r), p, p, d_sib)
        recv(("x", r, 1, 0), chunk(a, xr, t, 0, r0, n))
        p = part(a, xr, core, t, r0, n)
        send(("s", r), p, p, d_sib)
        recv(("xf", r), chunk(a, xf, t, 0, r0, n), chunk(a, xf, t, 1, r0, n))
        p = part(a, xf, core, t, r0, n)
        send(("s", r), p, p, d_sib)

    def sfin(r):
        a, rel, r0, n = ROUNDS[r]
        recv(("s", r), *[part(a, xp, oc, t_of[rel], r0, n) for xp in xorder])

    def forward(a, rel, r0, n):
        t = t_of[rel]
        terms = []
        for e in range(2 * nx):
            block = xb[a, e, rows(t * R + r0, n), :]
            cols = pl.ds((e % 2) * C, C)
            if a == 0:
                terms.append(dot(block, wgu[e // 2, cols, :], 1, 0))
            else:
                terms.append(dot(block, wdn[e // 2, :, cols], 1, 1))
        (pgu, ph)[a][rel, pl.ds(r0, n)] = functools.reduce(jnp.add, terms)

    REST = (HOME, R - HOME)

    def gate_up():
        return pgu[1, :, :F] + pgur[:, :F], pgu[1, :, F:] + pgur[:, F:]

    hsend()
    ysend(0)
    xsend_h(0, 0)
    relay(1, (0,))
    hfwd()
    xsend_h(0, 1)
    relay(1, (1,))
    hfin_a()
    yfwd(0)
    ysend(1)
    relay(3)
    xfwd(0)
    xsend(2)
    xsend(1)
    xsend(3)
    hfin_b()
    hs_outer()
    hz_inner(0)
    hz_inner(1)
    xfin(0)
    xfwd(2)
    hz_inner(2)
    yfin(0)
    sfin(0)
    hz_inner(3)
    forward(0, 0, 0, R)
    send("exg", pgu.at[0], pgur, d_zhi)
    yfwd(1)
    xfwd(1)
    xfwd(3)
    xfin(2)
    sfin(2)
    hsfin(0)
    yfin(1)
    forward(1, 0, 0, R)
    send("exh", ph.at[0], phr, d_zhi)
    xfin(1)
    for j in range(4):
        hz_outer(j)
    xfin(3)
    sfin(1)
    forward(0, 1, 0, R)
    recv("exg", pgur)
    mine, away = trow(1 - z_hi), trow(z_hi)
    gate, up = gate_up()
    ah[mine, :] = (gate * jax.nn.sigmoid(gate) * up).astype(BF)
    send("acth", ah.at[mine, :], ah.at[mine, :], d_zhi)
    hsfin(1)
    forward(1, 1, 0, HOME)
    sfin(3)
    forward(1, 1, *REST)

    recv("exh", phr)
    gate, up = gate_up()
    hg = ph[1] + phr[...]
    squashed = jax.nn.sigmoid(gate)
    activated = gate * squashed
    slope = squashed * (1.0 + gate * (1.0 - squashed))
    agu[mine, :F] = (hg * up * slope).astype(BF)
    agu[mine, F:] = (hg * activated).astype(BF)
    send("actg", agu.at[mine, :], agu.at[mine, :], d_zhi)

    order = (xf, xr, xl, x)
    RA = ((ZF, R - ZF), (0, ZF))

    def hrows(p, h):
        r0, n = RA[p]
        return pl.ds(r0 + h * (n // 2), n // 2)

    def arows(p):
        return pl.ds(*RA[p])

    def igblock(rel, xp, c):
        w = wgu[xp, pl.ds(pl.multiple_of(c * C, C), C), :]
        igp[rel, 2 * xp + c] = dot(agu[trow(t_of[rel]), :], w, 1, 1)

    def igstart(rel):
        for j, xp in enumerate(order):
            igblock(rel, xp, oc)
            send(("is", rel, j), igp.at[rel, 2 * xp + oc], sibr.at[rel, xp], d_sib)
        for xp in order:
            igblock(rel, xp, core)

    def addsib(rel, j):
        xp = order[j]
        recv(("is", rel, j), sibr.at[rel, xp])
        igp[rel, 2 * xp + core] += sibr[rel, xp]

    def zfirst(rel, j):
        xp = order[j]
        send("zf", igp.at[rel, 2 * xp + core, arows(1), :], zfr.at[xp], d_zlo,
             rs=slot(recvs, ("zf", j)), wait_later=False)

    def igfar(p, rel, k):
        for h, d in enumerate((d_xr, d_xl)):
            fs[k, h, pl.ds(0, RA[p][1] // 2), :] = igp[rel, 2 * xf + core, hrows(p, h), :].astype(BF)
            n = pl.ds(0, RA[p][1] // 2)
            send(("if", k, h), fs.at[k, h, n, :], farr.at[k, h, n, :], d)

    def ignear(p, rel, k):
        n = pl.ds(0, RA[p][1] // 2)
        for h, (xp, d) in enumerate(((xr, d_xr), (xl, d_xl))):
            rows_h = hrows(p, 1 - h)
            if k in ROUNDED:
                ns[k, h, n, :] = igp[rel, 2 * xp + core, rows_h, :].astype(BF)
                send(("in", k), ns.at[k, h, n, :], nowr.at[k, h, n, :], d)
            else:
                send(("in", k), igp.at[rel, 2 * xp + core, rows_h, :], nearr.at[rel, h, rows_h, :], d)

    def igsecond(p, rel, k):
        for h, (xp, d) in enumerate(((xr, d_xr), (xl, d_xl))):
            n = pl.ds(0, RA[p][1] // 2)
            recv(("if", k, h), farr.at[k, h, n, :])
            igp[rel, 2 * xp + core, hrows(p, h), :] += farr[k, h, n, :].astype(F32)
            send(("in", k), igp.at[rel, 2 * xp + core, hrows(p, h), :], nearr.at[rel, h, hrows(p, h), :], d)

    def iglast(p, rel, k):
        n = pl.ds(0, RA[p][1] // 2)
        first = [nowr.at[k, h, n, :] if k in ROUNDED else nearr.at[rel, h, hrows(p, 1 - h), :] for h in range(2)]
        second = [nearr.at[rel, h, hrows(p, h), :] for h in range(2)]
        recv(("in", k), *first, *second)
        for h in range(2):
            igp[rel, 2 * x + core, hrows(p, h), :] += second[h][...] + first[1 - h][...].astype(F32)

    def igfirst(rel, when):
        addsib(rel, 0)
        igfar(0, rel, rel)
        addsib(rel, 1)
        addsib(rel, 2)
        ignear(0, rel, rel)
        addsib(rel, 3)

        @pl.when(when)
        def _():
            for j in range(4):
                zfirst(rel, j)

    def gunit(e):
        g = dot(xb[0, e, : 2 * R], agu[...], 0, 0)
        ws[e] = g
        gb[e] = g.astype(BF)

    def hunit(e):
        d = dot(ah[...], xb[1, e, : 2 * R], 0, 0)
        hs[e] = d
        hb[e] = d.astype(BF)

    sides = ((yr, d_yr), (yl, d_yl))
    def zsend(rel):
        for h in range(2):
            send("zi", igp.at[rel, 2 * x + core, hrows(0, h), :], zr.at[hrows(0, h), :], d_zlo,
                 rs=slot(recvs, ("zir", h)), wait_later=False)

    def zfadd(j):
        xp = order[j]
        recv(("zf", j), zfr.at[xp])
        igp[keep, 2 * xp + core, arows(1), :] += zfr[xp]

    def hsecond(h):
        yp, d = sides[h]
        recv(("hf", h), hfr.at[h])
        hb[2 * yp + h] = (hs[2 * yp + h] + hfr[h].astype(F32)).astype(BF)
        send("gn", hb.at[2 * yp + h], hnr.at[h, h], d)

    def gsecond(h):
        yp, d = sides[h]
        recv(("gf", h), gfr.at[h])
        gb[2 * yp + h] = (ws[2 * yp + h] + gfr[h].astype(F32)).astype(BF)
        send("gn", gb.at[2 * yp + h], gnr.at[h, h], d)

    keep = inner
    igstart(1)
    recv("acth", ah.at[away, :])
    for h, (yp, d) in enumerate(sides):
        hunit(2 * yf + h)
        send(("hf", h), hb.at[2 * yf + h], hfr.at[h], d)
    igfirst(1, is_outer)
    for h, (yp, d) in enumerate(sides):
        hunit(2 * yp + 1 - h)
        send("gn", hb.at[2 * yp + 1 - h], hnr.at[h, 1 - h], d)
    recv("actg", agu.at[away, :])
    for h, (yp, d) in enumerate(sides):
        gunit(2 * yf + h)
        send(("gf", h), gb.at[2 * yf + h], gfr.at[h], d)
    igsecond(0, 1, 1)
    igstart(0)
    for h, (yp, d) in enumerate(sides):
        hunit(2 * yp + h)
    igfirst(0, is_inner)
    for h, (yp, d) in enumerate(sides):
        gunit(2 * yp + 1 - h)
        send("gn", gb.at[2 * yp + 1 - h], gnr.at[h, 1 - h], d)
    for h in range(2):
        hsecond(h)
    for h, (yp, d) in enumerate(sides):
        gunit(2 * yp + h)
    iglast(0, 1, 1)

    @pl.when(is_outer)
    def _():
        zsend(1)

    zfadd(0)
    igfar(1, keep, 2)
    gsecond(0)
    gsecond(1)
    igsecond(0, 0, 0)
    zfadd(1)
    zfadd(2)
    ignear(1, keep, 2)
    for h in range(2):
        gunit(2 * y + h)
        hunit(2 * y + h)
    igsecond(1, keep, 2)
    iglast(0, 0, 0)

    @pl.when(is_inner)
    def _():
        zsend(0)

    zfadd(3)
    iglast(1, keep, 2)

    @pl.when(is_inner)
    def _():
        igs[2, pl.ds(0, ZF), :] = igp[1, 2 * x + core, arows(1), :].astype(BF)
        send("zo", igs.at[2, pl.ds(0, ZF), :], igr.at[2, pl.ds(0, ZF), :], d_zz,
             rs=slot(recvs, ("zo", 2)), wait_later=False)
        n = pl.ds(0, (R - ZF) // 2)
        for h in range(2):
            recv(("zir", h), zr.at[hrows(0, h), :])
            igs[h, n, :] = (igp[1, 2 * x + core, hrows(0, h), :] + zr[hrows(0, h), :]).astype(BF)
            send("zo", igs.at[h, n, :], igr.at[h, n, :], d_zz,
                 rs=slot(recvs, ("zo", h)), wait_later=False)

    @pl.when(is_outer)
    def _():
        ig_o[arows(1), :] = igp[0, 2 * x + core, arows(1), :].astype(BF)

    recv("gn", *[b.at[s, h] for b in (gnr, hnr) for s in range(2) for h in range(2)])
    for h in range(2):
        g = (ws[2 * y + h] + gnr[0, h].astype(F32) + gnr[1, h].astype(F32)) * factor
        gg_o[pl.ds(h * C, C), :] = g[:, :F]
        ug_o[pl.ds(h * C, C), :] = g[:, F:]
        dg_o[:, pl.ds(h * C, C)] = (hs[2 * y + h] + hnr[0, h].astype(F32) + hnr[1, h].astype(F32)) * factor

    @pl.when(is_outer)
    def _():
        for h in range(2):
            recv(("zir", h), zr.at[hrows(0, h), :])
            ig_o[hrows(0, h), :] = (igp[0, 2 * x + core, hrows(0, h), :] + zr[hrows(0, h), :]).astype(BF)

    @pl.when(is_inner)
    def _():
        zs, n = pl.ds(0, ZF), pl.ds(0, (R - ZF) // 2)
        recv(("zo", 2), igr.at[2, zs, :])
        ig_o[arows(1), :] = igr[2, zs, :]
        for h in range(2):
            recv(("zo", h), igr.at[h, n, :])
            ig_o[hrows(0, h), :] = igr[h, n, :]
        wait_bytes(ssem.at[slot(sends, "zo")], R * C * 2)
        relayed = (ROUNDS[1][3] + ROUNDS[3][3] + 4 * HOME) * C * 2
        wait_bytes(ssem.at[slot(sends, "zrel")], relayed)

    wait_bytes(ssem.at[slot(sends, "zi")], (R - ZF) * C * 4)
    wait_bytes(ssem.at[slot(sends, "zf")], 4 * ZF * C * 4)
    wait_bytes(ssem.at[slot(sends, "hs")], 8 * HOME * C * 2)
    for k, sizes in enumerate(groups):
        wait_bytes(ssem.at[slot(sends, ("group", k))], sum(sizes))
    assert len(sends) <= NSEND and len(recvs) <= NRECV, (len(sends), len(recvs))


def deliver(*refs):
    n = (len(refs) - 1) // 2
    copies = [pltpu.make_async_copy(refs[k], refs[n + k], refs[-1].at[k]) for k in range(n)]
    for c in copies:
        c.start()
    for c in copies:
        c.wait()


def shards(tokens, out_grad, gate_weight, up_weight, down_weight):
    R, C = tokens.shape
    F = gate_weight.shape[1]
    H = R // 2
    factor = 1.0 / math.sqrt(R * lax.axis_size(FSDP))
    anyspec = pl.BlockSpec(memory_space=pl.ANY)
    vm = pl.BlockSpec(memory_space=pltpu.VMEM)
    V = pltpu.VMEM
    scratch = [
        V((2, R, C), BF), V((2, 8, 2 * R + HOME, C), BF), V((4, 2 * C, 2 * F), BF), V((4, F, 2 * C), BF),
        V((2, R, 2 * F), F32), V((2, R, F), F32), V((R, 2 * F), F32), V((R, F), F32),
        V((2 * R, 2 * F), BF), V((2 * R, F), BF),
        V((2, 8, R, C), F32), V((2, 4, R, C), F32), V((3, 2, H, C), BF), V((2, 2, R, C), F32), V((3, 2, H, C), BF), V((3, 2, H, C), BF), V((3, 2, H, C), BF), V((4, ZF, C), F32),
        V((R, C), F32), V((3, H, C), BF), V((3, H, C), BF),
        V((8, C, 2 * F), F32), V((8, F, C), F32), V((8, C, 2 * F), BF), V((8, F, C), BF),
        V((2, C, 2 * F), BF), V((2, F, C), BF), V((2, 2, C, 2 * F), BF), V((2, 2, F, C), BF),
        pltpu.SemaphoreType.DMA((8,)), pltpu.SemaphoreType.DMA((NSEND,)), pltpu.SemaphoreType.DMA((NRECV,)),
    ]
    held = pl.pallas_call(
        functools.partial(kernel, factor),
        out_shape=(
            V((R, C), BF),
            V((2 * C, F), F32),
            V((2 * C, F), F32),
            V((F, 2 * C), F32),
        ),
        in_specs=[anyspec] * 5,
        out_specs=(vm,) * 4,
        scratch_shapes=scratch,
        compiler_params=pltpu.CompilerParams(
            collective_id=0, has_side_effects=True, vmem_limit_bytes=60 * 1024 * 1024),
        name="ffn_backward",
    )(tokens, out_grad, gate_weight, up_weight, down_weight)
    return pl.pallas_call(
        deliver,
        out_shape=tuple(jax.ShapeDtypeStruct(a.shape, a.dtype) for a in held),
        in_specs=[vm] * len(held),
        out_specs=(anyspec,) * len(held),
        scratch_shapes=[pltpu.SemaphoreType.DMA((len(held),))],
        name="deliver",
    )(*[pltpu.with_memory_space_constraint(a, pltpu.VMEM) for a in held])


def solution(mesh):
    finer = Mesh(mesh.devices.reshape(2, 4, 2, 4, 2), ("z_hi", "y", "z_lo", "x", "core"))
    return jax.shard_map(
        shards,
        mesh=finer,
        in_specs=(P(FSDP, TP), P(FSDP, TP), P(FSDP, TP), P(FSDP, TP), P(TP, FSDP)),
        out_specs=(P(FSDP, TP), P(FSDP, TP), P(FSDP, TP), P(TP, FSDP)),
        check_vma=False,
    )
```

```python
import functools
import math

import jax
import jax.numpy as jnp
from jax import lax
from jax.experimental import pallas as pl
from jax.experimental.pallas import tpu as pltpu
from jax.sharding import Mesh
from jax.sharding import PartitionSpec as P

FSDP = ("z_hi", "y")
TP = ("z_lo", "x", "core")
MESH = pl.DeviceIdType.MESH
BF = jnp.bfloat16
F32 = jnp.float32
NSEND, NRECV = 23, 88
GROUP = 6
ROUNDED = (0, 1)
ZF = 64
HOME = 160
ROUNDS = ((0, 0, 0, 256), (0, 1, 0, 256), (1, 0, HOME, 256 - HOME), (1, 1, HOME, 256 - HOME))


def dot(a, b, ca, cb):
    return lax.dot_general(a, b, (((ca,), (cb,)), ((), ())), preferred_element_type=F32)


def kernel(factor, tok, og, wg, wu, wd, ig_o, gg_o, ug_o, dg_o,
           own, xb, wgu, wdn, pgu, ph, pgur, phr, agu, ah, igp, sibr, farr, nearr, fs, ns, nowr, zfr, zr, igs, igr,
           ws, hs, gb, hb, gfr, hfr, gnr, hnr, lsem, ssem, rsem):
    R, C = tok.shape
    F = wg.shape[1]
    H = R // 2
    z_hi, y, z_lo, x, core = (lax.axis_index(a) for a in ("z_hi", "y", "z_lo", "x", "core"))
    inner = (z_hi - z_lo) * (z_hi - z_lo)
    is_inner, is_outer = inner == 1, inner == 0
    nx, ny = 4, 4
    xr, xl, xf = lax.rem(x + 1, nx), lax.rem(x + nx - 1, nx), lax.rem(x + 2, nx)
    yr, yl, yf = lax.rem(y + 1, ny), lax.rem(y + ny - 1, ny), lax.rem(y + 2, ny)
    oc = 1 - core
    t_of = (z_hi, 1 - z_hi)
    d_xr, d_xl = (z_hi, y, z_lo, xr, core), (z_hi, y, z_lo, xl, core)
    d_yr, d_yl = (z_hi, yr, z_lo, x, core), (z_hi, yl, z_lo, x, core)
    d_sib = (z_hi, y, z_lo, x, oc)
    d_zlo = (z_hi, y, 1 - z_lo, x, core)
    d_zhi = (1 - z_hi, y, z_lo, x, core)
    d_zz = (1 - z_hi, y, 1 - z_lo, x, core)
    d_zs = (z_lo, y, 1 - z_lo, x, core)
    partners = (d_xr, d_xl, d_yr, d_yl, d_sib, d_zlo, d_zhi, d_zz)

    sends, recvs = {}, {}

    def slot(table, name):
        return table.setdefault(name, len(table))

    for k in range(8):
        slot(recvs, ("z", k))
    for k in range(8):
        slot(recvs, ("zh", k))
    groups = []

    def size(ref):
        return math.prod(ref.shape) * jnp.dtype(ref.dtype).itemsize

    def unit_of(nbytes):
        k = nbytes // 16384
        if nbytes % 16384 == 0:
            for n in (8, 7, 6, 5, 4, 3, 2, 1):
                if k % n == 0 and k // n <= 2 * R // 16:
                    return n, 16 * (k // n)
        return None

    def wait_bytes(sem, nbytes):
        n, m = unit_of(nbytes)
        r = xb.at[0, pl.ds(0, n), pl.ds(0, m), :]
        pltpu.make_async_copy(r, r, sem).wait()

    def remote(src, dst, dev, i, j):
        return pltpu.make_async_remote_copy(
            src_ref=src, dst_ref=dst, send_sem=ssem.at[i], recv_sem=rsem.at[j],
            device_id=dev, device_id_type=MESH)

    def send(name, src, dst, dev, rs=None, wait_later=True):
        if wait_later:
            total = sum(groups[-1]) if groups else 0
            if not groups or ((len(groups[-1]) >= GROUP or total >= 1 << 21) and unit_of(total) is not None):
                groups.append([])
            groups[-1].append(size(src))
            i = slot(sends, ("group", len(groups) - 1))
        else:
            i = slot(sends, name)
        remote(src, dst, dev, i, slot(recvs, name) if rs is None else rs).start()

    def recv(name, *dsts):
        if len(dsts) == 1:
            remote(dsts[0], dsts[0], d_sib, 0, slot(recvs, name)).wait_recv()
        else:
            wait_bytes(rsem.at[slot(recvs, name)], sum(size(d) for d in dsts))

    def trow(t):
        return pl.ds(pl.multiple_of(t * R, R), R)

    def blk(a, xp, c, t):
        return xb.at[a, 2 * xp + c, trow(t), :]

    def rows(start, n):
        return pl.ds(pl.multiple_of(start, 16), n)

    def chunk(a, xp, t, h, r0, n):
        return xb.at[a, 2 * xp + core, rows(t * R + r0 + h * (n // 2), n // 2), :]

    def part(a, xp, c, t, r0, n):
        return xb.at[a, 2 * xp + c, rows(t * R + r0, n), :]

    home_at = (1 - inner) * z_hi * R + inner * 2 * R

    def home(xp, h=None):
        if h is None:
            return xb.at[1, 2 * xp + core, rows(home_at, HOME), :]
        return xb.at[1, 2 * xp + core, rows(home_at + h * (HOME // 2), HOME // 2), :]

    loads_w = [
        pltpu.make_async_copy(wg, wgu.at[y, :, pl.ds(0, F)], lsem.at[0]),
        pltpu.make_async_copy(wu, wgu.at[y, :, pl.ds(F, F)], lsem.at[1]),
        pltpu.make_async_copy(wd, wdn.at[y], lsem.at[2]),
    ]
    loads_t = [
        pltpu.make_async_copy(tok, own.at[0], lsem.at[3]),
        pltpu.make_async_copy(og, own.at[1], lsem.at[4]),
    ]
    for c in loads_t + loads_w:
        c.start()

    outer_loads = (
        (tok, blk(0, x, core, z_hi), lsem.at[5]),
        (og.at[pl.ds(HOME, R - HOME), :], part(1, x, core, z_hi, HOME, R - HOME), lsem.at[6]),
    )
    load_home = pltpu.make_async_copy(og.at[pl.ds(0, HOME), :], home(x), lsem.at[7])
    load_home.start()

    @pl.when(is_outer)
    def _():
        for c in outer_loads:
            pltpu.make_async_copy(*c).start()

    barrier = pltpu.get_barrier_semaphore()
    for d in partners:
        pl.semaphore_signal(barrier, inc=1, device_id=d, device_id_type=MESH)
    pl.semaphore_wait(barrier, len(partners))

    for c in loads_t:
        c.wait()
    load_home.wait()

    for a, rel, r0, n in (ROUNDS[0], ROUNDS[2]):
        for h in range(2):
            k = 2 * a + h
            send(("zs", k), own.at[a, pl.ds(r0 + h * (n // 2), n // 2), :], chunk(a, x, z_hi, h, r0, n), d_zs,
                 rs=4 * inner + k)

    @pl.when(is_outer)
    def _():
        for c in outer_loads:
            pltpu.make_async_copy(*c).wait()

    for c in loads_w:
        c.wait()

    def wchunk(which, yp, h):
        if which == 0:
            return wgu.at[yp, pl.ds(h * C, C), :]
        return wdn.at[yp, pl.ds(h * (F // 2), F // 2), :]

    def ysend(w):
        for h in range(2):
            send(("yf", w) if h else ("y", w, 0), wchunk(w, y, h), wchunk(w, y, h), d_yr)
            send(("yf", w) if h else ("y", w, 1), wchunk(w, y, 1 - h), wchunk(w, y, 1 - h), d_yl)

    def yfwd(w):
        recv(("y", w, 0), wchunk(w, yl, 0))
        send(("yf", w), wchunk(w, yl, 0), wchunk(w, yl, 0), d_yr)
        recv(("y", w, 1), wchunk(w, yr, 1))
        send(("yf", w), wchunk(w, yr, 1), wchunk(w, yr, 1), d_yl)

    def yfin(w):
        recv(("yf", w), wchunk(w, yl, 1), wchunk(w, yr, 0), wchunk(w, yf, 0), wchunk(w, yf, 1))

    def hsend():
        for h in range(2):
            send(("h", 0, h), home(x, h), home(x, h), d_xr)
            send(("h", 1, 1 - h), home(x, 1 - h), home(x, 1 - h), d_xl)

    def homez(j, xp):
        send(("hz", j), home(xp), xb.at[1, 2 * xp + core, rows(z_hi * R, HOME), :], d_zs, rs=8 + 4 * inner + j)

    def hfwd():
        recv(("h", 0, 0), home(xl, 0))
        send("hf", home(xl, 0), home(xl, 0), d_xr)
        recv(("h", 1, 1), home(xr, 1))
        send("hf", home(xr, 1), home(xr, 1), d_xl)

    def hfin_a():
        homez(0, x)
        recv(("h", 0, 1), home(xl, 1))
        homez(1, xl)
        recv(("h", 1, 0), home(xr, 0))
        homez(2, xr)

    def hfin_b():
        recv("hf", home(xf, 0), home(xf, 1))
        homez(3, xf)

    xorder = (x, xl, xr, xf)

    def hpart(rel, j):
        return part(1, xorder[j], core, t_of[rel], 0, HOME)

    def hsib(rel, j):
        send("hs", hpart(rel, j), hpart(rel, j), d_sib, rs=slot(recvs, ("hs", rel)), wait_later=False)

    def hz_inner(j):
        @pl.when(is_inner)
        def _():
            recv(("zh", 4 + j), hpart(1, j))
            send("zrel", hpart(1, j), hpart(1, j), d_zlo, rs=12 + j, wait_later=False)
            hsib(1, j)
            recv(("zh", j), hpart(0, j))
            hsib(0, j)

    def hz_outer(j):
        @pl.when(is_outer)
        def _():
            recv(("zh", 4 + j), hpart(1, j))
            hsib(1, j)

    def hs_outer():
        @pl.when(is_outer)
        def _():
            for j in range(4):
                hsib(0, j)

    def hsfin(rel):
        recv(("hs", rel), *[part(1, xp, oc, t_of[rel], 0, HOME) for xp in xorder])

    def relay(r, hs=(0, 1)):
        a, rel, r0, n = ROUNDS[r]
        t = t_of[rel]
        for h in hs:
            k = 2 * a + h

            @pl.when(is_inner)
            def _():
                c = chunk(a, x, t, h, r0, n)
                recv(("z", 4 + k), c)
                send("zrel", c, c, d_zlo, rs=4 + k, wait_later=False)

    def xsend_h(r, h):
        a, rel, r0, n = ROUNDS[r]
        t = t_of[rel]
        k = 2 * a + h
        c = chunk(a, x, t, h, r0, n)
        if rel == 0:
            @pl.when(is_inner)
            def _():
                recv(("z", k), c)
        else:
            @pl.when(is_outer)
            def _():
                recv(("z", 4 + k), c)
        if h == 0:
            send(("x", r, 0, 0), c, c, d_xr)
        else:
            send(("x", r, 1, 1), c, c, d_xl)
            send(("x", r, 0, 1), c, c, d_xr)
            c = chunk(a, x, t, 0, r0, n)
            send(("x", r, 1, 0), c, c, d_xl)
            p = part(a, x, core, t, r0, n)
            send(("s", r), p, p, d_sib)

    def xsend(r):
        xsend_h(r, 0)
        xsend_h(r, 1)

    def xfwd(r):
        a, rel, r0, n = ROUNDS[r]
        t = t_of[rel]
        c = chunk(a, xl, t, 0, r0, n)
        recv(("x", r, 0, 0), c)
        send(("xf", r), c, c, d_xr)
        c = chunk(a, xr, t, 1, r0, n)
        recv(("x", r, 1, 1), c)
        send(("xf", r), c, c, d_xl)

    def xfin(r):
        a, rel, r0, n = ROUNDS[r]
        t = t_of[rel]
        recv(("x", r, 0, 1), chunk(a, xl, t, 1, r0, n))
        p = part(a, xl, core, t, r0, n)
        send(("s", r), p, p, d_sib)
        recv(("x", r, 1, 0), chunk(a, xr, t, 0, r0, n))
        p = part(a, xr, core, t, r0, n)
        send(("s", r), p, p, d_sib)
        recv(("xf", r), chunk(a, xf, t, 0, r0, n), chunk(a, xf, t, 1, r0, n))
        p = part(a, xf, core, t, r0, n)
        send(("s", r), p, p, d_sib)

    def sfin(r):
        a, rel, r0, n = ROUNDS[r]
        recv(("s", r), *[part(a, xp, oc, t_of[rel], r0, n) for xp in xorder])

    def forward(a, rel, r0, n):
        t = t_of[rel]
        terms = []
        for e in range(2 * nx):
            block = xb[a, e, rows(t * R + r0, n), :]
            cols = pl.ds((e % 2) * C, C)
            if a == 0:
                terms.append(dot(block, wgu[e // 2, cols, :], 1, 0))
            else:
                terms.append(dot(block, wdn[e // 2, :, cols], 1, 1))
        (pgu, ph)[a][rel, pl.ds(r0, n)] = functools.reduce(jnp.add, terms)

    REST = (HOME, R - HOME)

    def gate_up():
        return pgu[1, :, :F] + pgur[:, :F], pgu[1, :, F:] + pgur[:, F:]

    hsend()
    ysend(0)
    xsend_h(0, 0)
    relay(1, (0,))
    hfwd()
    xsend_h(0, 1)
    relay(1, (1,))
    hfin_a()
    yfwd(0)
    ysend(1)
    relay(3)
    xfwd(0)
    xsend(2)
    xsend(1)
    xsend(3)
    hfin_b()
    hs_outer()
    hz_inner(0)
    hz_inner(1)
    xfin(0)
    xfwd(2)
    hz_inner(2)
    yfin(0)
    sfin(0)
    hz_inner(3)
    forward(0, 0, 0, R)
    send("exg", pgu.at[0], pgur, d_zhi)
    yfwd(1)
    xfwd(1)
    xfwd(3)
    xfin(2)
    sfin(2)
    hsfin(0)
    yfin(1)
    forward(1, 0, 0, R)
    send("exh", ph.at[0], phr, d_zhi)
    xfin(1)
    for j in range(4):
        hz_outer(j)
    xfin(3)
    sfin(1)
    forward(0, 1, 0, R)
    recv("exg", pgur)
    mine, away = trow(1 - z_hi), trow(z_hi)
    gate, up = gate_up()
    ah[mine, :] = (gate * jax.nn.sigmoid(gate) * up).astype(BF)
    send("acth", ah.at[mine, :], ah.at[mine, :], d_zhi)
    hsfin(1)
    forward(1, 1, 0, HOME)
    sfin(3)
    forward(1, 1, *REST)

    recv("exh", phr)
    gate, up = gate_up()
    hg = ph[1] + phr[...]
    squashed = jax.nn.sigmoid(gate)
    activated = gate * squashed
    slope = squashed * (1.0 + gate * (1.0 - squashed))
    agu[mine, :F] = (hg * up * slope).astype(BF)
    agu[mine, F:] = (hg * activated).astype(BF)
    send("actg", agu.at[mine, :], agu.at[mine, :], d_zhi)

    order = (xf, xr, xl, x)
    RA = ((ZF, R - ZF), (0, ZF))

    def hrows(p, h):
        r0, n = RA[p]
        return pl.ds(r0 + h * (n // 2), n // 2)

    def arows(p):
        return pl.ds(*RA[p])

    def igblock(rel, xp, c):
        w = wgu[xp, pl.ds(pl.multiple_of(c * C, C), C), :]
        igp[rel, 2 * xp + c] = dot(agu[trow(t_of[rel]), :], w, 1, 1)

    def igstart(rel):
        for j, xp in enumerate(order):
            igblock(rel, xp, oc)
            send(("is", rel, j), igp.at[rel, 2 * xp + oc], sibr.at[rel, xp], d_sib)

    def igown(rel):
        for xp in order:
            igblock(rel, xp, core)

    def addsib(rel, j):
        xp = order[j]
        recv(("is", rel, j), sibr.at[rel, xp])
        igp[rel, 2 * xp + core] += sibr[rel, xp]

    def zfirst(rel, j):
        xp = order[j]
        send("zf", igp.at[rel, 2 * xp + core, arows(1), :], zfr.at[xp], d_zlo,
             rs=slot(recvs, ("zf", j)), wait_later=False)

    def igfar(p, rel, k):
        for h, d in enumerate((d_xr, d_xl)):
            fs[k, h, pl.ds(0, RA[p][1] // 2), :] = igp[rel, 2 * xf + core, hrows(p, h), :].astype(BF)
            n = pl.ds(0, RA[p][1] // 2)
            send(("if", k, h), fs.at[k, h, n, :], farr.at[k, h, n, :], d)

    def ignear(p, rel, k):
        n = pl.ds(0, RA[p][1] // 2)
        for h, (xp, d) in enumerate(((xr, d_xr), (xl, d_xl))):
            rows_h = hrows(p, 1 - h)
            if k in ROUNDED:
                ns[k, h, n, :] = igp[rel, 2 * xp + core, rows_h, :].astype(BF)
                send(("in", k), ns.at[k, h, n, :], nowr.at[k, h, n, :], d)
            else:
                send(("in", k), igp.at[rel, 2 * xp + core, rows_h, :], nearr.at[rel, h, rows_h, :], d)

    def igsecond(p, rel, k):
        for h, (xp, d) in enumerate(((xr, d_xr), (xl, d_xl))):
            n = pl.ds(0, RA[p][1] // 2)
            recv(("if", k, h), farr.at[k, h, n, :])
            igp[rel, 2 * xp + core, hrows(p, h), :] += farr[k, h, n, :].astype(F32)
            send(("in", k), igp.at[rel, 2 * xp + core, hrows(p, h), :], nearr.at[rel, h, hrows(p, h), :], d)

    def iglast(p, rel, k):
        n = pl.ds(0, RA[p][1] // 2)
        first = [nowr.at[k, h, n, :] if k in ROUNDED else nearr.at[rel, h, hrows(p, 1 - h), :] for h in range(2)]
        second = [nearr.at[rel, h, hrows(p, h), :] for h in range(2)]
        recv(("in", k), *first, *second)
        for h in range(2):
            igp[rel, 2 * x + core, hrows(p, h), :] += second[h][...] + first[1 - h][...].astype(F32)

    def igfirst(rel, when):
        addsib(rel, 0)
        igfar(0, rel, rel)
        addsib(rel, 1)
        addsib(rel, 2)
        ignear(0, rel, rel)
        addsib(rel, 3)

        @pl.when(when)
        def _():
            for j in range(4):
                zfirst(rel, j)

    def gunit(e):
        g = dot(xb[0, e, : 2 * R], agu[...], 0, 0)
        ws[e] = g
        gb[e] = g.astype(BF)

    def hunit(e):
        d = dot(ah[...], xb[1, e, : 2 * R], 0, 0)
        hs[e] = d
        hb[e] = d.astype(BF)

    sides = ((yr, d_yr), (yl, d_yl))
    def zsend(rel):
        for h in range(2):
            send("zi", igp.at[rel, 2 * x + core, hrows(0, h), :], zr.at[hrows(0, h), :], d_zlo,
                 rs=slot(recvs, ("zir", h)), wait_later=False)

    def zfadd(j):
        xp = order[j]
        recv(("zf", j), zfr.at[xp])
        igp[keep, 2 * xp + core, arows(1), :] += zfr[xp]

    def hsecond(h):
        yp, d = sides[h]
        recv(("hf", h), hfr.at[h])
        hb[2 * yp + h] = (hs[2 * yp + h] + hfr[h].astype(F32)).astype(BF)
        send("gn", hb.at[2 * yp + h], hnr.at[h, h], d)

    def gsecond(h):
        yp, d = sides[h]
        recv(("gf", h), gfr.at[h])
        gb[2 * yp + h] = (ws[2 * yp + h] + gfr[h].astype(F32)).astype(BF)
        send("gn", gb.at[2 * yp + h], gnr.at[h, h], d)

    keep = inner
    igstart(1)
    igown(1)
    recv("acth", ah.at[away, :])
    for h, (yp, d) in enumerate(sides):
        hunit(2 * yf + h)
        send(("hf", h), hb.at[2 * yf + h], hfr.at[h], d)
    igfirst(1, is_outer)
    for h, (yp, d) in enumerate(sides):
        hunit(2 * yp + 1 - h)
        send("gn", hb.at[2 * yp + 1 - h], hnr.at[h, 1 - h], d)
    recv("actg", agu.at[away, :])
    for h, (yp, d) in enumerate(sides):
        gunit(2 * yf + h)
        send(("gf", h), gb.at[2 * yf + h], gfr.at[h], d)
    igstart(0)
    igsecond(0, 1, 1)
    igown(0)
    for h, (yp, d) in enumerate(sides):
        hunit(2 * yp + h)
    igfirst(0, is_inner)
    for h, (yp, d) in enumerate(sides):
        gunit(2 * yp + 1 - h)
        send("gn", gb.at[2 * yp + 1 - h], gnr.at[h, 1 - h], d)
    for h in range(2):
        hsecond(h)
    for h, (yp, d) in enumerate(sides):
        gunit(2 * yp + h)
    iglast(0, 1, 1)

    @pl.when(is_outer)
    def _():
        zsend(1)

    zfadd(0)
    igfar(1, keep, 2)
    gsecond(0)
    gsecond(1)
    igsecond(0, 0, 0)
    zfadd(1)
    zfadd(2)
    ignear(1, keep, 2)
    for h in range(2):
        gunit(2 * y + h)
        hunit(2 * y + h)
    igsecond(1, keep, 2)
    iglast(0, 0, 0)

    @pl.when(is_inner)
    def _():
        zsend(0)

    zfadd(3)
    iglast(1, keep, 2)

    @pl.when(is_inner)
    def _():
        igs[2, pl.ds(0, ZF), :] = igp[1, 2 * x + core, arows(1), :].astype(BF)
        send("zo", igs.at[2, pl.ds(0, ZF), :], igr.at[2, pl.ds(0, ZF), :], d_zz,
             rs=slot(recvs, ("zo", 2)), wait_later=False)
        n = pl.ds(0, (R - ZF) // 2)
        for h in range(2):
            recv(("zir", h), zr.at[hrows(0, h), :])
            igs[h, n, :] = (igp[1, 2 * x + core, hrows(0, h), :] + zr[hrows(0, h), :]).astype(BF)
            send("zo", igs.at[h, n, :], igr.at[h, n, :], d_zz,
                 rs=slot(recvs, ("zo", h)), wait_later=False)

    @pl.when(is_outer)
    def _():
        ig_o[arows(1), :] = igp[0, 2 * x + core, arows(1), :].astype(BF)

    recv("gn", *[b.at[s, h] for b in (gnr, hnr) for s in range(2) for h in range(2)])
    for h in range(2):
        g = (ws[2 * y + h] + gnr[0, h].astype(F32) + gnr[1, h].astype(F32)) * factor
        gg_o[pl.ds(h * C, C), :] = g[:, :F]
        ug_o[pl.ds(h * C, C), :] = g[:, F:]
        dg_o[:, pl.ds(h * C, C)] = (hs[2 * y + h] + hnr[0, h].astype(F32) + hnr[1, h].astype(F32)) * factor

    @pl.when(is_outer)
    def _():
        for h in range(2):
            recv(("zir", h), zr.at[hrows(0, h), :])
            ig_o[hrows(0, h), :] = (igp[0, 2 * x + core, hrows(0, h), :] + zr[hrows(0, h), :]).astype(BF)

    @pl.when(is_inner)
    def _():
        zs, n = pl.ds(0, ZF), pl.ds(0, (R - ZF) // 2)
        recv(("zo", 2), igr.at[2, zs, :])
        ig_o[arows(1), :] = igr[2, zs, :]
        for h in range(2):
            recv(("zo", h), igr.at[h, n, :])
            ig_o[hrows(0, h), :] = igr[h, n, :]
        wait_bytes(ssem.at[slot(sends, "zo")], R * C * 2)
        relayed = (ROUNDS[1][3] + ROUNDS[3][3] + 4 * HOME) * C * 2
        wait_bytes(ssem.at[slot(sends, "zrel")], relayed)

    wait_bytes(ssem.at[slot(sends, "zi")], (R - ZF) * C * 4)
    wait_bytes(ssem.at[slot(sends, "zf")], 4 * ZF * C * 4)
    wait_bytes(ssem.at[slot(sends, "hs")], 8 * HOME * C * 2)
    for k, sizes in enumerate(groups):
        wait_bytes(ssem.at[slot(sends, ("group", k))], sum(sizes))
    assert len(sends) <= NSEND and len(recvs) <= NRECV, (len(sends), len(recvs))


def deliver(*refs):
    n = (len(refs) - 1) // 2
    copies = [pltpu.make_async_copy(refs[k], refs[n + k], refs[-1].at[k]) for k in range(n)]
    for c in copies:
        c.start()
    for c in copies:
        c.wait()


def shards(tokens, out_grad, gate_weight, up_weight, down_weight):
    R, C = tokens.shape
    F = gate_weight.shape[1]
    H = R // 2
    factor = 1.0 / math.sqrt(R * lax.axis_size(FSDP))
    anyspec = pl.BlockSpec(memory_space=pl.ANY)
    vm = pl.BlockSpec(memory_space=pltpu.VMEM)
    V = pltpu.VMEM
    scratch = [
        V((2, R, C), BF), V((2, 8, 2 * R + HOME, C), BF), V((4, 2 * C, 2 * F), BF), V((4, F, 2 * C), BF),
        V((2, R, 2 * F), F32), V((2, R, F), F32), V((R, 2 * F), F32), V((R, F), F32),
        V((2 * R, 2 * F), BF), V((2 * R, F), BF),
        V((2, 8, R, C), F32), V((2, 4, R, C), F32), V((3, 2, H, C), BF), V((2, 2, R, C), F32), V((3, 2, H, C), BF), V((3, 2, H, C), BF), V((3, 2, H, C), BF), V((4, ZF, C), F32),
        V((R, C), F32), V((3, H, C), BF), V((3, H, C), BF),
        V((8, C, 2 * F), F32), V((8, F, C), F32), V((8, C, 2 * F), BF), V((8, F, C), BF),
        V((2, C, 2 * F), BF), V((2, F, C), BF), V((2, 2, C, 2 * F), BF), V((2, 2, F, C), BF),
        pltpu.SemaphoreType.DMA((8,)), pltpu.SemaphoreType.DMA((NSEND,)), pltpu.SemaphoreType.DMA((NRECV,)),
    ]
    held = pl.pallas_call(
        functools.partial(kernel, factor),
        out_shape=(
            V((R, C), BF),
            V((2 * C, F), F32),
            V((2 * C, F), F32),
            V((F, 2 * C), F32),
        ),
        in_specs=[anyspec] * 5,
        out_specs=(vm,) * 4,
        scratch_shapes=scratch,
        compiler_params=pltpu.CompilerParams(
            collective_id=0, has_side_effects=True, vmem_limit_bytes=60 * 1024 * 1024),
        name="ffn_backward",
    )(tokens, out_grad, gate_weight, up_weight, down_weight)
    return pl.pallas_call(
        deliver,
        out_shape=tuple(jax.ShapeDtypeStruct(a.shape, a.dtype) for a in held),
        in_specs=[vm] * len(held),
        out_specs=(anyspec,) * len(held),
        scratch_shapes=[pltpu.SemaphoreType.DMA((len(held),))],
        name="deliver",
    )(*[pltpu.with_memory_space_constraint(a, pltpu.VMEM) for a in held])


def solution(mesh):
    finer = Mesh(mesh.devices.reshape(2, 4, 2, 4, 2), ("z_hi", "y", "z_lo", "x", "core"))
    return jax.shard_map(
        shards,
        mesh=finer,
        in_specs=(P(FSDP, TP), P(FSDP, TP), P(FSDP, TP), P(FSDP, TP), P(TP, FSDP)),
        out_specs=(P(FSDP, TP), P(FSDP, TP), P(FSDP, TP), P(TP, FSDP)),
        check_vma=False,
    )
```

```python
import functools
import math

import jax
import jax.numpy as jnp
from jax import lax
from jax.experimental import pallas as pl
from jax.experimental.pallas import tpu as pltpu
from jax.sharding import Mesh
from jax.sharding import PartitionSpec as P

FSDP = ("z_hi", "y")
TP = ("z_lo", "x", "core")
MESH = pl.DeviceIdType.MESH
BF = jnp.bfloat16
F32 = jnp.float32
NSEND, NRECV = 23, 88
GROUP = 6
ROUNDED = (0, 1, 2)
ZF = 64
HOME = 160
ROUNDS = ((0, 0, 0, 256), (0, 1, 0, 256), (1, 0, HOME, 256 - HOME), (1, 1, HOME, 256 - HOME))


def dot(a, b, ca, cb):
    return lax.dot_general(a, b, (((ca,), (cb,)), ((), ())), preferred_element_type=F32)


def kernel(factor, tok, og, wg, wu, wd, ig_o, gg_o, ug_o, dg_o,
           own, xb, wgu, wdn, pgu, ph, pgur, phr, agu, ah, igp, sibr, farr, nearr, fs, ns, nowr, zfr, zr, igs, igr,
           ws, hs, gb, hb, gfr, hfr, gnr, hnr, lsem, ssem, rsem):
    R, C = tok.shape
    F = wg.shape[1]
    H = R // 2
    z_hi, y, z_lo, x, core = (lax.axis_index(a) for a in ("z_hi", "y", "z_lo", "x", "core"))
    inner = (z_hi - z_lo) * (z_hi - z_lo)
    is_inner, is_outer = inner == 1, inner == 0
    nx, ny = 4, 4
    xr, xl, xf = lax.rem(x + 1, nx), lax.rem(x + nx - 1, nx), lax.rem(x + 2, nx)
    yr, yl, yf = lax.rem(y + 1, ny), lax.rem(y + ny - 1, ny), lax.rem(y + 2, ny)
    oc = 1 - core
    t_of = (z_hi, 1 - z_hi)
    d_xr, d_xl = (z_hi, y, z_lo, xr, core), (z_hi, y, z_lo, xl, core)
    d_yr, d_yl = (z_hi, yr, z_lo, x, core), (z_hi, yl, z_lo, x, core)
    d_sib = (z_hi, y, z_lo, x, oc)
    d_zlo = (z_hi, y, 1 - z_lo, x, core)
    d_zhi = (1 - z_hi, y, z_lo, x, core)
    d_zz = (1 - z_hi, y, 1 - z_lo, x, core)
    d_zs = (z_lo, y, 1 - z_lo, x, core)
    partners = (d_zhi, d_zlo, d_zz, d_xr, d_xl, d_yr, d_yl, d_sib)

    sends, recvs = {}, {}

    def slot(table, name):
        return table.setdefault(name, len(table))

    for k in range(8):
        slot(recvs, ("z", k))
    for k in range(8):
        slot(recvs, ("zh", k))
    groups = []

    def size(ref):
        return math.prod(ref.shape) * jnp.dtype(ref.dtype).itemsize

    def unit_of(nbytes):
        k = nbytes // 16384
        if nbytes % 16384 == 0:
            for n in (8, 7, 6, 5, 4, 3, 2, 1):
                if k % n == 0 and k // n <= 2 * R // 16:
                    return n, 16 * (k // n)
        return None

    def wait_bytes(sem, nbytes):
        n, m = unit_of(nbytes)
        r = xb.at[0, pl.ds(0, n), pl.ds(0, m), :]
        pltpu.make_async_copy(r, r, sem).wait()

    def remote(src, dst, dev, i, j):
        return pltpu.make_async_remote_copy(
            src_ref=src, dst_ref=dst, send_sem=ssem.at[i], recv_sem=rsem.at[j],
            device_id=dev, device_id_type=MESH)

    def send(name, src, dst, dev, rs=None, wait_later=True):
        if wait_later:
            total = sum(groups[-1]) if groups else 0
            if not groups or ((len(groups[-1]) >= GROUP or total >= 1 << 21) and unit_of(total) is not None):
                groups.append([])
            groups[-1].append(size(src))
            i = slot(sends, ("group", len(groups) - 1))
        else:
            i = slot(sends, name)
        remote(src, dst, dev, i, slot(recvs, name) if rs is None else rs).start()

    def recv(name, *dsts):
        if len(dsts) == 1:
            remote(dsts[0], dsts[0], d_sib, 0, slot(recvs, name)).wait_recv()
        else:
            wait_bytes(rsem.at[slot(recvs, name)], sum(size(d) for d in dsts))

    def trow(t):
        return pl.ds(pl.multiple_of(t * R, R), R)

    def blk(a, xp, c, t):
        return xb.at[a, 2 * xp + c, trow(t), :]

    def rows(start, n):
        return pl.ds(pl.multiple_of(start, 16), n)

    def chunk(a, xp, t, h, r0, n):
        return xb.at[a, 2 * xp + core, rows(t * R + r0 + h * (n // 2), n // 2), :]

    def part(a, xp, c, t, r0, n):
        return xb.at[a, 2 * xp + c, rows(t * R + r0, n), :]

    home_at = (1 - inner) * z_hi * R + inner * 2 * R

    def home(xp, h=None):
        if h is None:
            return xb.at[1, 2 * xp + core, rows(home_at, HOME), :]
        return xb.at[1, 2 * xp + core, rows(home_at + h * (HOME // 2), HOME // 2), :]

    loads_w = [
        pltpu.make_async_copy(wg, wgu.at[y, :, pl.ds(0, F)], lsem.at[0]),
        pltpu.make_async_copy(wu, wgu.at[y, :, pl.ds(F, F)], lsem.at[1]),
        pltpu.make_async_copy(wd, wdn.at[y], lsem.at[2]),
    ]
    loads_t = [
        pltpu.make_async_copy(tok, own.at[0], lsem.at[3]),
        pltpu.make_async_copy(og, own.at[1], lsem.at[4]),
    ]
    for c in loads_t + loads_w:
        c.start()

    outer_loads = (
        (tok, blk(0, x, core, z_hi), lsem.at[5]),
        (og.at[pl.ds(HOME, R - HOME), :], part(1, x, core, z_hi, HOME, R - HOME), lsem.at[6]),
    )
    load_home = pltpu.make_async_copy(og.at[pl.ds(0, HOME), :], home(x), lsem.at[7])
    load_home.start()

    @pl.when(is_outer)
    def _():
        for c in outer_loads:
            pltpu.make_async_copy(*c).start()

    barrier = pltpu.get_barrier_semaphore()
    for d in partners:
        pl.semaphore_signal(barrier, inc=1, device_id=d, device_id_type=MESH)
    pl.semaphore_wait(barrier, len(partners))

    for c in loads_t:
        c.wait()
    load_home.wait()

    for a, rel, r0, n in (ROUNDS[0], ROUNDS[2]):
        for h in range(2):
            k = 2 * a + h
            send(("zs", k), own.at[a, pl.ds(r0 + h * (n // 2), n // 2), :], chunk(a, x, z_hi, h, r0, n), d_zs,
                 rs=4 * inner + k)

    @pl.when(is_outer)
    def _():
        for c in outer_loads:
            pltpu.make_async_copy(*c).wait()

    for c in loads_w:
        c.wait()

    def wchunk(which, yp, h):
        if which == 0:
            return wgu.at[yp, pl.ds(h * C, C), :]
        return wdn.at[yp, pl.ds(h * (F // 2), F // 2), :]

    def ysend(w):
        for h in range(2):
            send(("yf", w) if h else ("y", w, 0), wchunk(w, y, h), wchunk(w, y, h), d_yr)
            send(("yf", w) if h else ("y", w, 1), wchunk(w, y, 1 - h), wchunk(w, y, 1 - h), d_yl)

    def yfwd(w):
        recv(("y", w, 0), wchunk(w, yl, 0))
        send(("yf", w), wchunk(w, yl, 0), wchunk(w, yl, 0), d_yr)
        recv(("y", w, 1), wchunk(w, yr, 1))
        send(("yf", w), wchunk(w, yr, 1), wchunk(w, yr, 1), d_yl)

    def yfin(w):
        recv(("yf", w), wchunk(w, yl, 1), wchunk(w, yr, 0), wchunk(w, yf, 0), wchunk(w, yf, 1))

    def hsend():
        for h in range(2):
            send(("h", 0, h), home(x, h), home(x, h), d_xr)
            send(("h", 1, 1 - h), home(x, 1 - h), home(x, 1 - h), d_xl)

    def homez(j, xp):
        send(("hz", j), home(xp), xb.at[1, 2 * xp + core, rows(z_hi * R, HOME), :], d_zs, rs=8 + 4 * inner + j)

    def hfwd():
        recv(("h", 0, 0), home(xl, 0))
        send("hf", home(xl, 0), home(xl, 0), d_xr)
        recv(("h", 1, 1), home(xr, 1))
        send("hf", home(xr, 1), home(xr, 1), d_xl)

    def hfin_a():
        homez(0, x)
        recv(("h", 0, 1), home(xl, 1))
        homez(1, xl)
        recv(("h", 1, 0), home(xr, 0))
        homez(2, xr)

    def hfin_b():
        recv("hf", home(xf, 0), home(xf, 1))
        homez(3, xf)

    xorder = (x, xl, xr, xf)

    def hpart(rel, j):
        return part(1, xorder[j], core, t_of[rel], 0, HOME)

    def hsib(rel, j):
        send("hs", hpart(rel, j), hpart(rel, j), d_sib, rs=slot(recvs, ("hs", rel)), wait_later=False)

    def hz_inner(j):
        @pl.when(is_inner)
        def _():
            recv(("zh", 4 + j), hpart(1, j))
            send("zrel", hpart(1, j), hpart(1, j), d_zlo, rs=12 + j, wait_later=False)
            hsib(1, j)
            recv(("zh", j), hpart(0, j))
            hsib(0, j)

    def hz_outer(j):
        @pl.when(is_outer)
        def _():
            recv(("zh", 4 + j), hpart(1, j))
            hsib(1, j)

    def hs_outer():
        @pl.when(is_outer)
        def _():
            for j in range(4):
                hsib(0, j)

    def hsfin(rel):
        recv(("hs", rel), *[part(1, xp, oc, t_of[rel], 0, HOME) for xp in xorder])

    def relay(r, hs=(0, 1)):
        a, rel, r0, n = ROUNDS[r]
        t = t_of[rel]
        for h in hs:
            k = 2 * a + h

            @pl.when(is_inner)
            def _():
                c = chunk(a, x, t, h, r0, n)
                recv(("z", 4 + k), c)
                send("zrel", c, c, d_zlo, rs=4 + k, wait_later=False)

    def xsend_h(r, h):
        a, rel, r0, n = ROUNDS[r]
        t = t_of[rel]
        k = 2 * a + h
        c = chunk(a, x, t, h, r0, n)
        if rel == 0:
            @pl.when(is_inner)
            def _():
                recv(("z", k), c)
        else:
            @pl.when(is_outer)
            def _():
                recv(("z", 4 + k), c)
        if h == 0:
            send(("x", r, 0, 0), c, c, d_xr)
        else:
            send(("x", r, 1, 1), c, c, d_xl)
            send(("x", r, 0, 1), c, c, d_xr)
            c = chunk(a, x, t, 0, r0, n)
            send(("x", r, 1, 0), c, c, d_xl)
            p = part(a, x, core, t, r0, n)
            send(("s", r), p, p, d_sib)

    def xsend(r):
        xsend_h(r, 0)
        xsend_h(r, 1)

    def xfwd(r):
        a, rel, r0, n = ROUNDS[r]
        t = t_of[rel]
        c = chunk(a, xl, t, 0, r0, n)
        recv(("x", r, 0, 0), c)
        send(("xf", r), c, c, d_xr)
        c = chunk(a, xr, t, 1, r0, n)
        recv(("x", r, 1, 1), c)
        send(("xf", r), c, c, d_xl)

    def xfin(r):
        a, rel, r0, n = ROUNDS[r]
        t = t_of[rel]
        recv(("x", r, 0, 1), chunk(a, xl, t, 1, r0, n))
        p = part(a, xl, core, t, r0, n)
        send(("s", r), p, p, d_sib)
        recv(("x", r, 1, 0), chunk(a, xr, t, 0, r0, n))
        p = part(a, xr, core, t, r0, n)
        send(("s", r), p, p, d_sib)
        recv(("xf", r), chunk(a, xf, t, 0, r0, n), chunk(a, xf, t, 1, r0, n))
        p = part(a, xf, core, t, r0, n)
        send(("s", r), p, p, d_sib)

    def sfin(r):
        a, rel, r0, n = ROUNDS[r]
        recv(("s", r), *[part(a, xp, oc, t_of[rel], r0, n) for xp in xorder])

    def forward(a, rel, r0, n):
        t = t_of[rel]
        terms = []
        for e in range(2 * nx):
            block = xb[a, e, rows(t * R + r0, n), :]
            cols = pl.ds((e % 2) * C, C)
            if a == 0:
                terms.append(dot(block, wgu[e // 2, cols, :], 1, 0))
            else:
                terms.append(dot(block, wdn[e // 2, :, cols], 1, 1))
        (pgu, ph)[a][rel, pl.ds(r0, n)] = functools.reduce(jnp.add, terms)

    REST = (HOME, R - HOME)

    def gate_up():
        return pgu[1, :, :F] + pgur[:, :F], pgu[1, :, F:] + pgur[:, F:]

    hsend()
    ysend(0)
    xsend_h(0, 0)
    relay(1, (0,))
    hfwd()
    xsend_h(0, 1)
    relay(1, (1,))
    hfin_a()
    yfwd(0)
    ysend(1)
    relay(3)
    xfwd(0)
    xsend(2)
    xsend(1)
    xsend(3)
    hfin_b()
    hs_outer()
    hz_inner(0)
    hz_inner(1)
    xfin(0)
    xfwd(2)
    hz_inner(2)
    yfin(0)
    sfin(0)
    hz_inner(3)
    forward(0, 0, 0, R)
    send("exg", pgu.at[0], pgur, d_zhi)
    yfwd(1)
    xfwd(1)
    xfwd(3)
    xfin(2)
    sfin(2)
    hsfin(0)
    yfin(1)
    forward(1, 0, 0, R)
    send("exh", ph.at[0], phr, d_zhi)
    xfin(1)
    for j in range(4):
        hz_outer(j)
    xfin(3)
    sfin(1)
    forward(0, 1, 0, R)
    recv("exg", pgur)
    mine, away = trow(1 - z_hi), trow(z_hi)
    gate, up = gate_up()
    ah[mine, :] = (gate * jax.nn.sigmoid(gate) * up).astype(BF)
    send("acth", ah.at[mine, :], ah.at[mine, :], d_zhi)
    hsfin(1)
    forward(1, 1, 0, HOME)
    sfin(3)
    forward(1, 1, *REST)

    recv("exh", phr)
    gate, up = gate_up()
    hg = ph[1] + phr[...]
    squashed = jax.nn.sigmoid(gate)
    activated = gate * squashed
    slope = squashed * (1.0 + gate * (1.0 - squashed))
    agu[mine, :F] = (hg * up * slope).astype(BF)
    agu[mine, F:] = (hg * activated).astype(BF)
    send("actg", agu.at[mine, :], agu.at[mine, :], d_zhi)

    order = (xf, xr, xl, x)
    RA = ((ZF, R - ZF), (0, ZF))

    def hrows(p, h):
        r0, n = RA[p]
        return pl.ds(r0 + h * (n // 2), n // 2)

    def arows(p):
        return pl.ds(*RA[p])

    def igblock(rel, xp, c):
        w = wgu[xp, pl.ds(pl.multiple_of(c * C, C), C), :]
        igp[rel, 2 * xp + c] = dot(agu[trow(t_of[rel]), :], w, 1, 1)

    def igstart(rel):
        for j, xp in enumerate(order):
            igblock(rel, xp, oc)
            send(("is", rel, j), igp.at[rel, 2 * xp + oc], sibr.at[rel, xp], d_sib)

    def igown(rel):
        for xp in order:
            igblock(rel, xp, core)

    def addsib(rel, j):
        xp = order[j]
        recv(("is", rel, j), sibr.at[rel, xp])
        igp[rel, 2 * xp + core] += sibr[rel, xp]

    def zfirst(rel, j):
        xp = order[j]
        send("zf", igp.at[rel, 2 * xp + core, arows(1), :], zfr.at[xp], d_zlo,
             rs=slot(recvs, ("zf", j)), wait_later=False)

    def igfar(p, rel, k):
        for h, d in enumerate((d_xr, d_xl)):
            fs[k, h, pl.ds(0, RA[p][1] // 2), :] = igp[rel, 2 * xf + core, hrows(p, h), :].astype(BF)
            n = pl.ds(0, RA[p][1] // 2)
            send(("if", k, h), fs.at[k, h, n, :], farr.at[k, h, n, :], d)

    def ignear(p, rel, k):
        n = pl.ds(0, RA[p][1] // 2)
        for h, (xp, d) in enumerate(((xr, d_xr), (xl, d_xl))):
            rows_h = hrows(p, 1 - h)
            if k in ROUNDED:
                ns[k, h, n, :] = igp[rel, 2 * xp + core, rows_h, :].astype(BF)
                send(("in", k), ns.at[k, h, n, :], nowr.at[k, h, n, :], d)
            else:
                send(("in", k), igp.at[rel, 2 * xp + core, rows_h, :], nearr.at[rel, h, rows_h, :], d)

    def igsecond(p, rel, k):
        for h, (xp, d) in enumerate(((xr, d_xr), (xl, d_xl))):
            n = pl.ds(0, RA[p][1] // 2)
            recv(("if", k, h), farr.at[k, h, n, :])
            igp[rel, 2 * xp + core, hrows(p, h), :] += farr[k, h, n, :].astype(F32)
            send(("in", k), igp.at[rel, 2 * xp + core, hrows(p, h), :], nearr.at[rel, h, hrows(p, h), :], d)

    def iglast(p, rel, k):
        n = pl.ds(0, RA[p][1] // 2)
        first = [nowr.at[k, h, n, :] if k in ROUNDED else nearr.at[rel, h, hrows(p, 1 - h), :] for h in range(2)]
        second = [nearr.at[rel, h, hrows(p, h), :] for h in range(2)]
        recv(("in", k), *first, *second)
        for h in range(2):
            igp[rel, 2 * x + core, hrows(p, h), :] += second[h][...] + first[1 - h][...].astype(F32)

    def igfirst(rel, when):
        addsib(rel, 0)
        igfar(0, rel, rel)
        addsib(rel, 1)
        addsib(rel, 2)
        ignear(0, rel, rel)
        addsib(rel, 3)

        @pl.when(when)
        def _():
            for j in range(4):
                zfirst(rel, j)

    def gunit(e):
        g = dot(xb[0, e, : 2 * R], agu[...], 0, 0)
        ws[e] = g
        gb[e] = g.astype(BF)

    def hunit(e):
        d = dot(ah[...], xb[1, e, : 2 * R], 0, 0)
        hs[e] = d
        hb[e] = d.astype(BF)

    sides = ((yr, d_yr), (yl, d_yl))
    def zsend(rel):
        for h in range(2):
            send("zi", igp.at[rel, 2 * x + core, hrows(0, h), :], zr.at[hrows(0, h), :], d_zlo,
                 rs=slot(recvs, ("zir", h)), wait_later=False)

    def zfadd(j):
        xp = order[j]
        recv(("zf", j), zfr.at[xp])
        igp[keep, 2 * xp + core, arows(1), :] += zfr[xp]

    def hsecond(h):
        yp, d = sides[h]
        recv(("hf", h), hfr.at[h])
        hb[2 * yp + h] = (hs[2 * yp + h] + hfr[h].astype(F32)).astype(BF)
        send("gn", hb.at[2 * yp + h], hnr.at[h, h], d)

    def gsecond(h):
        yp, d = sides[h]
        recv(("gf", h), gfr.at[h])
        gb[2 * yp + h] = (ws[2 * yp + h] + gfr[h].astype(F32)).astype(BF)
        send("gn", gb.at[2 * yp + h], gnr.at[h, h], d)

    keep = inner
    igstart(1)
    igown(1)
    recv("acth", ah.at[away, :])
    for h, (yp, d) in enumerate(sides):
        hunit(2 * yf + h)
        send(("hf", h), hb.at[2 * yf + h], hfr.at[h], d)
    igfirst(1, is_outer)
    for h, (yp, d) in enumerate(sides):
        hunit(2 * yp + 1 - h)
        send("gn", hb.at[2 * yp + 1 - h], hnr.at[h, 1 - h], d)
    recv("actg", agu.at[away, :])
    for h, (yp, d) in enumerate(sides):
        gunit(2 * yf + h)
        send(("gf", h), gb.at[2 * yf + h], gfr.at[h], d)
    igstart(0)
    igsecond(0, 1, 1)
    igown(0)
    for h, (yp, d) in enumerate(sides):
        hunit(2 * yp + h)
    igfirst(0, is_inner)
    for h, (yp, d) in enumerate(sides):
        gunit(2 * yp + 1 - h)
        send("gn", gb.at[2 * yp + 1 - h], gnr.at[h, 1 - h], d)
    for h in range(2):
        hsecond(h)
    for h, (yp, d) in enumerate(sides):
        gunit(2 * yp + h)
    iglast(0, 1, 1)

    @pl.when(is_outer)
    def _():
        zsend(1)

    zfadd(0)
    igfar(1, keep, 2)
    gsecond(0)
    gsecond(1)
    igsecond(0, 0, 0)
    zfadd(1)
    zfadd(2)
    ignear(1, keep, 2)
    for h in range(2):
        gunit(2 * y + h)
        hunit(2 * y + h)
    igsecond(1, keep, 2)
    iglast(0, 0, 0)

    @pl.when(is_inner)
    def _():
        zsend(0)

    zfadd(3)
    iglast(1, keep, 2)

    @pl.when(is_inner)
    def _():
        igs[2, pl.ds(0, ZF), :] = igp[1, 2 * x + core, arows(1), :].astype(BF)
        send("zo", igs.at[2, pl.ds(0, ZF), :], igr.at[2, pl.ds(0, ZF), :], d_zz,
             rs=slot(recvs, ("zo", 2)), wait_later=False)
        n = pl.ds(0, (R - ZF) // 2)
        for h in range(2):
            recv(("zir", h), zr.at[hrows(0, h), :])
            igs[h, n, :] = (igp[1, 2 * x + core, hrows(0, h), :] + zr[hrows(0, h), :]).astype(BF)
            send("zo", igs.at[h, n, :], igr.at[h, n, :], d_zz,
                 rs=slot(recvs, ("zo", h)), wait_later=False)

    @pl.when(is_outer)
    def _():
        ig_o[arows(1), :] = igp[0, 2 * x + core, arows(1), :].astype(BF)

    recv("gn", *[b.at[s, h] for b in (gnr, hnr) for s in range(2) for h in range(2)])
    for h in range(2):
        g = (ws[2 * y + h] + gnr[0, h].astype(F32) + gnr[1, h].astype(F32)) * factor
        gg_o[pl.ds(h * C, C), :] = g[:, :F]
        ug_o[pl.ds(h * C, C), :] = g[:, F:]
        dg_o[:, pl.ds(h * C, C)] = (hs[2 * y + h] + hnr[0, h].astype(F32) + hnr[1, h].astype(F32)) * factor

    @pl.when(is_outer)
    def _():
        for h in range(2):
            recv(("zir", h), zr.at[hrows(0, h), :])
            ig_o[hrows(0, h), :] = (igp[0, 2 * x + core, hrows(0, h), :] + zr[hrows(0, h), :]).astype(BF)

    @pl.when(is_inner)
    def _():
        zs, n = pl.ds(0, ZF), pl.ds(0, (R - ZF) // 2)
        recv(("zo", 2), igr.at[2, zs, :])
        ig_o[arows(1), :] = igr[2, zs, :]
        for h in range(2):
            recv(("zo", h), igr.at[h, n, :])
            ig_o[hrows(0, h), :] = igr[h, n, :]
        wait_bytes(ssem.at[slot(sends, "zo")], R * C * 2)
        relayed = (ROUNDS[1][3] + ROUNDS[3][3] + 4 * HOME) * C * 2
        wait_bytes(ssem.at[slot(sends, "zrel")], relayed)

    wait_bytes(ssem.at[slot(sends, "zi")], (R - ZF) * C * 4)
    wait_bytes(ssem.at[slot(sends, "zf")], 4 * ZF * C * 4)
    wait_bytes(ssem.at[slot(sends, "hs")], 8 * HOME * C * 2)
    for k, sizes in enumerate(groups):
        wait_bytes(ssem.at[slot(sends, ("group", k))], sum(sizes))
    assert len(sends) <= NSEND and len(recvs) <= NRECV, (len(sends), len(recvs))


def deliver(*refs):
    n = (len(refs) - 1) // 2
    copies = [pltpu.make_async_copy(refs[k], refs[n + k], refs[-1].at[k]) for k in range(n)]
    for c in copies:
        c.start()
    for c in copies:
        c.wait()


def shards(tokens, out_grad, gate_weight, up_weight, down_weight):
    R, C = tokens.shape
    F = gate_weight.shape[1]
    H = R // 2
    factor = 1.0 / math.sqrt(R * lax.axis_size(FSDP))
    anyspec = pl.BlockSpec(memory_space=pl.ANY)
    vm = pl.BlockSpec(memory_space=pltpu.VMEM)
    V = pltpu.VMEM
    scratch = [
        V((2, R, C), BF), V((2, 8, 2 * R + HOME, C), BF), V((4, 2 * C, 2 * F), BF), V((4, F, 2 * C), BF),
        V((2, R, 2 * F), F32), V((2, R, F), F32), V((R, 2 * F), F32), V((R, F), F32),
        V((2 * R, 2 * F), BF), V((2 * R, F), BF),
        V((2, 8, R, C), F32), V((2, 4, R, C), F32), V((3, 2, H, C), BF), V((2, 2, R, C), F32), V((3, 2, H, C), BF), V((3, 2, H, C), BF), V((3, 2, H, C), BF), V((4, ZF, C), F32),
        V((R, C), F32), V((3, H, C), BF), V((3, H, C), BF),
        V((8, C, 2 * F), F32), V((8, F, C), F32), V((8, C, 2 * F), BF), V((8, F, C), BF),
        V((2, C, 2 * F), BF), V((2, F, C), BF), V((2, 2, C, 2 * F), BF), V((2, 2, F, C), BF),
        pltpu.SemaphoreType.DMA((8,)), pltpu.SemaphoreType.DMA((NSEND,)), pltpu.SemaphoreType.DMA((NRECV,)),
    ]
    held = pl.pallas_call(
        functools.partial(kernel, factor),
        out_shape=(
            V((R, C), BF),
            V((2 * C, F), F32),
            V((2 * C, F), F32),
            V((F, 2 * C), F32),
        ),
        in_specs=[anyspec] * 5,
        out_specs=(vm,) * 4,
        scratch_shapes=scratch,
        compiler_params=pltpu.CompilerParams(
            collective_id=0, has_side_effects=True, vmem_limit_bytes=60 * 1024 * 1024),
        name="ffn_backward",
    )(tokens, out_grad, gate_weight, up_weight, down_weight)
    return pl.pallas_call(
        deliver,
        out_shape=tuple(jax.ShapeDtypeStruct(a.shape, a.dtype) for a in held),
        in_specs=[vm] * len(held),
        out_specs=(anyspec,) * len(held),
        scratch_shapes=[pltpu.SemaphoreType.DMA((len(held),))],
        name="deliver",
    )(*[pltpu.with_memory_space_constraint(a, pltpu.VMEM) for a in held])


def solution(mesh):
    finer = Mesh(mesh.devices.reshape(2, 4, 2, 4, 2), ("z_hi", "y", "z_lo", "x", "core"))
    return jax.shard_map(
        shards,
        mesh=finer,
        in_specs=(P(FSDP, TP), P(FSDP, TP), P(FSDP, TP), P(FSDP, TP), P(TP, FSDP)),
        out_specs=(P(FSDP, TP), P(FSDP, TP), P(FSDP, TP), P(TP, FSDP)),
        check_vma=False,
    )
```

```python
import functools
import math

import jax
import jax.numpy as jnp
from jax import lax
from jax.experimental import pallas as pl
from jax.experimental.pallas import tpu as pltpu
from jax.sharding import Mesh
from jax.sharding import PartitionSpec as P

FSDP = ("z_hi", "y")
TP = ("z_lo", "x", "core")
MESH = pl.DeviceIdType.MESH
BF = jnp.bfloat16
F32 = jnp.float32
NSEND, NRECV = 23, 88
GROUP = 6
ROUNDED = (0, 1)
ZF = 64
HOME = 160
ROUNDS = ((0, 0, 0, 256), (0, 1, 0, 256), (1, 0, HOME, 256 - HOME), (1, 1, HOME, 256 - HOME))


def dot(a, b, ca, cb):
    return lax.dot_general(a, b, (((ca,), (cb,)), ((), ())), preferred_element_type=F32)


def kernel(factor, tok, og, wg, wu, wd, ig_o, gg_o, ug_o, dg_o,
           own, xb, wgu, wdn, pgu, ph, pgur, phr, agu, ah, igp, sibr, farr, nearr, fs, ns, nowr, zfr, zr, igs, igr,
           ws, hs, gb, hb, gfr, hfr, gnr, hnr, lsem, ssem, rsem):
    R, C = tok.shape
    F = wg.shape[1]
    H = R // 2
    z_hi, y, z_lo, x, core = (lax.axis_index(a) for a in ("z_hi", "y", "z_lo", "x", "core"))
    inner = (z_hi - z_lo) * (z_hi - z_lo)
    is_inner, is_outer = inner == 1, inner == 0
    nx, ny = 4, 4
    xr, xl, xf = lax.rem(x + 1, nx), lax.rem(x + nx - 1, nx), lax.rem(x + 2, nx)
    yr, yl, yf = lax.rem(y + 1, ny), lax.rem(y + ny - 1, ny), lax.rem(y + 2, ny)
    oc = 1 - core
    t_of = (z_hi, 1 - z_hi)
    d_xr, d_xl = (z_hi, y, z_lo, xr, core), (z_hi, y, z_lo, xl, core)
    d_yr, d_yl = (z_hi, yr, z_lo, x, core), (z_hi, yl, z_lo, x, core)
    d_sib = (z_hi, y, z_lo, x, oc)
    d_zlo = (z_hi, y, 1 - z_lo, x, core)
    d_zhi = (1 - z_hi, y, z_lo, x, core)
    d_zz = (1 - z_hi, y, 1 - z_lo, x, core)
    d_zs = (z_lo, y, 1 - z_lo, x, core)
    partners = (d_zhi, d_zlo, d_zz, d_xr, d_xl, d_yr, d_yl, d_sib)

    sends, recvs = {}, {}

    def slot(table, name):
        return table.setdefault(name, len(table))

    for k in range(8):
        slot(recvs, ("z", k))
    for k in range(8):
        slot(recvs, ("zh", k))
    groups = []

    def size(ref):
        return math.prod(ref.shape) * jnp.dtype(ref.dtype).itemsize

    def unit_of(nbytes):
        k = nbytes // 16384
        if nbytes % 16384 == 0:
            for n in (8, 7, 6, 5, 4, 3, 2, 1):
                if k % n == 0 and k // n <= 2 * R // 16:
                    return n, 16 * (k // n)
        return None

    def wait_bytes(sem, nbytes):
        n, m = unit_of(nbytes)
        r = xb.at[0, pl.ds(0, n), pl.ds(0, m), :]
        pltpu.make_async_copy(r, r, sem).wait()

    def remote(src, dst, dev, i, j):
        return pltpu.make_async_remote_copy(
            src_ref=src, dst_ref=dst, send_sem=ssem.at[i], recv_sem=rsem.at[j],
            device_id=dev, device_id_type=MESH)

    def send(name, src, dst, dev, rs=None, wait_later=True):
        if wait_later:
            total = sum(groups[-1]) if groups else 0
            if not groups or ((len(groups[-1]) >= GROUP or total >= 1 << 21) and unit_of(total) is not None):
                groups.append([])
            groups[-1].append(size(src))
            i = slot(sends, ("group", len(groups) - 1))
        else:
            i = slot(sends, name)
        remote(src, dst, dev, i, slot(recvs, name) if rs is None else rs).start()

    def recv(name, *dsts):
        if len(dsts) == 1:
            remote(dsts[0], dsts[0], d_sib, 0, slot(recvs, name)).wait_recv()
        else:
            wait_bytes(rsem.at[slot(recvs, name)], sum(size(d) for d in dsts))

    def trow(t):
        return pl.ds(pl.multiple_of(t * R, R), R)

    def blk(a, xp, c, t):
        return xb.at[a, 2 * xp + c, trow(t), :]

    def rows(start, n):
        return pl.ds(pl.multiple_of(start, 16), n)

    def chunk(a, xp, t, h, r0, n):
        return xb.at[a, 2 * xp + core, rows(t * R + r0 + h * (n // 2), n // 2), :]

    def part(a, xp, c, t, r0, n):
        return xb.at[a, 2 * xp + c, rows(t * R + r0, n), :]

    home_at = (1 - inner) * z_hi * R + inner * 2 * R

    def home(xp, h=None):
        if h is None:
            return xb.at[1, 2 * xp + core, rows(home_at, HOME), :]
        return xb.at[1, 2 * xp + core, rows(home_at + h * (HOME // 2), HOME // 2), :]

    loads_w = [
        pltpu.make_async_copy(wg, wgu.at[y, :, pl.ds(0, F)], lsem.at[0]),
        pltpu.make_async_copy(wu, wgu.at[y, :, pl.ds(F, F)], lsem.at[1]),
        pltpu.make_async_copy(wd, wdn.at[y], lsem.at[2]),
    ]
    loads_t = [
        pltpu.make_async_copy(tok, own.at[0], lsem.at[3]),
        pltpu.make_async_copy(og, own.at[1], lsem.at[4]),
    ]
    for c in loads_t + loads_w:
        c.start()

    outer_loads = (
        (tok, blk(0, x, core, z_hi), lsem.at[5]),
        (og.at[pl.ds(HOME, R - HOME), :], part(1, x, core, z_hi, HOME, R - HOME), lsem.at[6]),
    )
    load_home = pltpu.make_async_copy(og.at[pl.ds(0, HOME), :], home(x), lsem.at[7])
    load_home.start()

    @pl.when(is_outer)
    def _():
        for c in outer_loads:
            pltpu.make_async_copy(*c).start()

    barrier = pltpu.get_barrier_semaphore()
    for d in partners:
        pl.semaphore_signal(barrier, inc=1, device_id=d, device_id_type=MESH)
    pl.semaphore_wait(barrier, len(partners))

    for c in loads_t:
        c.wait()
    load_home.wait()

    for a, rel, r0, n in (ROUNDS[0], ROUNDS[2]):
        for h in range(2):
            k = 2 * a + h
            send(("zs", k), own.at[a, pl.ds(r0 + h * (n // 2), n // 2), :], chunk(a, x, z_hi, h, r0, n), d_zs,
                 rs=4 * inner + k)

    @pl.when(is_outer)
    def _():
        for c in outer_loads:
            pltpu.make_async_copy(*c).wait()

    for c in loads_w:
        c.wait()

    def wchunk(which, yp, h):
        if which == 0:
            return wgu.at[yp, pl.ds(h * C, C), :]
        return wdn.at[yp, pl.ds(h * (F // 2), F // 2), :]

    def ysend(w):
        for h in range(2):
            send(("yf", w) if h else ("y", w, 0), wchunk(w, y, h), wchunk(w, y, h), d_yr)
            send(("yf", w) if h else ("y", w, 1), wchunk(w, y, 1 - h), wchunk(w, y, 1 - h), d_yl)

    def yfwd(w):
        recv(("y", w, 0), wchunk(w, yl, 0))
        send(("yf", w), wchunk(w, yl, 0), wchunk(w, yl, 0), d_yr)
        recv(("y", w, 1), wchunk(w, yr, 1))
        send(("yf", w), wchunk(w, yr, 1), wchunk(w, yr, 1), d_yl)

    def yfin(w):
        recv(("yf", w), wchunk(w, yl, 1), wchunk(w, yr, 0), wchunk(w, yf, 0), wchunk(w, yf, 1))

    def hsend():
        for h in range(2):
            send(("h", 0, h), home(x, h), home(x, h), d_xr)
            send(("h", 1, 1 - h), home(x, 1 - h), home(x, 1 - h), d_xl)

    def homez(j, xp):
        send(("hz", j), home(xp), xb.at[1, 2 * xp + core, rows(z_hi * R, HOME), :], d_zs, rs=8 + 4 * inner + j)

    def hfwd():
        recv(("h", 0, 0), home(xl, 0))
        send("hf", home(xl, 0), home(xl, 0), d_xr)
        recv(("h", 1, 1), home(xr, 1))
        send("hf", home(xr, 1), home(xr, 1), d_xl)

    def hfin_a():
        homez(0, x)
        recv(("h", 0, 1), home(xl, 1))
        homez(1, xl)
        recv(("h", 1, 0), home(xr, 0))
        homez(2, xr)

    def hfin_b():
        recv("hf", home(xf, 0), home(xf, 1))
        homez(3, xf)

    xorder = (x, xl, xr, xf)

    def hpart(rel, j):
        return part(1, xorder[j], core, t_of[rel], 0, HOME)

    def hsib(rel, j):
        send("hs", hpart(rel, j), hpart(rel, j), d_sib, rs=slot(recvs, ("hs", rel)), wait_later=False)

    def hz_inner(j):
        @pl.when(is_inner)
        def _():
            recv(("zh", 4 + j), hpart(1, j))
            send("zrel", hpart(1, j), hpart(1, j), d_zlo, rs=12 + j, wait_later=False)
            hsib(1, j)
            recv(("zh", j), hpart(0, j))
            hsib(0, j)

    def hz_outer(j):
        @pl.when(is_outer)
        def _():
            recv(("zh", 4 + j), hpart(1, j))
            hsib(1, j)

    def hs_outer():
        @pl.when(is_outer)
        def _():
            for j in range(4):
                hsib(0, j)

    def hsfin(rel):
        recv(("hs", rel), *[part(1, xp, oc, t_of[rel], 0, HOME) for xp in xorder])

    def relay(r, hs=(0, 1)):
        a, rel, r0, n = ROUNDS[r]
        t = t_of[rel]
        for h in hs:
            k = 2 * a + h

            @pl.when(is_inner)
            def _():
                c = chunk(a, x, t, h, r0, n)
                recv(("z", 4 + k), c)
                send("zrel", c, c, d_zlo, rs=4 + k, wait_later=False)

    def xsend_h(r, h):
        a, rel, r0, n = ROUNDS[r]
        t = t_of[rel]
        k = 2 * a + h
        c = chunk(a, x, t, h, r0, n)
        if rel == 0:
            @pl.when(is_inner)
            def _():
                recv(("z", k), c)
        else:
            @pl.when(is_outer)
            def _():
                recv(("z", 4 + k), c)
        if h == 0:
            send(("x", r, 0, 0), c, c, d_xr)
        else:
            send(("x", r, 1, 1), c, c, d_xl)
            send(("x", r, 0, 1), c, c, d_xr)
            c = chunk(a, x, t, 0, r0, n)
            send(("x", r, 1, 0), c, c, d_xl)
            p = part(a, x, core, t, r0, n)
            send(("s", r), p, p, d_sib)

    def xsend(r):
        xsend_h(r, 0)
        xsend_h(r, 1)

    def xfwd(r):
        a, rel, r0, n = ROUNDS[r]
        t = t_of[rel]
        c = chunk(a, xl, t, 0, r0, n)
        recv(("x", r, 0, 0), c)
        send(("xf", r), c, c, d_xr)
        c = chunk(a, xr, t, 1, r0, n)
        recv(("x", r, 1, 1), c)
        send(("xf", r), c, c, d_xl)

    def xfin(r):
        a, rel, r0, n = ROUNDS[r]
        t = t_of[rel]
        recv(("x", r, 0, 1), chunk(a, xl, t, 1, r0, n))
        p = part(a, xl, core, t, r0, n)
        send(("s", r), p, p, d_sib)
        recv(("x", r, 1, 0), chunk(a, xr, t, 0, r0, n))
        p = part(a, xr, core, t, r0, n)
        send(("s", r), p, p, d_sib)
        recv(("xf", r), chunk(a, xf, t, 0, r0, n), chunk(a, xf, t, 1, r0, n))
        p = part(a, xf, core, t, r0, n)
        send(("s", r), p, p, d_sib)

    def sfin(r):
        a, rel, r0, n = ROUNDS[r]
        recv(("s", r), *[part(a, xp, oc, t_of[rel], r0, n) for xp in xorder])

    def forward(a, rel, r0, n):
        t = t_of[rel]
        terms = []
        for e in range(2 * nx):
            block = xb[a, e, rows(t * R + r0, n), :]
            cols = pl.ds((e % 2) * C, C)
            if a == 0:
                terms.append(dot(block, wgu[e // 2, cols, :], 1, 0))
            else:
                terms.append(dot(block, wdn[e // 2, :, cols], 1, 1))
        (pgu, ph)[a][rel, pl.ds(r0, n)] = functools.reduce(jnp.add, terms)

    REST = (HOME, R - HOME)

    def gate_up():
        return pgu[1, :, :F] + pgur[:, :F], pgu[1, :, F:] + pgur[:, F:]

    hsend()
    ysend(0)
    xsend_h(0, 0)
    relay(1, (0,))
    hfwd()
    xsend_h(0, 1)
    relay(1, (1,))
    hfin_a()
    yfwd(0)
    ysend(1)
    relay(3)
    xfwd(0)
    xsend(2)
    xsend(1)
    xsend(3)
    hfin_b()
    hs_outer()
    hz_inner(0)
    hz_inner(1)
    xfin(0)
    xfwd(2)
    hz_inner(2)
    yfin(0)
    sfin(0)
    hz_inner(3)
    forward(0, 0, 0, R)
    send("exg", pgu.at[0], pgur, d_zhi)
    yfwd(1)
    xfwd(1)
    xfwd(3)
    xfin(2)
    sfin(2)
    hsfin(0)
    yfin(1)
    forward(1, 0, 0, R)
    send("exh", ph.at[0], phr, d_zhi)
    xfin(1)
    for j in range(4):
        hz_outer(j)
    xfin(3)
    sfin(1)
    forward(0, 1, 0, R)
    recv("exg", pgur)
    mine, away = trow(1 - z_hi), trow(z_hi)
    gate, up = gate_up()
    ah[mine, :] = (gate * jax.nn.sigmoid(gate) * up).astype(BF)
    send("acth", ah.at[mine, :], ah.at[mine, :], d_zhi)
    hsfin(1)
    forward(1, 1, 0, HOME)
    sfin(3)
    forward(1, 1, *REST)

    recv("exh", phr)
    gate, up = gate_up()
    hg = ph[1] + phr[...]
    squashed = jax.nn.sigmoid(gate)
    activated = gate * squashed
    slope = squashed * (1.0 + gate * (1.0 - squashed))
    agu[mine, :F] = (hg * up * slope).astype(BF)
    agu[mine, F:] = (hg * activated).astype(BF)
    send("actg", agu.at[mine, :], agu.at[mine, :], d_zhi)

    order = (xf, xr, xl, x)
    RA = ((ZF, R - ZF), (0, ZF))

    def hrows(p, h):
        r0, n = RA[p]
        return pl.ds(r0 + h * (n // 2), n // 2)

    def arows(p):
        return pl.ds(*RA[p])

    def igblock(rel, xp, c):
        w = wgu[xp, pl.ds(pl.multiple_of(c * C, C), C), :]
        igp[rel, 2 * xp + c] = dot(agu[trow(t_of[rel]), :], w, 1, 1)

    def igstart(rel):
        for j, xp in enumerate(order):
            igblock(rel, xp, oc)
            send(("is", rel, j), igp.at[rel, 2 * xp + oc], sibr.at[rel, xp], d_sib)

    def igown(rel):
        for xp in order:
            igblock(rel, xp, core)

    def addsib(rel, j):
        xp = order[j]
        recv(("is", rel, j), sibr.at[rel, xp])
        igp[rel, 2 * xp + core] += sibr[rel, xp]

    def zfirst(rel, j):
        xp = order[j]
        send("zf", igp.at[rel, 2 * xp + core, arows(1), :], zfr.at[xp], d_zlo,
             rs=slot(recvs, ("zf", j)), wait_later=False)

    def igfar(p, rel, k):
        for h, d in enumerate((d_xr, d_xl)):
            fs[k, h, pl.ds(0, RA[p][1] // 2), :] = igp[rel, 2 * xf + core, hrows(p, h), :].astype(BF)
            n = pl.ds(0, RA[p][1] // 2)
            send(("if", k, h), fs.at[k, h, n, :], farr.at[k, h, n, :], d)

    def ignear(p, rel, k):
        n = pl.ds(0, RA[p][1] // 2)
        for h, (xp, d) in enumerate(((xr, d_xr), (xl, d_xl))):
            rows_h = hrows(p, 1 - h)
            if k in ROUNDED:
                ns[k, h, n, :] = igp[rel, 2 * xp + core, rows_h, :].astype(BF)
                send(("in", k), ns.at[k, h, n, :], nowr.at[k, h, n, :], d)
            else:
                send(("in", k), igp.at[rel, 2 * xp + core, rows_h, :], nearr.at[rel, h, rows_h, :], d)

    def igsecond(p, rel, k):
        for h, (xp, d) in enumerate(((xr, d_xr), (xl, d_xl))):
            n = pl.ds(0, RA[p][1] // 2)
            recv(("if", k, h), farr.at[k, h, n, :])
            igp[rel, 2 * xp + core, hrows(p, h), :] += farr[k, h, n, :].astype(F32)
            send(("in", k), igp.at[rel, 2 * xp + core, hrows(p, h), :], nearr.at[rel, h, hrows(p, h), :], d)

    def iglast(p, rel, k):
        n = pl.ds(0, RA[p][1] // 2)
        first = [nowr.at[k, h, n, :] if k in ROUNDED else nearr.at[rel, h, hrows(p, 1 - h), :] for h in range(2)]
        second = [nearr.at[rel, h, hrows(p, h), :] for h in range(2)]
        recv(("in", k), *first, *second)
        for h in range(2):
            igp[rel, 2 * x + core, hrows(p, h), :] += second[h][...] + first[1 - h][...].astype(F32)

    def igfirst(rel, when):
        addsib(rel, 0)
        igfar(0, rel, rel)
        addsib(rel, 1)
        addsib(rel, 2)
        ignear(0, rel, rel)
        addsib(rel, 3)

        @pl.when(when)
        def _():
            for j in range(4):
                zfirst(rel, j)

    def gunit(e):
        g = dot(xb[0, e, : 2 * R], agu[...], 0, 0)
        ws[e] = g
        gb[e] = g.astype(BF)

    def hunit(e):
        d = dot(ah[...], xb[1, e, : 2 * R], 0, 0)
        hs[e] = d
        hb[e] = d.astype(BF)

    sides = ((yr, d_yr), (yl, d_yl))
    def zsend(rel):
        for h in range(2):
            send("zi", igp.at[rel, 2 * x + core, hrows(0, h), :], zr.at[hrows(0, h), :], d_zlo,
                 rs=slot(recvs, ("zir", h)), wait_later=False)

    def zfadd(j):
        xp = order[j]
        recv(("zf", j), zfr.at[xp])
        igp[keep, 2 * xp + core, arows(1), :] += zfr[xp]

    def hsecond(h):
        yp, d = sides[h]
        recv(("hf", h), hfr.at[h])
        hb[2 * yp + h] = (hs[2 * yp + h] + hfr[h].astype(F32)).astype(BF)
        send("gn", hb.at[2 * yp + h], hnr.at[h, h], d)

    def gsecond(h):
        yp, d = sides[h]
        recv(("gf", h), gfr.at[h])
        gb[2 * yp + h] = (ws[2 * yp + h] + gfr[h].astype(F32)).astype(BF)
        send("gn", gb.at[2 * yp + h], gnr.at[h, h], d)

    keep = inner
    igstart(1)
    igown(1)
    recv("acth", ah.at[away, :])
    for h, (yp, d) in enumerate(sides):
        hunit(2 * yf + h)
        send(("hf", h), hb.at[2 * yf + h], hfr.at[h], d)
    igfirst(1, is_outer)
    for h, (yp, d) in enumerate(sides):
        hunit(2 * yp + 1 - h)
        send("gn", hb.at[2 * yp + 1 - h], hnr.at[h, 1 - h], d)
    recv("actg", agu.at[away, :])
    for h, (yp, d) in enumerate(sides):
        gunit(2 * yf + h)
        send(("gf", h), gb.at[2 * yf + h], gfr.at[h], d)
    igstart(0)
    igsecond(0, 1, 1)
    igown(0)
    for h, (yp, d) in enumerate(sides):
        hunit(2 * yp + h)
    igfirst(0, is_inner)
    for h, (yp, d) in enumerate(sides):
        gunit(2 * yp + 1 - h)
        send("gn", gb.at[2 * yp + 1 - h], gnr.at[h, 1 - h], d)
    for h in range(2):
        hsecond(h)
    for h, (yp, d) in enumerate(sides):
        gunit(2 * yp + h)
    iglast(0, 1, 1)

    @pl.when(is_outer)
    def _():
        zsend(1)

    zfadd(0)
    igfar(1, keep, 2)
    gsecond(0)
    gsecond(1)
    igsecond(0, 0, 0)
    zfadd(1)
    zfadd(2)
    ignear(1, keep, 2)
    for h in range(2):
        gunit(2 * y + h)
        hunit(2 * y + h)
    igsecond(1, keep, 2)
    iglast(0, 0, 0)

    @pl.when(is_inner)
    def _():
        zsend(0)

    zfadd(3)
    iglast(1, keep, 2)

    @pl.when(is_inner)
    def _():
        igs[2, pl.ds(0, ZF), :] = igp[1, 2 * x + core, arows(1), :].astype(BF)
        send("zo", igs.at[2, pl.ds(0, ZF), :], igr.at[2, pl.ds(0, ZF), :], d_zz,
             rs=slot(recvs, ("zo", 2)), wait_later=False)
        n = pl.ds(0, (R - ZF) // 2)
        for h in range(2):
            recv(("zir", h), zr.at[hrows(0, h), :])
            igs[h, n, :] = (igp[1, 2 * x + core, hrows(0, h), :] + zr[hrows(0, h), :]).astype(BF)
            send("zo", igs.at[h, n, :], igr.at[h, n, :], d_zz,
                 rs=slot(recvs, ("zo", h)), wait_later=False)

    @pl.when(is_outer)
    def _():
        ig_o[arows(1), :] = igp[0, 2 * x + core, arows(1), :].astype(BF)

    recv("gn", *[b.at[s, h] for b in (gnr, hnr) for s in range(2) for h in range(2)])
    for h in range(2):
        g = (ws[2 * y + h] + gnr[0, h].astype(F32) + gnr[1, h].astype(F32)) * factor
        gg_o[pl.ds(h * C, C), :] = g[:, :F]
        ug_o[pl.ds(h * C, C), :] = g[:, F:]
        dg_o[:, pl.ds(h * C, C)] = (hs[2 * y + h] + hnr[0, h].astype(F32) + hnr[1, h].astype(F32)) * factor

    @pl.when(is_outer)
    def _():
        for h in range(2):
            recv(("zir", h), zr.at[hrows(0, h), :])
            ig_o[hrows(0, h), :] = (igp[0, 2 * x + core, hrows(0, h), :] + zr[hrows(0, h), :]).astype(BF)

    @pl.when(is_inner)
    def _():
        zs, n = pl.ds(0, ZF), pl.ds(0, (R - ZF) // 2)
        recv(("zo", 2), igr.at[2, zs, :])
        ig_o[arows(1), :] = igr[2, zs, :]
        for h in range(2):
            recv(("zo", h), igr.at[h, n, :])
            ig_o[hrows(0, h), :] = igr[h, n, :]
        wait_bytes(ssem.at[slot(sends, "zo")], R * C * 2)
        relayed = (ROUNDS[1][3] + ROUNDS[3][3] + 4 * HOME) * C * 2
        wait_bytes(ssem.at[slot(sends, "zrel")], relayed)

    wait_bytes(ssem.at[slot(sends, "zi")], (R - ZF) * C * 4)
    wait_bytes(ssem.at[slot(sends, "zf")], 4 * ZF * C * 4)
    wait_bytes(ssem.at[slot(sends, "hs")], 8 * HOME * C * 2)
    for k, sizes in enumerate(groups):
        wait_bytes(ssem.at[slot(sends, ("group", k))], sum(sizes))
    assert len(sends) <= NSEND and len(recvs) <= NRECV, (len(sends), len(recvs))


def deliver(*refs):
    n = (len(refs) - 1) // 2
    copies = [pltpu.make_async_copy(refs[k], refs[n + k], refs[-1].at[k]) for k in range(n)]
    for c in copies:
        c.start()
    for c in copies:
        c.wait()


def shards(tokens, out_grad, gate_weight, up_weight, down_weight):
    R, C = tokens.shape
    F = gate_weight.shape[1]
    H = R // 2
    factor = 1.0 / math.sqrt(R * lax.axis_size(FSDP))
    anyspec = pl.BlockSpec(memory_space=pl.ANY)
    vm = pl.BlockSpec(memory_space=pltpu.VMEM)
    V = pltpu.VMEM
    scratch = [
        V((2, R, C), BF), V((2, 8, 2 * R + HOME, C), BF), V((4, 2 * C, 2 * F), BF), V((4, F, 2 * C), BF),
        V((2, R, 2 * F), F32), V((2, R, F), F32), V((R, 2 * F), F32), V((R, F), F32),
        V((2 * R, 2 * F), BF), V((2 * R, F), BF),
        V((2, 8, R, C), F32), V((2, 4, R, C), F32), V((3, 2, H, C), BF), V((2, 2, R, C), F32), V((3, 2, H, C), BF), V((3, 2, H, C), BF), V((3, 2, H, C), BF), V((4, ZF, C), F32),
        V((R, C), F32), V((3, H, C), BF), V((3, H, C), BF),
        V((8, C, 2 * F), F32), V((8, F, C), F32), V((8, C, 2 * F), BF), V((8, F, C), BF),
        V((2, C, 2 * F), BF), V((2, F, C), BF), V((2, 2, C, 2 * F), BF), V((2, 2, F, C), BF),
        pltpu.SemaphoreType.DMA((8,)), pltpu.SemaphoreType.DMA((NSEND,)), pltpu.SemaphoreType.DMA((NRECV,)),
    ]
    held = pl.pallas_call(
        functools.partial(kernel, factor),
        out_shape=(
            V((R, C), BF),
            V((2 * C, F), F32),
            V((2 * C, F), F32),
            V((F, 2 * C), F32),
        ),
        in_specs=[anyspec] * 5,
        out_specs=(vm,) * 4,
        scratch_shapes=scratch,
        compiler_params=pltpu.CompilerParams(
            collective_id=0, has_side_effects=True, vmem_limit_bytes=60 * 1024 * 1024),
        name="ffn_backward",
    )(tokens, out_grad, gate_weight, up_weight, down_weight)
    return pl.pallas_call(
        deliver,
        out_shape=tuple(jax.ShapeDtypeStruct(a.shape, a.dtype) for a in held),
        in_specs=[vm] * len(held),
        out_specs=(anyspec,) * len(held),
        scratch_shapes=[pltpu.SemaphoreType.DMA((len(held),))],
        name="deliver",
    )(*[pltpu.with_memory_space_constraint(a, pltpu.VMEM) for a in held])


def solution(mesh):
    finer = Mesh(mesh.devices.reshape(2, 4, 2, 4, 2), ("z_hi", "y", "z_lo", "x", "core"))
    return jax.shard_map(
        shards,
        mesh=finer,
        in_specs=(P(FSDP, TP), P(FSDP, TP), P(FSDP, TP), P(FSDP, TP), P(TP, FSDP)),
        out_specs=(P(FSDP, TP), P(FSDP, TP), P(FSDP, TP), P(TP, FSDP)),
        check_vma=False,
    )
```

```python
import functools
import math

import jax
import jax.numpy as jnp
from jax import lax
from jax.experimental import pallas as pl
from jax.experimental.pallas import tpu as pltpu
from jax.sharding import Mesh
from jax.sharding import PartitionSpec as P

FSDP = ("z_hi", "y")
TP = ("z_lo", "x", "core")
MESH = pl.DeviceIdType.MESH
BF = jnp.bfloat16
F32 = jnp.float32
NSEND, NRECV = 23, 88
GROUP = 6
ROUNDED = (0, 1, 2)
ZF = 64
HOME = 160
ROUNDS = ((0, 0, 0, 256), (0, 1, 0, 256), (1, 0, HOME, 256 - HOME), (1, 1, HOME, 256 - HOME))


def dot(a, b, ca, cb):
    return lax.dot_general(a, b, (((ca,), (cb,)), ((), ())), preferred_element_type=F32)


def kernel(factor, tok, og, wg, wu, wd, ig_o, gg_o, ug_o, dg_o,
           own, xb, wgu, wdn, pgu, ph, pgur, phr, agu, ah, igp, sibr, farr, nearr, fs, ns, nowr, zfr, zr, igs, igr,
           ws, hs, gb, hb, gfr, hfr, gnr, hnr, lsem, ssem, rsem):
    R, C = tok.shape
    F = wg.shape[1]
    H = R // 2
    z_hi, y, z_lo, x, core = (lax.axis_index(a) for a in ("z_hi", "y", "z_lo", "x", "core"))
    inner = (z_hi - z_lo) * (z_hi - z_lo)
    is_inner, is_outer = inner == 1, inner == 0
    nx, ny = 4, 4
    xr, xl, xf = lax.rem(x + 1, nx), lax.rem(x + nx - 1, nx), lax.rem(x + 2, nx)
    yr, yl, yf = lax.rem(y + 1, ny), lax.rem(y + ny - 1, ny), lax.rem(y + 2, ny)
    oc = 1 - core
    t_of = (z_hi, 1 - z_hi)
    d_xr, d_xl = (z_hi, y, z_lo, xr, core), (z_hi, y, z_lo, xl, core)
    d_yr, d_yl = (z_hi, yr, z_lo, x, core), (z_hi, yl, z_lo, x, core)
    d_sib = (z_hi, y, z_lo, x, oc)
    d_zlo = (z_hi, y, 1 - z_lo, x, core)
    d_zhi = (1 - z_hi, y, z_lo, x, core)
    d_zz = (1 - z_hi, y, 1 - z_lo, x, core)
    d_zs = (z_lo, y, 1 - z_lo, x, core)
    partners = (d_zhi, d_zlo, d_zz, d_xr, d_xl, d_yr, d_yl, d_sib)

    sends, recvs = {}, {}

    def slot(table, name):
        return table.setdefault(name, len(table))

    for k in range(8):
        slot(recvs, ("z", k))
    for k in range(8):
        slot(recvs, ("zh", k))
    groups = []

    def size(ref):
        return math.prod(ref.shape) * jnp.dtype(ref.dtype).itemsize

    def unit_of(nbytes):
        k = nbytes // 16384
        if nbytes % 16384 == 0:
            for n in (8, 7, 6, 5, 4, 3, 2, 1):
                if k % n == 0 and k // n <= 2 * R // 16:
                    return n, 16 * (k // n)
        return None

    def wait_bytes(sem, nbytes):
        n, m = unit_of(nbytes)
        r = xb.at[0, pl.ds(0, n), pl.ds(0, m), :]
        pltpu.make_async_copy(r, r, sem).wait()

    def remote(src, dst, dev, i, j):
        return pltpu.make_async_remote_copy(
            src_ref=src, dst_ref=dst, send_sem=ssem.at[i], recv_sem=rsem.at[j],
            device_id=dev, device_id_type=MESH)

    def send(name, src, dst, dev, rs=None, wait_later=True):
        if wait_later:
            total = sum(groups[-1]) if groups else 0
            if not groups or ((len(groups[-1]) >= GROUP or total >= 1 << 21) and unit_of(total) is not None):
                groups.append([])
            groups[-1].append(size(src))
            i = slot(sends, ("group", len(groups) - 1))
        else:
            i = slot(sends, name)
        remote(src, dst, dev, i, slot(recvs, name) if rs is None else rs).start()

    def recv(name, *dsts):
        if len(dsts) == 1:
            remote(dsts[0], dsts[0], d_sib, 0, slot(recvs, name)).wait_recv()
        else:
            wait_bytes(rsem.at[slot(recvs, name)], sum(size(d) for d in dsts))

    def trow(t):
        return pl.ds(pl.multiple_of(t * R, R), R)

    def blk(a, xp, c, t):
        return xb.at[a, 2 * xp + c, trow(t), :]

    def rows(start, n):
        return pl.ds(pl.multiple_of(start, 16), n)

    def chunk(a, xp, t, h, r0, n):
        return xb.at[a, 2 * xp + core, rows(t * R + r0 + h * (n // 2), n // 2), :]

    def part(a, xp, c, t, r0, n):
        return xb.at[a, 2 * xp + c, rows(t * R + r0, n), :]

    home_at = (1 - inner) * z_hi * R + inner * 2 * R

    def home(xp, h=None):
        if h is None:
            return xb.at[1, 2 * xp + core, rows(home_at, HOME), :]
        return xb.at[1, 2 * xp + core, rows(home_at + h * (HOME // 2), HOME // 2), :]

    loads_w = [
        pltpu.make_async_copy(wg, wgu.at[y, :, pl.ds(0, F)], lsem.at[0]),
        pltpu.make_async_copy(wu, wgu.at[y, :, pl.ds(F, F)], lsem.at[1]),
        pltpu.make_async_copy(wd, wdn.at[y], lsem.at[2]),
    ]
    loads_t = [
        pltpu.make_async_copy(tok, own.at[0], lsem.at[3]),
        pltpu.make_async_copy(og, own.at[1], lsem.at[4]),
    ]
    for c in loads_t + loads_w:
        c.start()

    outer_loads = (
        (tok, blk(0, x, core, z_hi), lsem.at[5]),
        (og.at[pl.ds(HOME, R - HOME), :], part(1, x, core, z_hi, HOME, R - HOME), lsem.at[6]),
    )
    load_home = pltpu.make_async_copy(og.at[pl.ds(0, HOME), :], home(x), lsem.at[7])
    load_home.start()

    @pl.when(is_outer)
    def _():
        for c in outer_loads:
            pltpu.make_async_copy(*c).start()

    barrier = pltpu.get_barrier_semaphore()
    for d in partners:
        pl.semaphore_signal(barrier, inc=1, device_id=d, device_id_type=MESH)
    pl.semaphore_wait(barrier, len(partners))

    for c in loads_t:
        c.wait()
    load_home.wait()

    for a, rel, r0, n in (ROUNDS[0], ROUNDS[2]):
        for h in range(2):
            k = 2 * a + h
            send(("zs", k), own.at[a, pl.ds(r0 + h * (n // 2), n // 2), :], chunk(a, x, z_hi, h, r0, n), d_zs,
                 rs=4 * inner + k)

    @pl.when(is_outer)
    def _():
        for c in outer_loads:
            pltpu.make_async_copy(*c).wait()

    for c in loads_w:
        c.wait()

    def wchunk(which, yp, h):
        if which == 0:
            return wgu.at[yp, pl.ds(h * C, C), :]
        return wdn.at[yp, pl.ds(h * (F // 2), F // 2), :]

    def ysend(w):
        for h in range(2):
            send(("yf", w) if h else ("y", w, 0), wchunk(w, y, h), wchunk(w, y, h), d_yr)
            send(("yf", w) if h else ("y", w, 1), wchunk(w, y, 1 - h), wchunk(w, y, 1 - h), d_yl)

    def yfwd(w):
        recv(("y", w, 0), wchunk(w, yl, 0))
        send(("yf", w), wchunk(w, yl, 0), wchunk(w, yl, 0), d_yr)
        recv(("y", w, 1), wchunk(w, yr, 1))
        send(("yf", w), wchunk(w, yr, 1), wchunk(w, yr, 1), d_yl)

    def yfin(w):
        recv(("yf", w), wchunk(w, yl, 1), wchunk(w, yr, 0), wchunk(w, yf, 0), wchunk(w, yf, 1))

    def hsend():
        for h in range(2):
            send(("h", 0, h), home(x, h), home(x, h), d_xr)
            send(("h", 1, 1 - h), home(x, 1 - h), home(x, 1 - h), d_xl)

    def homez(j, xp):
        send(("hz", j), home(xp), xb.at[1, 2 * xp + core, rows(z_hi * R, HOME), :], d_zs, rs=8 + 4 * inner + j)

    def hfwd():
        recv(("h", 0, 0), home(xl, 0))
        send("hf", home(xl, 0), home(xl, 0), d_xr)
        recv(("h", 1, 1), home(xr, 1))
        send("hf", home(xr, 1), home(xr, 1), d_xl)

    def hfin_a():
        homez(0, x)
        recv(("h", 0, 1), home(xl, 1))
        homez(1, xl)
        recv(("h", 1, 0), home(xr, 0))
        homez(2, xr)

    def hfin_b():
        recv("hf", home(xf, 0), home(xf, 1))
        homez(3, xf)

    xorder = (x, xl, xr, xf)

    def hpart(rel, j):
        return part(1, xorder[j], core, t_of[rel], 0, HOME)

    def hsib(rel, j):
        send("hs", hpart(rel, j), hpart(rel, j), d_sib, rs=slot(recvs, ("hs", rel)), wait_later=False)

    def hz_inner(j):
        @pl.when(is_inner)
        def _():
            recv(("zh", 4 + j), hpart(1, j))
            send("zrel", hpart(1, j), hpart(1, j), d_zlo, rs=12 + j, wait_later=False)
            hsib(1, j)
            recv(("zh", j), hpart(0, j))
            hsib(0, j)

    def hz_outer(j):
        @pl.when(is_outer)
        def _():
            recv(("zh", 4 + j), hpart(1, j))
            hsib(1, j)

    def hs_outer():
        @pl.when(is_outer)
        def _():
            for j in range(4):
                hsib(0, j)

    def hsfin(rel):
        recv(("hs", rel), *[part(1, xp, oc, t_of[rel], 0, HOME) for xp in xorder])

    def relay(r, hs=(0, 1)):
        a, rel, r0, n = ROUNDS[r]
        t = t_of[rel]
        for h in hs:
            k = 2 * a + h

            @pl.when(is_inner)
            def _():
                c = chunk(a, x, t, h, r0, n)
                recv(("z", 4 + k), c)
                send("zrel", c, c, d_zlo, rs=4 + k, wait_later=False)

    def xsend_h(r, h):
        a, rel, r0, n = ROUNDS[r]
        t = t_of[rel]
        k = 2 * a + h
        c = chunk(a, x, t, h, r0, n)
        if rel == 0:
            @pl.when(is_inner)
            def _():
                recv(("z", k), c)
        else:
            @pl.when(is_outer)
            def _():
                recv(("z", 4 + k), c)
        if h == 0:
            send(("x", r, 0, 0), c, c, d_xr)
        else:
            send(("x", r, 1, 1), c, c, d_xl)
            send(("x", r, 0, 1), c, c, d_xr)
            c = chunk(a, x, t, 0, r0, n)
            send(("x", r, 1, 0), c, c, d_xl)
            p = part(a, x, core, t, r0, n)
            send(("s", r), p, p, d_sib)

    def xsend(r):
        xsend_h(r, 0)
        xsend_h(r, 1)

    def xfwd(r):
        a, rel, r0, n = ROUNDS[r]
        t = t_of[rel]
        c = chunk(a, xl, t, 0, r0, n)
        recv(("x", r, 0, 0), c)
        send(("xf", r), c, c, d_xr)
        c = chunk(a, xr, t, 1, r0, n)
        recv(("x", r, 1, 1), c)
        send(("xf", r), c, c, d_xl)

    def xfin(r):
        a, rel, r0, n = ROUNDS[r]
        t = t_of[rel]
        recv(("x", r, 0, 1), chunk(a, xl, t, 1, r0, n))
        p = part(a, xl, core, t, r0, n)
        send(("s", r), p, p, d_sib)
        recv(("x", r, 1, 0), chunk(a, xr, t, 0, r0, n))
        p = part(a, xr, core, t, r0, n)
        send(("s", r), p, p, d_sib)
        recv(("xf", r), chunk(a, xf, t, 0, r0, n), chunk(a, xf, t, 1, r0, n))
        p = part(a, xf, core, t, r0, n)
        send(("s", r), p, p, d_sib)

    def sfin(r):
        a, rel, r0, n = ROUNDS[r]
        recv(("s", r), *[part(a, xp, oc, t_of[rel], r0, n) for xp in xorder])

    def forward(a, rel, r0, n):
        t = t_of[rel]
        terms = []
        for e in range(2 * nx):
            block = xb[a, e, rows(t * R + r0, n), :]
            cols = pl.ds((e % 2) * C, C)
            if a == 0:
                terms.append(dot(block, wgu[e // 2, cols, :], 1, 0))
            else:
                terms.append(dot(block, wdn[e // 2, :, cols], 1, 1))
        (pgu, ph)[a][rel, pl.ds(r0, n)] = functools.reduce(jnp.add, terms)

    REST = (HOME, R - HOME)

    def gate_up():
        return pgu[1, :, :F] + pgur[:, :F], pgu[1, :, F:] + pgur[:, F:]

    hsend()
    ysend(0)
    xsend_h(0, 0)
    relay(1, (0,))
    hfwd()
    xsend_h(0, 1)
    relay(1, (1,))
    hfin_a()
    yfwd(0)
    ysend(1)
    relay(3)
    xfwd(0)
    xsend(2)
    xsend(1)
    xsend(3)
    hfin_b()
    hs_outer()
    hz_inner(0)
    hz_inner(1)
    xfin(0)
    xfwd(2)
    hz_inner(2)
    yfin(0)
    sfin(0)
    hz_inner(3)
    forward(0, 0, 0, R)
    send("exg", pgu.at[0], pgur, d_zhi)
    yfwd(1)
    xfwd(1)
    xfwd(3)
    xfin(2)
    sfin(2)
    hsfin(0)
    yfin(1)
    forward(1, 0, 0, R)
    send("exh", ph.at[0], phr, d_zhi)
    xfin(1)
    for j in range(4):
        hz_outer(j)
    xfin(3)
    sfin(1)
    forward(0, 1, 0, R)
    recv("exg", pgur)
    mine, away = trow(1 - z_hi), trow(z_hi)
    gate, up = gate_up()
    ah[mine, :] = (gate * jax.nn.sigmoid(gate) * up).astype(BF)
    send("acth", ah.at[mine, :], ah.at[mine, :], d_zhi)
    hsfin(1)
    forward(1, 1, 0, HOME)
    sfin(3)
    forward(1, 1, *REST)

    recv("exh", phr)
    gate, up = gate_up()
    hg = ph[1] + phr[...]
    squashed = jax.nn.sigmoid(gate)
    activated = gate * squashed
    slope = squashed * (1.0 + gate * (1.0 - squashed))
    agu[mine, :F] = (hg * up * slope).astype(BF)
    agu[mine, F:] = (hg * activated).astype(BF)
    send("actg", agu.at[mine, :], agu.at[mine, :], d_zhi)

    order = (xf, xr, xl, x)
    RA = ((ZF, R - ZF), (0, ZF))

    def hrows(p, h):
        r0, n = RA[p]
        return pl.ds(r0 + h * (n // 2), n // 2)

    def arows(p):
        return pl.ds(*RA[p])

    def igblock(rel, xp, c):
        w = wgu[xp, pl.ds(pl.multiple_of(c * C, C), C), :]
        igp[rel, 2 * xp + c] = dot(agu[trow(t_of[rel]), :], w, 1, 1)

    def igstart(rel):
        for j, xp in enumerate(order):
            igblock(rel, xp, oc)
            send(("is", rel, j), igp.at[rel, 2 * xp + oc], sibr.at[rel, xp], d_sib)

    def igown(rel):
        for xp in order:
            igblock(rel, xp, core)

    def addsib(rel, j):
        xp = order[j]
        recv(("is", rel, j), sibr.at[rel, xp])
        igp[rel, 2 * xp + core] += sibr[rel, xp]

    def zfirst(rel, j):
        xp = order[j]
        send("zf", igp.at[rel, 2 * xp + core, arows(1), :], zfr.at[xp], d_zlo,
             rs=slot(recvs, ("zf", j)), wait_later=False)

    def igfar(p, rel, k):
        for h, d in enumerate((d_xr, d_xl)):
            fs[k, h, pl.ds(0, RA[p][1] // 2), :] = igp[rel, 2 * xf + core, hrows(p, h), :].astype(BF)
            n = pl.ds(0, RA[p][1] // 2)
            send(("if", k, h), fs.at[k, h, n, :], farr.at[k, h, n, :], d)

    def ignear(p, rel, k):
        n = pl.ds(0, RA[p][1] // 2)
        for h, (xp, d) in enumerate(((xr, d_xr), (xl, d_xl))):
            rows_h = hrows(p, 1 - h)
            if k in ROUNDED:
                ns[k, h, n, :] = igp[rel, 2 * xp + core, rows_h, :].astype(BF)
                send(("in", k), ns.at[k, h, n, :], nowr.at[k, h, n, :], d)
            else:
                send(("in", k), igp.at[rel, 2 * xp + core, rows_h, :], nearr.at[rel, h, rows_h, :], d)

    def igsecond(p, rel, k):
        for h, (xp, d) in enumerate(((xr, d_xr), (xl, d_xl))):
            n = pl.ds(0, RA[p][1] // 2)
            recv(("if", k, h), farr.at[k, h, n, :])
            igp[rel, 2 * xp + core, hrows(p, h), :] += farr[k, h, n, :].astype(F32)
            send(("in", k), igp.at[rel, 2 * xp + core, hrows(p, h), :], nearr.at[rel, h, hrows(p, h), :], d)

    def iglast(p, rel, k):
        n = pl.ds(0, RA[p][1] // 2)
        first = [nowr.at[k, h, n, :] if k in ROUNDED else nearr.at[rel, h, hrows(p, 1 - h), :] for h in range(2)]
        second = [nearr.at[rel, h, hrows(p, h), :] for h in range(2)]
        recv(("in", k), *first, *second)
        for h in range(2):
            igp[rel, 2 * x + core, hrows(p, h), :] += second[h][...] + first[1 - h][...].astype(F32)

    def igfirst(rel, when):
        addsib(rel, 0)
        igfar(0, rel, rel)
        addsib(rel, 1)
        addsib(rel, 2)
        ignear(0, rel, rel)
        addsib(rel, 3)

        @pl.when(when)
        def _():
            for j in range(4):
                zfirst(rel, j)

    def gunit(e, send=True, sum=True):
        g = dot(xb[0, e, : 2 * R], agu[...], 0, 0)
        if sum:
            ws[e] = g
        if send:
            gb[e] = g.astype(BF)

    def hunit(e, send=True, sum=True):
        d = dot(ah[...], xb[1, e, : 2 * R], 0, 0)
        if sum:
            hs[e] = d
        if send:
            hb[e] = d.astype(BF)

    sides = ((yr, d_yr), (yl, d_yl))
    def zsend(rel):
        for h in range(2):
            send("zi", igp.at[rel, 2 * x + core, hrows(0, h), :], zr.at[hrows(0, h), :], d_zlo,
                 rs=slot(recvs, ("zir", h)), wait_later=False)

    def zfadd(j):
        xp = order[j]
        recv(("zf", j), zfr.at[xp])
        igp[keep, 2 * xp + core, arows(1), :] += zfr[xp]

    def hsecond(h):
        yp, d = sides[h]
        recv(("hf", h), hfr.at[h])
        hb[2 * yp + h] = (hs[2 * yp + h] + hfr[h].astype(F32)).astype(BF)
        send("gn", hb.at[2 * yp + h], hnr.at[h, h], d)

    def gsecond(h):
        yp, d = sides[h]
        recv(("gf", h), gfr.at[h])
        gb[2 * yp + h] = (ws[2 * yp + h] + gfr[h].astype(F32)).astype(BF)
        send("gn", gb.at[2 * yp + h], gnr.at[h, h], d)

    keep = inner
    igstart(1)
    igown(1)
    recv("acth", ah.at[away, :])
    for h, (yp, d) in enumerate(sides):
        hunit(2 * yf + h, sum=False)
        send(("hf", h), hb.at[2 * yf + h], hfr.at[h], d)
    igfirst(1, is_outer)
    for h, (yp, d) in enumerate(sides):
        hunit(2 * yp + 1 - h, sum=False)
        send("gn", hb.at[2 * yp + 1 - h], hnr.at[h, 1 - h], d)
    recv("actg", agu.at[away, :])
    for h, (yp, d) in enumerate(sides):
        gunit(2 * yf + h, sum=False)
        send(("gf", h), gb.at[2 * yf + h], gfr.at[h], d)
    igstart(0)
    igsecond(0, 1, 1)
    igown(0)
    for h, (yp, d) in enumerate(sides):
        hunit(2 * yp + h, send=False)
    igfirst(0, is_inner)
    for h, (yp, d) in enumerate(sides):
        gunit(2 * yp + 1 - h, sum=False)
        send("gn", gb.at[2 * yp + 1 - h], gnr.at[h, 1 - h], d)
    for h in range(2):
        hsecond(h)
    for h, (yp, d) in enumerate(sides):
        gunit(2 * yp + h, send=False)
    iglast(0, 1, 1)

    @pl.when(is_outer)
    def _():
        zsend(1)

    zfadd(0)
    igfar(1, keep, 2)
    gsecond(0)
    gsecond(1)
    igsecond(0, 0, 0)
    zfadd(1)
    zfadd(2)
    ignear(1, keep, 2)
    for h in range(2):
        gunit(2 * y + h, send=False)
        hunit(2 * y + h, send=False)
    igsecond(1, keep, 2)
    iglast(0, 0, 0)

    @pl.when(is_inner)
    def _():
        zsend(0)

    zfadd(3)
    iglast(1, keep, 2)

    @pl.when(is_inner)
    def _():
        igs[2, pl.ds(0, ZF), :] = igp[1, 2 * x + core, arows(1), :].astype(BF)
        send("zo", igs.at[2, pl.ds(0, ZF), :], igr.at[2, pl.ds(0, ZF), :], d_zz,
             rs=slot(recvs, ("zo", 2)), wait_later=False)
        n = pl.ds(0, (R - ZF) // 2)
        for h in range(2):
            recv(("zir", h), zr.at[hrows(0, h), :])
            igs[h, n, :] = (igp[1, 2 * x + core, hrows(0, h), :] + zr[hrows(0, h), :]).astype(BF)
            send("zo", igs.at[h, n, :], igr.at[h, n, :], d_zz,
                 rs=slot(recvs, ("zo", h)), wait_later=False)

    @pl.when(is_outer)
    def _():
        ig_o[arows(1), :] = igp[0, 2 * x + core, arows(1), :].astype(BF)

    recv("gn", *[b.at[s, h] for b in (gnr, hnr) for s in range(2) for h in range(2)])
    for h in range(2):
        g = (ws[2 * y + h] + gnr[0, h].astype(F32) + gnr[1, h].astype(F32)) * factor
        gg_o[pl.ds(h * C, C), :] = g[:, :F]
        ug_o[pl.ds(h * C, C), :] = g[:, F:]
        dg_o[:, pl.ds(h * C, C)] = (hs[2 * y + h] + hnr[0, h].astype(F32) + hnr[1, h].astype(F32)) * factor

    @pl.when(is_outer)
    def _():
        for h in range(2):
            recv(("zir", h), zr.at[hrows(0, h), :])
            ig_o[hrows(0, h), :] = (igp[0, 2 * x + core, hrows(0, h), :] + zr[hrows(0, h), :]).astype(BF)

    @pl.when(is_inner)
    def _():
        zs, n = pl.ds(0, ZF), pl.ds(0, (R - ZF) // 2)
        recv(("zo", 2), igr.at[2, zs, :])
        ig_o[arows(1), :] = igr[2, zs, :]
        for h in range(2):
            recv(("zo", h), igr.at[h, n, :])
            ig_o[hrows(0, h), :] = igr[h, n, :]
        wait_bytes(ssem.at[slot(sends, "zo")], R * C * 2)
        relayed = (ROUNDS[1][3] + ROUNDS[3][3] + 4 * HOME) * C * 2
        wait_bytes(ssem.at[slot(sends, "zrel")], relayed)

    wait_bytes(ssem.at[slot(sends, "zi")], (R - ZF) * C * 4)
    wait_bytes(ssem.at[slot(sends, "zf")], 4 * ZF * C * 4)
    wait_bytes(ssem.at[slot(sends, "hs")], 8 * HOME * C * 2)
    for k, sizes in enumerate(groups):
        wait_bytes(ssem.at[slot(sends, ("group", k))], sum(sizes))
    assert len(sends) <= NSEND and len(recvs) <= NRECV, (len(sends), len(recvs))


def deliver(*refs):
    n = (len(refs) - 1) // 2
    copies = [pltpu.make_async_copy(refs[k], refs[n + k], refs[-1].at[k]) for k in range(n)]
    for c in copies:
        c.start()
    for c in copies:
        c.wait()


def shards(tokens, out_grad, gate_weight, up_weight, down_weight):
    R, C = tokens.shape
    F = gate_weight.shape[1]
    H = R // 2
    factor = 1.0 / math.sqrt(R * lax.axis_size(FSDP))
    anyspec = pl.BlockSpec(memory_space=pl.ANY)
    vm = pl.BlockSpec(memory_space=pltpu.VMEM)
    V = pltpu.VMEM
    scratch = [
        V((2, R, C), BF), V((2, 8, 2 * R + HOME, C), BF), V((4, 2 * C, 2 * F), BF), V((4, F, 2 * C), BF),
        V((2, R, 2 * F), F32), V((2, R, F), F32), V((R, 2 * F), F32), V((R, F), F32),
        V((2 * R, 2 * F), BF), V((2 * R, F), BF),
        V((2, 8, R, C), F32), V((2, 4, R, C), F32), V((3, 2, H, C), BF), V((2, 2, R, C), F32), V((3, 2, H, C), BF), V((3, 2, H, C), BF), V((3, 2, H, C), BF), V((4, ZF, C), F32),
        V((R, C), F32), V((3, H, C), BF), V((3, H, C), BF),
        V((8, C, 2 * F), F32), V((8, F, C), F32), V((8, C, 2 * F), BF), V((8, F, C), BF),
        V((2, C, 2 * F), BF), V((2, F, C), BF), V((2, 2, C, 2 * F), BF), V((2, 2, F, C), BF),
        pltpu.SemaphoreType.DMA((8,)), pltpu.SemaphoreType.DMA((NSEND,)), pltpu.SemaphoreType.DMA((NRECV,)),
    ]
    held = pl.pallas_call(
        functools.partial(kernel, factor),
        out_shape=(
            V((R, C), BF),
            V((2 * C, F), F32),
            V((2 * C, F), F32),
            V((F, 2 * C), F32),
        ),
        in_specs=[anyspec] * 5,
        out_specs=(vm,) * 4,
        scratch_shapes=scratch,
        compiler_params=pltpu.CompilerParams(
            collective_id=0, has_side_effects=True, vmem_limit_bytes=60 * 1024 * 1024),
        name="ffn_backward",
    )(tokens, out_grad, gate_weight, up_weight, down_weight)
    return pl.pallas_call(
        deliver,
        out_shape=tuple(jax.ShapeDtypeStruct(a.shape, a.dtype) for a in held),
        in_specs=[vm] * len(held),
        out_specs=(anyspec,) * len(held),
        scratch_shapes=[pltpu.SemaphoreType.DMA((len(held),))],
        name="deliver",
    )(*[pltpu.with_memory_space_constraint(a, pltpu.VMEM) for a in held])


def solution(mesh):
    finer = Mesh(mesh.devices.reshape(2, 4, 2, 4, 2), ("z_hi", "y", "z_lo", "x", "core"))
    return jax.shard_map(
        shards,
        mesh=finer,
        in_specs=(P(FSDP, TP), P(FSDP, TP), P(FSDP, TP), P(FSDP, TP), P(TP, FSDP)),
        out_specs=(P(FSDP, TP), P(FSDP, TP), P(FSDP, TP), P(TP, FSDP)),
        check_vma=False,
    )
```
